32 devices in a mesh: tm: 8 (over z, x), lev: 4 (over y, core).
Axes of the slice: x: 2, y: 2, z: 4, core: 2. Of those that a mesh axis runs over, the one named last changes fastest.
Arguments:
- increment: float32 [8, 3, 8, 256, 512], P('tm', None, 'lev'), may hold values from -6 to 6
- multiplier: float32 [8, 3, 8, 256, 512], P('tm', None, 'lev'), may hold values from -6 to 6
- error_var: float32 [8, 3, 8, 256, 512], P('tm', None, 'lev'), may hold values from 0.1 to 1
- obs_cell: int32 [8, 8, 512], P('tm', 'lev'), may hold values from 0 to 131071
- obs_dual: float32 [8, 8, 512], P('tm', 'lev'), may hold values from -6 to 6
- obs_var: float32 [8, 8, 512], P('tm', 'lev'), may hold values from 0.5 to 2
- level_gain: float32 [8], P('lev'), may hold values from 0.5 to 1.5
- mean_depth: float32 [8], P('lev'), may hold values from 0.5 to 2
- chain_decay: float32 [8, 3, 8], P('tm', None, 'lev'), may hold values from 0 to 1
Outputs:
- dual_product: float32 [8, 3, 8, 256, 512], P('tm', None, 'lev')
- obs_product: float32 [8, 8, 512], P('tm', 'lev')
- state_block_product: float32 [8, 3, 8, 256, 512], P('tm', None, 'lev')
- chain_solution: float32 [8, 3, 8, 256, 512], P('tm', None, 'lev')
The draws below stay inside these ranges and needn't reach their ends.
All inputs are finite; a program needn't handle non-finite values.
Results may differ from the reference program's by a relative error of at most 0.0001.
Values sent between devices are 32-bit elements; how exact they have to be, the bound alone decides.
A program may use at most 320 MiB of HBM per device.

```python
import math
import jax
import jax.numpy as jnp
from jax import lax

GX = 256
GY = 512
STEPS = 2
NOBS = 512
WINDOW_PIECES = 8
LEVELS = 8


def draw_chain_decay(key, part):
    key_slow = jax.random.fold_in(key, 11)
    key_base = jax.random.fold_in(key, 12)
    key_jitter = jax.random.fold_in(key, 13)
    pulse_seed_handle = jax.random.fold_in(key, 14)
    key_depth = jax.random.fold_in(key, 15)
    slow_share = 0.5
    slow = jax.random.uniform(key_slow, (3, LEVELS), jnp.float32) < slow_share
    fast_rate = jnp.exp(jax.random.uniform(key_base, (3, LEVELS), jnp.float32, jnp.log(0.5), jnp.log(1.5)))
    slow_rate = jnp.full((3, LEVELS), -jnp.log(0.3) / WINDOW_PIECES, jnp.float32)
    base = jnp.where(slow, slow_rate, fast_rate)
    jitter = jax.random.uniform(key_jitter, (WINDOW_PIECES, 3, LEVELS), jnp.float32, 0.5, 1.5)
    scale_multiplier = jnp.exp(-base[None] * jitter)
    piece_pulses_sampled = jax.random.randint(pulse_seed_handle, (2,), 0, WINDOW_PIECES)
    measured_positions = jnp.arange(WINDOW_PIECES)
    measured_indicator = jnp.any(measured_positions[:, None] == piece_pulses_sampled[None, :], axis=1)
    depth_draw = jax.random.uniform(key_depth, (WINDOW_PIECES, 3, LEVELS), jnp.float32, 0.5, 0.8)
    return jnp.where(measured_indicator[:, None, None], scale_multiplier * depth_draw, scale_multiplier)


def set_ends(values, stream_key, least, top_value):
    longest = values.shape.index(max(values.shape))
    spots = []
    for shift in (0, 1):
        where = [jax.random.randint(jax.random.fold_in(stream_key, axis), (), 0, length) for axis, length in enumerate(values.shape)]
        where[longest] = (where[longest] + shift) % values.shape[longest]
        spots.append(tuple(where))
    return values.at[spots[0]].set(least).at[spots[1]].set(top_value)


def shard_levels(rng, dims, split, smallest, high):
    def one(axis_at, shards_of):
        heights = jax.random.uniform(jax.random.fold_in(jax.random.fold_in(rng, 6), axis_at), (shards_of,), jnp.float32, smallest / len(split), high / len(split))
        return jnp.repeat(jnp.exp(heights), dims[axis_at] // shards_of).reshape((-1,) + (1,) * (len(dims) - axis_at - 1))

    factor_of = one(*split[0])
    for cut in split[1:]:
        factor_of = factor_of * one(*cut)
    return factor_of


def normal_values(stream_key, dims, width, most, shards=(), dtype=jnp.bfloat16):
    loudness = shard_levels(stream_key, dims, shards, -0.22, 0.18) if shards else 1.0
    values = jax.random.normal(stream_key, dims, jnp.float32) * width * loudness
    return jnp.minimum(jnp.maximum(values, -most), most).astype(dtype)


def setup_inputs(seed: int = 0) -> dict:
    splits = jax.random.split(jax.random.key(seed), 10)
    increment = normal_values(splits[0], (WINDOW_PIECES, 3, LEVELS, GX, GY), 1.0, 6.0, ((0, 8), (2, 4)), jnp.float32)
    multiplier = normal_values(splits[1], (WINDOW_PIECES, 3, LEVELS, GX, GY), 1.0, 6.0, ((0, 8), (2, 4)), jnp.float32)
    error_var = jnp.clip(jnp.exp(math.log(1.0) - 2.3025851 * jax.random.uniform(splits[2], (WINDOW_PIECES, 3, LEVELS, GX, GY), jnp.float32) ** shard_levels(splits[2], (WINDOW_PIECES, 3, LEVELS, GX, GY), ((0, 8), (2, 4)), -0.2, 0.2)), 0.1, 1.0)
    obs_cell = set_ends(jax.random.randint(splits[3], (WINDOW_PIECES, LEVELS, NOBS), 0, GX * GY), jax.random.fold_in(splits[3], 1), 0, (GX * GY) - 1).astype(jnp.int32)
    obs_dual = normal_values(splits[4], (WINDOW_PIECES, LEVELS, NOBS), 1.0, 6.0, ((0, 8), (1, 4)), jnp.float32)
    obs_var = jnp.clip(jnp.exp(math.log(2.0) - 1.3862944 * jax.random.uniform(splits[5], (WINDOW_PIECES, LEVELS, NOBS), jnp.float32) ** shard_levels(splits[5], (WINDOW_PIECES, LEVELS, NOBS), ((0, 8), (1, 4)), -0.2, 0.2)), 0.5, 2.0)
    level_gain = jnp.clip(0.5 + 1.0 * jax.random.uniform(splits[6], (LEVELS,), jnp.float32) ** shard_levels(splits[6], (LEVELS,), ((0, 4),), -0.2, 0.2), 0.5, 1.5)
    mean_depth = jnp.clip(jnp.exp(math.log(2.0) - 1.3862944 * jax.random.uniform(splits[7], (LEVELS,), jnp.float32) ** shard_levels(splits[7], (LEVELS,), ((0, 4),), -0.2, 0.2)), 0.5, 2.0)
    chain_decay = draw_chain_decay(jax.random.fold_in(splits[9], 71), 0)
    return dict(increment=increment, multiplier=multiplier, error_var=error_var, obs_cell=obs_cell, obs_dual=obs_dual, obs_var=obs_var, level_gain=level_gain, mean_depth=mean_depth, chain_decay=chain_decay)


TIME_STEP = 0.25
ROTATION_PARAM = 0.5
COUPLING = 0.25

def dynamics_advance(state, column, level_gain, mean_depth):
    h, u, v = (state[0], state[1], state[2])
    p = level_gain[:, None, None] * h + COUPLING * column[None]
    gradient_eastward = jnp.concatenate([p[:, 1:, :], jnp.zeros_like(p[:, :1, :])], axis=1) - p
    grad_y = jnp.concatenate([p[:, :, 1:], jnp.zeros_like(p[:, :, :1])], axis=2) - p
    u_new = u + TIME_STEP * (ROTATION_PARAM * v - gradient_eastward)
    v_new = v - TIME_STEP * (ROTATION_PARAM * u + grad_y)
    back_x = u_new - jnp.concatenate([jnp.zeros_like(u_new[:, :1, :]), u_new[:, :-1, :]], axis=1)
    back_y = v_new - jnp.concatenate([jnp.zeros_like(v_new[:, :, :1]), v_new[:, :, :-1]], axis=2)
    h_new = h - TIME_STEP * mean_depth[:, None, None] * (back_x + back_y)
    return jnp.stack([h_new, u_new, v_new])

def reference(increment, multiplier, error_var, obs_cell, obs_dual, obs_var, level_gain, mean_depth, chain_decay):

    def advance(state):
        for step in range(STEPS):
            state = dynamics_advance(state, lax.optimization_barrier(jnp.sum(state[0], axis=0)), level_gain, mean_depth)
        return state

    def flip_matrix(state):
        return jax.vjp(advance, state)[1](state)[0]
    advanced = lax.map(advance, increment)
    returned = lax.map(flip_matrix, multiplier)
    forward_term = jnp.concatenate([jnp.zeros_like(advanced[:1]), advanced[:-1]], axis=0)
    backward_term = jnp.concatenate([returned[1:], jnp.zeros_like(returned[:1])], axis=0)
    dual_product = error_var * multiplier + increment - forward_term
    flat_h = increment[:, 0].reshape(WINDOW_PIECES, LEVELS, GX * GY)
    picked = jnp.take_along_axis(flat_h, obs_cell, axis=2)
    obs_product = obs_var * obs_dual + picked

    def spread(cells, values):
        return jnp.zeros((GX * GY,), jnp.float32).at[cells].add(values)
    added = jax.vmap(jax.vmap(spread))(obs_cell, obs_dual).reshape(WINDOW_PIECES, LEVELS, GX, GY)
    state_block_product = multiplier - backward_term
    state_block_product = state_block_product.at[:, 0].add(added)

    def recur(carry, inputs):
        scale_multiplier, value = inputs
        result = scale_multiplier[:, :, None, None] * carry + value
        return (result, result)
    first = jnp.zeros_like(dual_product[0])
    unused, chain_solution = lax.scan(recur, first, (chain_decay, dual_product))
    return (dual_product, obs_product, state_block_product, chain_solution)
```

```python
import functools
from typing import Any, NamedTuple

import jax
import jax.numpy as jnp
from jax import lax
from jax.experimental import pallas as pl
from jax.experimental.pallas import tpu as pltpu
from jax.sharding import PartitionSpec as P

TIME_STEP = 0.25
ROTATION_PARAM = 0.5
COUPLING = 0.25
HALF = TIME_STEP * ROTATION_PARAM
SPLIT = 2
PAD = 8
MESH_ID = pl.DeviceIdType.MESH


class Scratch(NamedTuple):
    inc: Any
    mult: Any
    work: Any
    b1: Any
    own: Any
    swap: Any
    tangent: Any
    adjoint: Any
    tangent_in: Any
    adjoint_in: Any
    carried: Any
    sent: Any
    relay_t: Any
    relay_a: Any
    sums: Any
    met: Any
    total: Any
    columns: Any
    added: Any
    decay: Any
    decay_in: Any
    own_send: Any
    own_recv: Any
    tan_send: Any
    tan_recv: Any
    adj_send: Any
    adj_recv: Any
    rt_send: Any
    rt_recv: Any
    ra_send: Any
    ra_recv: Any
    ch_send: Any
    ch_recv: Any
    dual_sem: Any
    block_sem: Any
    chain_sem: Any
    decay_send: Any
    decay_recv: Any
    loads: Any
    lev_send: Any
    lev_recv: Any


def pieces(rows):
    return SPLIT if rows % (8 * SPLIT) == 0 else 1


def block_rows(rows):
    part = rows // pieces(rows)
    return next(b for b in (32, 16, 8, part) if part % b == 0)


def up_y(a):
    lane = lax.broadcasted_iota(jnp.int32, a.shape, 1)
    return jnp.where(lane == a.shape[1] - 1, 0.0, pltpu.roll(a, a.shape[1] - 1, 1))


def down_y(a):
    lane = lax.broadcasted_iota(jnp.int32, a.shape, 1)
    return jnp.where(lane == 0, 0.0, pltpu.roll(a, 1, 1))


def up_x(a):
    return pltpu.roll(a, a.shape[0] - 1, 0)


def down_x(a):
    return pltpu.roll(a, 1, 0)


def kernel(
    n, size, increment, multiplier, error_var, obs_cell, obs_dual, obs_var, level_gain, mean_depth,
    chain_decay, dual_out, obs_out, block_out, chain_out, *scratch,
):
    b = Scratch(*scratch)
    fields, levels, rows, cols = increment.shape[1:]
    planes = fields * levels
    per = pieces(rows)
    chunks = planes * per
    part = rows // per
    step = block_rows(rows)
    wide = step + 2 * PAD

    s = lax.axis_index("tm")
    lev = lax.axis_index("lev")
    odd = s % 2
    even = odd == 0
    pair = s // 2
    pairs = n // 2
    partner = s + 1 - 2 * odd

    def adjoint_cut(k):
        return chunks * (pairs - 1 - k) // pairs

    def tangent_cut(k):
        return jnp.minimum(chunks, chunks * (k + 1) // pairs + 1)

    def loop(low, high, fn):
        lax.fori_loop(low, high, lambda c, z: (fn(c), z)[1], 0)

    def where_in(c):
        return c // per, pl.ds(pl.multiple_of((c % per) * part, 8), part)

    def piece(ref, c):
        p, r = where_in(c)
        return ref.at[p, r, :]

    def remote(src, dst, send, recv, where):
        return pltpu.make_async_remote_copy(
            src_ref=src, dst_ref=dst, send_sem=send, recv_sem=recv, device_id=where, device_id_type=MESH_ID,
        )

    def move(src, dst, send, recv, c, to):
        return remote(piece(src, c), piece(dst, c), send.at[c], recv.at[c], {"tm": to})

    def lev_move(src, dst, i, to):
        return remote(src, dst, b.lev_send.at[i], b.lev_recv.at[i], {"lev": to})

    def own_copy(c):
        return move(b.own, b.swap, b.own_send, b.own_recv, c, partner)

    def tangent_copy(c):
        return move(b.tangent, b.tangent_in, b.tan_send, b.tan_recv, c, s + 1)

    def adjoint_copy(c):
        return move(b.adjoint, b.adjoint_in, b.adj_send, b.adj_recv, c, s - 1)

    def chain_copy(c):
        return move(b.sent, b.carried, b.ch_send, b.ch_recv, c, s + 2)

    def tangent_leg(c, to):
        return move(b.tangent, b.relay_t, b.tan_send, b.rt_recv, c, to)

    def tangent_turn(c, to):
        return move(b.relay_t, b.tangent_in, b.rt_send, b.tan_recv, c, to)

    def adjoint_leg(c, to):
        return move(b.adjoint, b.relay_a, b.adj_send, b.ra_recv, c, to)

    def adjoint_turn(c, to):
        return move(b.relay_a, b.adjoint_in, b.ra_send, b.adj_recv, c, to)

    def result_copy(src, out, sems, c):
        p, r = where_in(c)
        return pltpu.make_async_copy(piece(src, c), out.at[0, p // levels, p % levels, r, :], sems.at[c])

    def dual_copy(c):
        return result_copy(b.tangent_in, dual_out, b.dual_sem, c)

    def chain_result(c):
        return result_copy(b.carried, chain_out, b.chain_sem, c)

    def block_copy(c):
        return result_copy(b.adjoint_in, block_out, b.block_sem, c)

    decay_copy = remote(b.decay, b.decay_in, b.decay_send.at[0], b.decay_recv.at[0], {"tm": s - 1})

    def load(i, p):
        src = (increment, multiplier, error_var)[i]
        dst = (b.inc, b.mult, b.work)[i]
        return pltpu.make_async_copy(
            src.at[0, p // levels, p % levels], dst.at[p, pl.ds(PAD, rows), :], b.loads.at[i * planes + p]
        )

    for p in range(planes):
        for i in range(3):
            load(i, p).start()

    barrier = pltpu.get_barrier_semaphore()
    near = ((s >= 1, s - 1), (s >= 2, s - 2), (s < n - 1, s + 1), (s < n - 2, s + 2))
    for there, who in near:
        @pl.when(there)
        def _():
            pl.semaphore_signal(barrier, inc=1, device_id={"tm": who}, device_id_type=MESH_ID)
    bits = []
    bit = 1
    while bit < size:
        bits.append(bit)
        bit *= 2

    def across(bit):
        return lev + bit - 2 * bit * ((lev // bit) % 2)

    for bit in bits:
        pl.semaphore_signal(barrier, inc=1, device_id={"lev": across(bit)}, device_id_type=MESH_ID)

    def edges(ref, planes):
        zero = jnp.zeros((PAD, cols), jnp.float32)
        for p in range(planes):
            ref[p, pl.ds(0, PAD), :] = zero
            ref[p, pl.ds(PAD + rows, PAD), :] = zero

    for ref in (b.inc, b.mult, b.work, b.b1):
        edges(ref, planes)
    edges(b.columns, 4)
    for f in range(fields):
        for l in range(levels):
            b.decay[f * levels + l] = jnp.full((1, 128), chain_decay[0, f, l], jnp.float32)

    def own_at(c):
        p, r = where_in(c)

        @pl.when(c % per == 0)
        def _():
            for i in range(3):
                load(i, p).wait()

        inner = pl.ds(pl.multiple_of((c % per) * part + PAD, 8), part)
        b.own[p, r, :] = b.work[p, inner, :] * b.mult[p, inner, :] + b.inc[p, inner, :]

    gives_own = jnp.logical_or(even, s < n - 1)

    def give_own(c):
        @pl.when(gives_own)
        def _():
            own_copy(c).start()

    own_at(0)
    pl.semaphore_wait(barrier, len(bits) + sum(there.astype(jnp.int32) for there, _ in near))

    def own_next(c):
        own_at(c)
        give_own(c - 1)

    loop(1, chunks, own_next)
    give_own(chunks - 1)

    @pl.when(s >= 1)
    def _():
        decay_copy.start()

    def row_index(r0):
        return lax.broadcasted_iota(jnp.int32, (wide, cols), 0) + (r0 - PAD)

    def forward(h, u, v, column, r0, gain, depth):
        p = gain * h
        if column is not None:
            p = p + COUPLING * column
        u_new = u + TIME_STEP * (ROTATION_PARAM * v - (up_x(p) - p))
        v_new = v - TIME_STEP * (ROTATION_PARAM * u + (up_y(p) - p))
        u_new = jnp.where(row_index(r0) < 0, 0.0, u_new)
        h_new = h - TIME_STEP * depth * ((u_new - down_x(u_new)) + (v_new - down_y(v_new)))
        return h_new, u_new, v_new

    def back(h, u, v, r0, gain, depth):
        w = depth * h
        u2 = u + TIME_STEP * (up_x(w) - w)
        v2 = v + TIME_STEP * (up_y(w) - w)
        u2 = jnp.where(row_index(r0) < 0, 0.0, u2)
        p = TIME_STEP * ((u2 - down_x(u2)) + (v2 - down_y(v2)))
        return h + gain * p, u2 - HALF * v2, v2 + HALF * u2, p

    def middle(a):
        return a[PAD:PAD + step]

    def state_at(ref, l, r0):
        at = pl.ds(r0, wide)
        return ref[l, at, :], ref[levels + l, at, :], ref[2 * levels + l, at, :]

    def sweep(fn):
        loop(0, rows // step, lambda i: fn(pl.multiple_of(i * step, 8)))

    def put(ref, l, r0, values):
        for f, value in enumerate(values):
            ref[f * levels + l, pl.ds(r0, step), :] = middle(value)

    def put_padded(ref, l, r0, values):
        put(ref, l, r0 + PAD, values)

    sums = b.sums

    def ahead(r0):
        c0 = c1 = None
        for l in range(levels):
            h, u, v = state_at(b.inc, l, r0)
            h_new, _, _ = forward(h, u, v, None, r0, level_gain[l], mean_depth[l])
            c0 = middle(h) if c0 is None else c0 + middle(h)
            c1 = middle(h_new) if c1 is None else c1 + middle(h_new)
        sums[0, pl.ds(r0, step), :] = c0
        sums[0, pl.ds(rows + r0, step), :] = c1

    def behind(source, to):
        def fn(r0):
            bar = None
            for l in range(levels):
                h, u, v = state_at(source, l, r0)
                h2, u2, v2, p = back(h, u, v, r0, level_gain[l], mean_depth[l])
                if to == 0:
                    put_padded(b.b1, l, r0, (h2, u2, v2))
                bar = middle(p) if bar is None else bar + middle(p)
            sums[1, pl.ds(to * rows + r0, step), :] = COUPLING * bar
        return fn

    sweep(ahead)
    sweep(behind(b.mult, 0))
    sweep(behind(b.b1, 1))
    depth_sum = mean_depth[0]
    for l in range(1, levels):
        depth_sum = depth_sum + mean_depth[l]
    for k in range(2):
        sums[k, pl.ds(2 * rows, PAD), :] = jnp.full((PAD, cols), depth_sum, jnp.float32)

    half = lev % 2
    tall = 2 * rows + PAD
    total = b.total

    def meet_copy():
        return lev_move(sums.at[1 - half], b.met.at[0], 0, across(1))

    def add_met(slot, first):
        def fn(r0):
            at = pl.ds(r0, PAD)
            kept = sums[half, at, :] if first else total[at, :]
            total[at, :] = kept + b.met[slot, at, :]
        loop(0, tall // PAD, lambda i: fn(pl.multiple_of(i * PAD, 8)))

    meet = meet_copy()
    meet.start()
    meet.wait()
    add_met(0, True)

    def observe():
        count = obs_cell.shape[2]
        if cols & (cols - 1) == 0:
            shift = cols.bit_length() - 1

            def split(cells):
                return cells >> shift, cells & (cols - 1)
        else:
            def split(cells):
                return lax.div(cells, cols), lax.rem(cells, cols)

        row = lax.broadcasted_iota(jnp.int32, (rows, count), 0)
        col = lax.broadcasted_iota(jnp.int32, (cols, count), 0)
        for l in range(levels):
            at_row, at_col = split(obs_cell[0, pl.ds(l, 1), :])
            values = obs_dual[0, pl.ds(l, 1), :]
            hit_row = jnp.where(row == at_row, 1.0, 0.0)
            hit_col = jnp.where(col == at_col, 1.0, 0.0)
            seen = lax.dot_general(
                b.inc[l, pl.ds(PAD, rows), :], hit_col, (((1,), (0,)), ((), ())),
                precision=lax.Precision.HIGHEST, preferred_element_type=jnp.float32,
            )
            picked = jnp.sum(hit_row * seen, axis=0, keepdims=True)
            obs_out[0, pl.ds(l, 1), :] = obs_var[0, pl.ds(l, 1), :] * values + picked
            b.added[l] = lax.dot_general(
                hit_row * values, hit_col, (((1,), (1,)), ((), ())),
                precision=lax.Precision.HIGHEST, preferred_element_type=jnp.float32,
            )

    for i, bit in enumerate(bits[1:], 1):
        far = lev_move(total, b.met.at[i], i, across(bit))
        far.start()
        if i == 1:
            observe()
        far.wait()
        add_met(i, False)
    if len(bits) < 2:
        observe()

    columns = b.columns

    def first_column(r0):
        columns[2 * half, pl.ds(r0 + PAD, step), :] = total[pl.ds(r0, step), :]

    def second_column(r0):
        c = columns[2 * half, pl.ds(r0, wide), :]
        gx = jnp.where(row_index(r0) < 0, 0.0, up_x(c) - c)
        gy = up_y(c) - c
        lap = (gx - down_x(gx)) + (gy - down_y(gy))
        scale = (TIME_STEP * TIME_STEP * COUPLING) * total[pl.ds(2 * rows, 1), pl.ds(0, 1)]
        columns[2 * half + 1, pl.ds(r0 + PAD, step), :] = total[pl.ds(rows + r0, step), :] + scale * middle(lap)

    sweep(first_column)
    sweep(second_column)
    mine = columns.at[pl.ds(2 * half, 2)]
    near_copy = lev_move(mine, mine, len(bits), across(1))
    near_copy.start()
    near_copy.wait()

    def last_back(r0):
        at = pl.ds(r0, wide)
        bar0, bar1 = columns[2, at, :], columns[3, at, :]
        for l in range(levels):
            h, u, v = state_at(b.b1, l, r0)
            h2, u2, v2, _ = back(h + bar0, u, v, r0, level_gain[l], mean_depth[l])
            put(b.adjoint, l, r0, (h2 + bar1, u2, v2))

    def first_forward(r0):
        column = columns[0, pl.ds(r0, wide), :]
        for l in range(levels):
            h, u, v = state_at(b.inc, l, r0)
            put_padded(b.work, l, r0, forward(h, u, v, column, r0, level_gain[l], mean_depth[l]))

    def last_forward(r0):
        column = columns[1, pl.ds(r0, wide), :]
        for l in range(levels):
            h, u, v = state_at(b.work, l, r0)
            put(b.tangent, l, r0, forward(h, u, v, column, r0, level_gain[l], mean_depth[l]))

    sweep(last_back)
    below = pair - 1
    down_cut = adjoint_cut(below)
    across_cut = adjoint_cut(pair)

    @pl.when(jnp.logical_and(even, s >= 2))
    def _():
        loop(0, down_cut, lambda c: adjoint_leg(c, s - 2).start())
        loop(down_cut, chunks, lambda c: adjoint_leg(c, s + 1).start())

    sweep(first_forward)
    sweep(last_forward)
    up_cut = tangent_cut(pair)
    here_cut = tangent_cut(below)
    climbs = jnp.logical_and(odd == 1, s < n - 1)

    @pl.when(even)
    def _():
        loop(0, chunks, lambda c: tangent_copy(c).start())

    @pl.when(climbs)
    def _():
        loop(0, up_cut, lambda c: tangent_leg(c, s + 2).start())
        loop(up_cut, chunks, lambda c: tangent_leg(c, s - 1).start())

    @pl.when(s < n - 1)
    def _():
        decay_copy.wait_recv()

    def chain_step(c):
        p, r = where_in(c)
        d = chain_decay[0, p // levels, p % levels]

        @pl.when(s >= 1)
        def _():
            tangent_copy(c).wait_recv()

        @pl.when(s == 0)
        def _():
            b.tangent_in[p, r, :] = jnp.zeros((part, cols), jnp.float32)

        @pl.when(s >= 2)
        def _():
            chain_copy(c).wait_recv()

        @pl.when(s < 2)
        def _():
            b.carried[p, r, :] = jnp.zeros((part, cols), jnp.float32)

        @pl.when(jnp.logical_or(odd == 1, s < n - 2))
        def _():
            own_copy(c).wait_recv()

        swap = b.swap[p, r, :]
        product = b.own[p, r, :] - b.tangent_in[p, r, :]
        here = d * (b.carried[p, r, :] + jnp.where(odd == 1, swap, 0.0)) + product
        b.tangent_in[p, r, :] = product
        b.carried[p, r, :] = here

        @pl.when(s < n - 2)
        def _():
            d_next = b.decay_in[p][:, :1]
            b.sent[p, r, :] = d_next * here + (jnp.where(even, swap, 0.0) - b.tangent[p, r, :])
            chain_copy(c).start()

        dual_copy(c).start()
        chain_result(c).start()

    loop(0, jnp.where(s == 0, chunks, 0), chain_step)

    @pl.when(jnp.logical_and(even, s < n - 2))
    def _():
        def turn_up(c):
            tangent_leg(c, s - 1).wait_recv()
            tangent_turn(c, s + 2).start()

        def turn_across(c):
            adjoint_leg(c, s - 2).wait_recv()
            adjoint_turn(c, s + 1).start()

        loop(up_cut, chunks, turn_up)
        loop(0, across_cut, turn_across)

    @pl.when(odd == 1)
    def _():
        @pl.when(s >= 3)
        def _():
            def turn_across(c):
                tangent_leg(c, s + 2).wait_recv()
                tangent_turn(c, s - 1).start()

            loop(0, here_cut, turn_across)

        loop(0, chunks, lambda c: adjoint_copy(c).start())

        @pl.when(s >= 3)
        def _():
            def turn_down(c):
                adjoint_leg(c, s + 1).wait_recv()
                adjoint_turn(c, s - 2).start()

            loop(down_cut, chunks, turn_down)

    loop(0, jnp.where(s == 0, 0, chunks), chain_step)

    def block_step(i):
        c = lax.rem(i + across_cut * odd, chunks)
        p, r = where_in(c)
        inner = pl.ds(pl.multiple_of((c % per) * part + PAD, 8), part)

        @pl.when(s < n - 1)
        def _():
            adjoint_copy(c).wait_recv()

        kept = b.mult[p, inner, :] - jnp.where(s < n - 1, b.adjoint_in[p, r, :], 0.0)
        b.adjoint_in[p, r, :] = kept

        @pl.when(p < levels)
        def _():
            b.adjoint_in[p, r, :] = kept + b.added[jnp.minimum(p, levels - 1), r, :]

        block_copy(c).start()

    loop(0, chunks, block_step)

    @pl.when(gives_own)
    def _():
        loop(0, chunks, lambda c: own_copy(c).wait_send())

    @pl.when(s < n - 1)
    def _():
        loop(0, chunks, lambda c: tangent_copy(c).wait_send())

    @pl.when(s >= 1)
    def _():
        loop(0, chunks, lambda c: adjoint_copy(c).wait_send())
        decay_copy.wait_send()

    @pl.when(jnp.logical_and(even, s < n - 2))
    def _():
        loop(up_cut, chunks, lambda c: tangent_turn(c, s + 2).wait_send())
        loop(0, across_cut, lambda c: adjoint_turn(c, s + 1).wait_send())

    @pl.when(jnp.logical_and(odd == 1, s >= 3))
    def _():
        loop(0, here_cut, lambda c: tangent_turn(c, s - 1).wait_send())
        loop(down_cut, chunks, lambda c: adjoint_turn(c, s - 2).wait_send())

    @pl.when(s < n - 2)
    def _():
        loop(0, chunks, lambda c: chain_copy(c).wait_send())

    loop(0, chunks, lambda c: dual_copy(c).wait())
    loop(0, chunks, lambda c: chain_result(c).wait())
    loop(0, chunks, lambda c: block_copy(c).wait())


def shards(
    increment, multiplier, error_var, obs_cell, obs_dual, obs_var,
    level_gain, mean_depth, chain_decay,
):
    n = lax.axis_size("tm")
    size = lax.axis_size("lev")
    if n % 2 or size < 2 or size & (size - 1):
        raise ValueError("unsupported mesh")
    _, fields, levels, rows, cols = increment.shape
    planes = fields * levels
    chunks = planes * pieces(rows)
    rounds = size.bit_length() - 1
    tall = 2 * rows + PAD

    def room(*shape):
        return pltpu.VMEM(shape, jnp.float32)

    def flags(count):
        return pltpu.SemaphoreType.DMA((count,))

    scratch = Scratch(
        *[room(planes, rows + 2 * PAD, cols)] * 4,
        *[room(planes, rows, cols)] * 10,
        room(2, tall, cols), room(rounds, tall, cols), room(tall, cols),
        room(4, rows + 2 * PAD, cols), room(levels, rows, cols),
        room(planes, 1, 128), room(planes, 1, 128),
        *[flags(chunks)] * 15,
        flags(1), flags(1), flags(3 * planes), flags(rounds + 1), flags(rounds + 1),
    )
    state = jax.ShapeDtypeStruct(increment.shape, jnp.float32)
    place = pl.BlockSpec(memory_space=pl.ANY)
    small = pl.BlockSpec(memory_space=pltpu.VMEM)
    scalar = pl.BlockSpec(memory_space=pltpu.SMEM)
    return pl.pallas_call(
        functools.partial(kernel, n, size),
        out_shape=[state, jax.ShapeDtypeStruct(obs_dual.shape, jnp.float32), state, state],
        in_specs=[place] * 3 + [small] * 3 + [scalar] * 3,
        out_specs=[place, small, place, place],
        scratch_shapes=list(scratch),
        compiler_params=pltpu.CompilerParams(
            collective_id=0, has_side_effects=True, vmem_limit_bytes=63 * 1024 * 1024
        ),
    )(
        increment, multiplier, error_var, obs_cell, obs_dual, obs_var,
        level_gain, mean_depth, chain_decay,
    )


def solution(mesh):
    state = P("tm", None, "lev", None, None)
    obs = P("tm", "lev", None)
    return jax.shard_map(
        shards,
        mesh=mesh,
        in_specs=(state, state, state, obs, obs, obs, P("lev"), P("lev"), P("tm", None, "lev")),
        out_specs=(state, obs, state, state),
        check_vma=False,
    )
```

```python
import functools
from typing import Any, NamedTuple

import jax
import jax.numpy as jnp
from jax import lax
from jax.experimental import pallas as pl
from jax.experimental.pallas import tpu as pltpu
from jax.sharding import PartitionSpec as P

TIME_STEP = 0.25
ROTATION_PARAM = 0.5
COUPLING = 0.25
HALF = TIME_STEP * ROTATION_PARAM
SPLIT = 2
PAD = 8
MESH_ID = pl.DeviceIdType.MESH


class Scratch(NamedTuple):
    inc: Any
    mult: Any
    work: Any
    b1: Any
    own: Any
    swap: Any
    tangent: Any
    adjoint: Any
    sent: Any
    relay_t: Any
    relay_a: Any
    sums: Any
    met: Any
    total: Any
    columns: Any
    added: Any
    decay: Any
    decay_in: Any
    own_send: Any
    own_recv: Any
    tan_send: Any
    tan_recv: Any
    adj_send: Any
    adj_recv: Any
    rt_send: Any
    rt_recv: Any
    ra_send: Any
    ra_recv: Any
    ch_send: Any
    ch_recv: Any
    decay_send: Any
    decay_recv: Any
    loads: Any
    lev_send: Any
    lev_recv: Any


def pieces(rows):
    return SPLIT if rows % (8 * SPLIT) == 0 else 1


def block_rows(rows):
    part = rows // pieces(rows)
    return next(b for b in (32, 16, 8, part) if part % b == 0)


def up_y(a):
    lane = lax.broadcasted_iota(jnp.int32, a.shape, 1)
    return jnp.where(lane == a.shape[1] - 1, 0.0, pltpu.roll(a, a.shape[1] - 1, 1))


def down_y(a):
    lane = lax.broadcasted_iota(jnp.int32, a.shape, 1)
    return jnp.where(lane == 0, 0.0, pltpu.roll(a, 1, 1))


def up_x(a):
    return pltpu.roll(a, a.shape[0] - 1, 0)


def down_x(a):
    return pltpu.roll(a, 1, 0)


def kernel(
    n, size, increment, multiplier, error_var, obs_cell, obs_dual, obs_var, level_gain, mean_depth,
    chain_decay, tangent_in, obs_out, adjoint_in, carried, *scratch,
):
    b = Scratch(*scratch)
    fields, levels, rows, cols = increment.shape[1:]
    planes = fields * levels
    per = pieces(rows)
    chunks = planes * per
    part = rows // per
    step = block_rows(rows)
    wide = step + 2 * PAD

    s = lax.axis_index("tm")
    lev = lax.axis_index("lev")
    odd = s % 2
    even = odd == 0
    pair = s // 2
    pairs = n // 2
    partner = s + 1 - 2 * odd

    def adjoint_cut(k):
        return chunks * (pairs - 1 - k) // pairs

    def tangent_cut(k):
        return jnp.minimum(chunks, chunks * (k + 1) // pairs + 1)

    def loop(low, high, fn):
        lax.fori_loop(low, high, lambda c, z: (fn(c), z)[1], 0)

    def where_in(c):
        return c // per, pl.ds(pl.multiple_of((c % per) * part, 8), part)

    def piece(ref, c):
        p, r = where_in(c)
        return ref.at[p, r, :]

    def remote(src, dst, send, recv, where):
        return pltpu.make_async_remote_copy(
            src_ref=src, dst_ref=dst, send_sem=send, recv_sem=recv, device_id=where, device_id_type=MESH_ID,
        )

    def move(src, dst, send, recv, c, to):
        return remote(piece(src, c), piece(dst, c), send.at[c], recv.at[c], {"tm": to})

    def lev_move(src, dst, i, to):
        return remote(src, dst, b.lev_send.at[i], b.lev_recv.at[i], {"lev": to})

    def own_copy(c):
        return move(b.own, b.swap, b.own_send, b.own_recv, c, partner)

    def tangent_copy(c):
        return move(b.tangent, tangent_in, b.tan_send, b.tan_recv, c, s + 1)

    def adjoint_copy(c):
        return move(b.adjoint, adjoint_in, b.adj_send, b.adj_recv, c, s - 1)

    def chain_copy(c):
        return move(b.sent, carried, b.ch_send, b.ch_recv, c, s + 2)

    def tangent_leg(c, to):
        return move(b.tangent, b.relay_t, b.tan_send, b.rt_recv, c, to)

    def tangent_turn(c, to):
        return move(b.relay_t, tangent_in, b.rt_send, b.tan_recv, c, to)

    def adjoint_leg(c, to):
        return move(b.adjoint, b.relay_a, b.adj_send, b.ra_recv, c, to)

    def adjoint_turn(c, to):
        return move(b.relay_a, adjoint_in, b.ra_send, b.adj_recv, c, to)

    decay_copy = remote(b.decay, b.decay_in, b.decay_send.at[0], b.decay_recv.at[0], {"tm": s - 1})

    def load(i, p):
        src = (increment, multiplier, error_var)[i]
        dst = (b.inc, b.mult, b.work)[i]
        return pltpu.make_async_copy(
            src.at[0, p // levels, p % levels], dst.at[p, pl.ds(PAD, rows), :], b.loads.at[i * planes + p]
        )

    for p in range(planes):
        for i in range(3):
            load(i, p).start()

    barrier = pltpu.get_barrier_semaphore()
    near = ((s >= 1, s - 1), (s >= 2, s - 2), (s < n - 1, s + 1), (s < n - 2, s + 2))
    for there, who in near:
        @pl.when(there)
        def _():
            pl.semaphore_signal(barrier, inc=1, device_id={"tm": who}, device_id_type=MESH_ID)
    bits = []
    bit = 1
    while bit < size:
        bits.append(bit)
        bit *= 2

    def across(bit):
        return lev + bit - 2 * bit * ((lev // bit) % 2)

    for bit in bits:
        pl.semaphore_signal(barrier, inc=1, device_id={"lev": across(bit)}, device_id_type=MESH_ID)

    def edges(ref, planes):
        zero = jnp.zeros((PAD, cols), jnp.float32)
        for p in range(planes):
            ref[p, pl.ds(0, PAD), :] = zero
            ref[p, pl.ds(PAD + rows, PAD), :] = zero

    for ref in (b.inc, b.mult, b.work, b.b1):
        edges(ref, planes)
    edges(b.columns, 4)
    for f in range(fields):
        for l in range(levels):
            b.decay[f * levels + l] = jnp.full((1, 128), chain_decay[0, l, f], jnp.float32)

    def own_at(c):
        p, r = where_in(c)

        @pl.when(c % per == 0)
        def _():
            for i in range(3):
                load(i, p).wait()

        inner = pl.ds(pl.multiple_of((c % per) * part + PAD, 8), part)
        b.own[p, r, :] = b.work[p, inner, :] * b.mult[p, inner, :] + b.inc[p, inner, :]

    gives_own = jnp.logical_or(even, s < n - 1)

    def give_own(c):
        @pl.when(gives_own)
        def _():
            own_copy(c).start()

    with jax.named_scope("greet"):
        own_at(0)
        pl.semaphore_wait(barrier, len(bits) + sum(there.astype(jnp.int32) for there, _ in near))

    @pl.when(s >= 1)
    def _():
        decay_copy.start()

    def own_next(c):
        own_at(c)
        give_own(c - 1)

    with jax.named_scope("own"):
        loop(1, chunks, own_next)
        give_own(chunks - 1)

    def row_index(r0):
        return lax.broadcasted_iota(jnp.int32, (wide, cols), 0) + (r0 - PAD)

    def forward(h, u, v, column, r0, gain, depth):
        p = gain * h
        if column is not None:
            p = p + COUPLING * column
        u_new = u + TIME_STEP * (ROTATION_PARAM * v - (up_x(p) - p))
        v_new = v - TIME_STEP * (ROTATION_PARAM * u + (up_y(p) - p))
        u_new = jnp.where(row_index(r0) < 0, 0.0, u_new)
        h_new = h - TIME_STEP * depth * ((u_new - down_x(u_new)) + (v_new - down_y(v_new)))
        return h_new, u_new, v_new

    def back(h, u, v, r0, gain, depth):
        w = depth * h
        u2 = u + TIME_STEP * (up_x(w) - w)
        v2 = v + TIME_STEP * (up_y(w) - w)
        u2 = jnp.where(row_index(r0) < 0, 0.0, u2)
        p = TIME_STEP * ((u2 - down_x(u2)) + (v2 - down_y(v2)))
        return h + gain * p, u2 - HALF * v2, v2 + HALF * u2, p

    def middle(a):
        return a[PAD:PAD + step]

    def state_at(ref, l, r0):
        at = pl.ds(r0, wide)
        return ref[l, at, :], ref[levels + l, at, :], ref[2 * levels + l, at, :]

    def sweep(fn):
        loop(0, rows // step, lambda i: fn(pl.multiple_of(i * step, 8)))

    def put(ref, l, r0, values):
        for f, value in enumerate(values):
            ref[f * levels + l, pl.ds(r0, step), :] = middle(value)

    def put_padded(ref, l, r0, values):
        put(ref, l, r0 + PAD, values)

    sums = b.sums

    def ahead(r0):
        c0 = c1 = None
        for l in range(levels):
            h, u, v = state_at(b.inc, l, r0)
            h_new, _, _ = forward(h, u, v, None, r0, level_gain[l], mean_depth[l])
            c0 = middle(h) if c0 is None else c0 + middle(h)
            c1 = middle(h_new) if c1 is None else c1 + middle(h_new)
        sums[0, pl.ds(r0, step), :] = c0
        sums[0, pl.ds(rows + r0, step), :] = c1

    def behind(source, to):
        def fn(r0):
            bar = None
            for l in range(levels):
                h, u, v = state_at(source, l, r0)
                h2, u2, v2, p = back(h, u, v, r0, level_gain[l], mean_depth[l])
                if to == 0:
                    put_padded(b.b1, l, r0, (h2, u2, v2))
                bar = middle(p) if bar is None else bar + middle(p)
            sums[1, pl.ds(to * rows + r0, step), :] = COUPLING * bar
        return fn

    with jax.named_scope("ahead"):
        sweep(ahead)
    with jax.named_scope("behind"):
        sweep(behind(b.mult, 0))
        sweep(behind(b.b1, 1))
    depth_sum = mean_depth[0]
    for l in range(1, levels):
        depth_sum = depth_sum + mean_depth[l]
    for k in range(2):
        sums[k, pl.ds(2 * rows, PAD), :] = jnp.full((PAD, cols), depth_sum, jnp.float32)

    half = lev % 2
    tall = 2 * rows + PAD
    total = b.total

    def meet_copy():
        return lev_move(sums.at[1 - half], b.met.at[0], 0, across(1))

    def add_met(slot, first):
        def fn(r0):
            at = pl.ds(r0, PAD)
            kept = sums[half, at, :] if first else total[at, :]
            total[at, :] = kept + b.met[slot, at, :]
        loop(0, tall // PAD, lambda i: fn(pl.multiple_of(i * PAD, 8)))

    meet = meet_copy()
    with jax.named_scope("meet"):
        meet.start()
        meet.wait()
        add_met(0, True)

    def observe():
        count = obs_cell.shape[2]
        if cols & (cols - 1) == 0:
            shift = cols.bit_length() - 1

            def split(cells):
                return cells >> shift, cells & (cols - 1)
        else:
            def split(cells):
                return lax.div(cells, cols), lax.rem(cells, cols)

        row = lax.broadcasted_iota(jnp.int32, (rows, count), 0)
        col = lax.broadcasted_iota(jnp.int32, (cols, count), 0)
        for l in range(levels):
            at_row, at_col = split(obs_cell[0, pl.ds(l, 1), :])
            values = obs_dual[0, pl.ds(l, 1), :]
            hit_row = jnp.where(row == at_row, 1.0, 0.0)
            hit_col = jnp.where(col == at_col, 1.0, 0.0)
            seen = lax.dot_general(
                b.inc[l, pl.ds(PAD, rows), :], hit_col, (((1,), (0,)), ((), ())),
                precision=lax.Precision.HIGHEST, preferred_element_type=jnp.float32,
            )
            picked = jnp.sum(hit_row * seen, axis=0, keepdims=True)
            obs_out[0, pl.ds(l, 1), :] = obs_var[0, pl.ds(l, 1), :] * values + picked
            b.added[l] = lax.dot_general(
                hit_row * values, hit_col, (((1,), (1,)), ((), ())),
                precision=lax.Precision.HIGHEST, preferred_element_type=jnp.float32,
            )

    for i, bit in enumerate(bits[1:], 1):
        far = lev_move(total, b.met.at[i], i, across(bit))
        far.start()
        if i == 1:
            with jax.named_scope("observe"):
                observe()
        with jax.named_scope("far"):
            far.wait()
            add_met(i, False)
    if len(bits) < 2:
        observe()

    columns = b.columns

    def first_column(r0):
        columns[2 * half, pl.ds(r0 + PAD, step), :] = total[pl.ds(r0, step), :]

    def second_column(r0):
        c = columns[2 * half, pl.ds(r0, wide), :]
        gx = jnp.where(row_index(r0) < 0, 0.0, up_x(c) - c)
        gy = up_y(c) - c
        lap = (gx - down_x(gx)) + (gy - down_y(gy))
        scale = (TIME_STEP * TIME_STEP * COUPLING) * total[pl.ds(2 * rows, 1), pl.ds(0, 1)]
        columns[2 * half + 1, pl.ds(r0 + PAD, step), :] = total[pl.ds(rows + r0, step), :] + scale * middle(lap)

    with jax.named_scope("column"):
        sweep(first_column)
        sweep(second_column)
    mine = columns.at[pl.ds(2 * half, 2)]
    near_copy = lev_move(mine, mine, len(bits), across(1))
    with jax.named_scope("near"):
        near_copy.start()
        near_copy.wait()

    def last_back(r0):
        at = pl.ds(r0, wide)
        bar0, bar1 = columns[2, at, :], columns[3, at, :]
        for l in range(levels):
            h, u, v = state_at(b.b1, l, r0)
            h2, u2, v2, _ = back(h + bar0, u, v, r0, level_gain[l], mean_depth[l])
            put(b.adjoint, l, r0, (h2 + bar1, u2, v2))

    def first_forward(r0):
        column = columns[0, pl.ds(r0, wide), :]
        for l in range(levels):
            h, u, v = state_at(b.inc, l, r0)
            put_padded(b.work, l, r0, forward(h, u, v, column, r0, level_gain[l], mean_depth[l]))

    def last_forward(r0):
        column = columns[1, pl.ds(r0, wide), :]
        for l in range(levels):
            h, u, v = state_at(b.work, l, r0)
            put(b.tangent, l, r0, forward(h, u, v, column, r0, level_gain[l], mean_depth[l]))

    with jax.named_scope("back"):
        sweep(last_back)
    below = pair - 1
    down_cut = adjoint_cut(below)
    across_cut = adjoint_cut(pair)

    @pl.when(jnp.logical_and(even, s >= 2))
    def _():
        loop(0, down_cut, lambda c: adjoint_leg(c, s - 2).start())
        loop(down_cut, chunks, lambda c: adjoint_leg(c, s + 1).start())

    with jax.named_scope("forward"):
        sweep(first_forward)
        sweep(last_forward)
    up_cut = tangent_cut(pair)
    here_cut = tangent_cut(below)
    climbs = jnp.logical_and(odd == 1, s < n - 1)

    @pl.when(even)
    def _():
        loop(0, chunks, lambda c: tangent_copy(c).start())

    @pl.when(climbs)
    def _():
        loop(0, up_cut, lambda c: tangent_leg(c, s + 2).start())
        loop(up_cut, chunks, lambda c: tangent_leg(c, s - 1).start())

    @pl.when(s < n - 1)
    def _():
        decay_copy.wait_recv()

    def chain_step(c):
        p, r = where_in(c)
        d = chain_decay[0, p % levels, p // levels]

        @pl.when(s >= 1)
        def _():
            tangent_copy(c).wait_recv()

        @pl.when(s == 0)
        def _():
            tangent_in[p, r, :] = jnp.zeros((part, cols), jnp.float32)

        @pl.when(s >= 2)
        def _():
            chain_copy(c).wait_recv()

        @pl.when(s < 2)
        def _():
            carried[p, r, :] = jnp.zeros((part, cols), jnp.float32)

        @pl.when(jnp.logical_or(odd == 1, s < n - 2))
        def _():
            own_copy(c).wait_recv()

        swap = b.swap[p, r, :]
        product = b.own[p, r, :] - tangent_in[p, r, :]
        here = d * (carried[p, r, :] + jnp.where(odd == 1, swap, 0.0)) + product
        tangent_in[p, r, :] = product
        carried[p, r, :] = here

        @pl.when(s < n - 2)
        def _():
            d_next = b.decay_in[p][:, :1]
            b.sent[p, r, :] = d_next * here + (jnp.where(even, swap, 0.0) - b.tangent[p, r, :])
            chain_copy(c).start()

    with jax.named_scope("chain0"):
        loop(0, jnp.where(s == 0, chunks, 0), chain_step)

    @pl.when(jnp.logical_and(even, s < n - 2))
    def _():
        def turn_up(c):
            tangent_leg(c, s - 1).wait_recv()
            tangent_turn(c, s + 2).start()

        def turn_across(c):
            adjoint_leg(c, s - 2).wait_recv()
            adjoint_turn(c, s + 1).start()

        with jax.named_scope("turn_up"):
            loop(up_cut, chunks, turn_up)
        with jax.named_scope("turn_over"):
            loop(0, across_cut, turn_across)

    @pl.when(odd == 1)
    def _():
        @pl.when(s >= 3)
        def _():
            def turn_across(c):
                tangent_leg(c, s + 2).wait_recv()
                tangent_turn(c, s - 1).start()

            with jax.named_scope("turn_back"):
                loop(0, here_cut, turn_across)

        loop(0, chunks, lambda c: adjoint_copy(c).start())

        @pl.when(s >= 3)
        def _():
            def turn_down(c):
                adjoint_leg(c, s + 1).wait_recv()
                adjoint_turn(c, s - 2).start()

            with jax.named_scope("turn_down"):
                loop(down_cut, chunks, turn_down)

    with jax.named_scope("chain"):
        loop(0, jnp.where(s == 0, 0, chunks), chain_step)

    def block_step(i):
        c = lax.rem(i + across_cut * odd, chunks)
        p, r = where_in(c)
        inner = pl.ds(pl.multiple_of((c % per) * part + PAD, 8), part)

        @pl.when(s < n - 1)
        def _():
            adjoint_copy(c).wait_recv()

        kept = b.mult[p, inner, :] - jnp.where(s < n - 1, adjoint_in[p, r, :], 0.0)
        adjoint_in[p, r, :] = kept

        @pl.when(p < levels)
        def _():
            adjoint_in[p, r, :] = kept + b.added[jnp.minimum(p, levels - 1), r, :]

    with jax.named_scope("block"):
        loop(0, chunks, block_step)

    with jax.named_scope("drain"):
        @pl.when(gives_own)
        def _():
            loop(0, chunks, lambda c: own_copy(c).wait_send())

        @pl.when(s < n - 1)
        def _():
            loop(0, chunks, lambda c: tangent_copy(c).wait_send())

        @pl.when(s >= 1)
        def _():
            loop(0, chunks, lambda c: adjoint_copy(c).wait_send())
            decay_copy.wait_send()

        @pl.when(jnp.logical_and(even, s < n - 2))
        def _():
            loop(up_cut, chunks, lambda c: tangent_turn(c, s + 2).wait_send())
            loop(0, across_cut, lambda c: adjoint_turn(c, s + 1).wait_send())

        @pl.when(jnp.logical_and(odd == 1, s >= 3))
        def _():
            loop(0, here_cut, lambda c: tangent_turn(c, s - 1).wait_send())
            loop(down_cut, chunks, lambda c: adjoint_turn(c, s - 2).wait_send())

        @pl.when(s < n - 2)
        def _():
            loop(0, chunks, lambda c: chain_copy(c).wait_send())


def write_out(dual_in, seen_in, block_in, chain_in, dual, seen, block, chain, sems):
    planes = dual.shape[0]
    copies = [pltpu.make_async_copy(seen_in, seen, sems.at[3 * planes])]
    for i, (src, dst) in enumerate(((dual_in, dual), (block_in, block), (chain_in, chain))):
        for p in range(planes):
            copies.append(pltpu.make_async_copy(src.at[p], dst.at[p], sems.at[i * planes + p]))
    for copy in copies:
        copy.start()
    for copy in copies:
        copy.wait()


def shards(
    increment, multiplier, error_var, obs_cell, obs_dual, obs_var,
    level_gain, mean_depth, chain_decay,
):
    n = lax.axis_size("tm")
    size = lax.axis_size("lev")
    if n % 2 or size < 2 or size & (size - 1):
        raise ValueError("unsupported mesh")
    _, fields, levels, rows, cols = increment.shape
    planes = fields * levels
    chunks = planes * pieces(rows)
    rounds = size.bit_length() - 1
    tall = 2 * rows + PAD

    def room(*shape):
        return pltpu.VMEM(shape, jnp.float32)

    def flags(count):
        return pltpu.SemaphoreType.DMA((count,))

    scratch = Scratch(
        *[room(planes, rows + 2 * PAD, cols)] * 4,
        *[room(planes, rows, cols)] * 7,
        room(2, tall, cols), room(rounds, tall, cols), room(tall, cols),
        room(4, rows + 2 * PAD, cols), room(levels, rows, cols),
        room(planes, 1, 128), room(planes, 1, 128),
        *[flags(chunks)] * 12,
        flags(1), flags(1), flags(3 * planes), flags(rounds + 1), flags(rounds + 1),
    )
    place = pl.BlockSpec(memory_space=pl.ANY)
    small = pl.BlockSpec(memory_space=pltpu.VMEM)
    scalar = pl.BlockSpec(memory_space=pltpu.SMEM)
    held = pltpu.VMEM((planes, rows, cols), jnp.float32)
    results = pl.pallas_call(
        functools.partial(kernel, n, size),
        out_shape=[held, pltpu.VMEM(obs_dual.shape, jnp.float32), held, held],
        in_specs=[place] * 3 + [small] * 3 + [scalar] * 3,
        out_specs=[small] * 4,
        scratch_shapes=list(scratch),
        compiler_params=pltpu.CompilerParams(
            collective_id=0, has_side_effects=True, vmem_limit_bytes=50 * 1024 * 1024
        ),
    )(
        increment, multiplier, error_var, obs_cell, obs_dual, obs_var,
        level_gain, mean_depth, jnp.swapaxes(chain_decay, 1, 2),
    )
    dual, seen, block, chain = pl.pallas_call(
        write_out,
        out_shape=[jax.ShapeDtypeStruct(r.shape, jnp.float32) for r in results],
        in_specs=[small] * 4,
        out_specs=[place] * 4,
        scratch_shapes=[flags(3 * planes + 1)],
        compiler_params=pltpu.CompilerParams(vmem_limit_bytes=1024 * 1024),
    )(*[pltpu.with_memory_space_constraint(r, pltpu.VMEM) for r in results])
    return (
        dual.reshape(increment.shape), seen, block.reshape(increment.shape), chain.reshape(increment.shape),
    )


def solution(mesh):
    state = P("tm", None, "lev", None, None)
    obs = P("tm", "lev", None)
    return jax.shard_map(
        shards,
        mesh=mesh,
        in_specs=(state, state, state, obs, obs, obs, P("lev"), P("lev"), P("tm", None, "lev")),
        out_specs=(state, obs, state, state),
        check_vma=False,
    )
```

```python
import functools
from typing import Any, NamedTuple

import jax
import jax.numpy as jnp
from jax import lax
from jax.experimental import pallas as pl
from jax.experimental.pallas import tpu as pltpu
from jax.sharding import PartitionSpec as P

TIME_STEP = 0.25
ROTATION_PARAM = 0.5
COUPLING = 0.25
HALF = TIME_STEP * ROTATION_PARAM
SPLIT = 2
PAD = 8
MESH_ID = pl.DeviceIdType.MESH


class Scratch(NamedTuple):
    inc: Any
    mult: Any
    work: Any
    b1: Any
    own: Any
    swap: Any
    tangent: Any
    adjoint: Any
    sent: Any
    relay_t: Any
    relay_a: Any
    sums: Any
    met: Any
    total: Any
    columns: Any
    added: Any
    decay: Any
    decay_in: Any
    decay_relay: Any
    cells: Any
    obs_dual: Any
    obs_var: Any
    gain: Any
    depth: Any
    chain_decay: Any
    sends: Any
    own_recv: Any
    loads: Any
    tan_recv: Any
    adj_recv: Any
    rt_send: Any
    rt_recv: Any
    ra_send: Any
    ra_recv: Any
    ch_recv: Any
    decay_send: Any
    decay_recv: Any
    small_loads: Any
    lev_send: Any
    lev_recv: Any


def pieces(rows):
    return SPLIT if rows % (8 * SPLIT) == 0 else 1


def block_rows(rows):
    part = rows // pieces(rows)
    return next(b for b in (32, 16, 8, part) if part % b == 0)


def up_y(a):
    lane = lax.broadcasted_iota(jnp.int32, a.shape, 1)
    return jnp.where(lane == a.shape[1] - 1, 0.0, pltpu.roll(a, a.shape[1] - 1, 1))


def down_y(a):
    lane = lax.broadcasted_iota(jnp.int32, a.shape, 1)
    return jnp.where(lane == 0, 0.0, pltpu.roll(a, 1, 1))


def up_x(a):
    return pltpu.roll(a, a.shape[0] - 1, 0)


def down_x(a):
    return pltpu.roll(a, 1, 0)


def kernel(
    n, size, increment, multiplier, error_var, cell_at, obs_dual_at, obs_var_at, gain_at, depth_at,
    decay_at, tangent_in, obs_out, adjoint_in, carried, *scratch,
):
    b = Scratch(*scratch)
    obs_cell, obs_dual, obs_var = b.cells, b.obs_dual, b.obs_var
    level_gain, mean_depth, chain_decay = b.gain, b.depth, b.chain_decay
    fields, levels, rows, cols = increment.shape[1:]
    planes = fields * levels
    per = pieces(rows)
    chunks = planes * per
    part = rows // per
    step = block_rows(rows)
    wide = step + 2 * PAD

    s = lax.axis_index("tm")
    lev = lax.axis_index("lev")
    odd = s % 2
    even = odd == 0
    pair = s // 2
    pairs = n // 2
    partner = s + 1 - 2 * odd

    def adjoint_cut(k):
        return chunks * (pairs - 1 - k) // pairs

    def tangent_cut(k):
        return jnp.minimum(chunks, chunks * (k + 1) // max(pairs - 1, 1))

    def loop(low, high, fn):
        lax.fori_loop(low, high, lambda c, z: (fn(c), z)[1], 0)

    def where_in(c):
        return c // per, pl.ds(pl.multiple_of((c % per) * part, 8), part)

    def piece(ref, c):
        p, r = where_in(c)
        return ref.at[p, r, :]

    def remote(src, dst, send, recv, where):
        return pltpu.make_async_remote_copy(
            src_ref=src, dst_ref=dst, send_sem=send, recv_sem=recv, device_id=where, device_id_type=MESH_ID,
        )

    def move(src, dst, send, recv, c, to):
        return remote(piece(src, c), piece(dst, c), send, recv.at[c], {"tm": to})

    def lev_move(src, dst, i, to):
        return remote(src, dst, b.lev_send.at[i], b.lev_recv.at[i], {"lev": to})

    def own_copy(c):
        return remote(piece(b.own, c), piece(b.swap, c), b.sends.at[0], b.own_recv.at[c // per], {"tm": partner})

    def own_plane(p):
        return remote(b.own.at[p], b.swap.at[p], b.sends.at[0], b.own_recv.at[p], {"tm": partner})

    def all_sent(src, dst, i):
        remote(src, dst, b.sends.at[i], b.own_recv.at[0], {"tm": partner}).wait_send()

    def tangent_copy(c):
        return move(b.tangent, tangent_in, b.sends.at[1], b.tan_recv, c, s + 1)

    def adjoint_copy(c):
        return move(b.adjoint, adjoint_in, b.sends.at[2], b.adj_recv, c, s - 1)

    def chain_copy(c):
        return move(b.sent, carried, b.sends.at[3], b.ch_recv, c, s + 2)

    def tangent_leg(c, to):
        return move(b.tangent, b.relay_t, b.sends.at[1], b.rt_recv, c, to)

    def tangent_turn(c, to):
        return move(b.relay_t, tangent_in, b.rt_send.at[c], b.tan_recv, c, to)

    def adjoint_leg(c, to):
        return move(b.adjoint, b.relay_a, b.sends.at[2], b.ra_recv, c, to)

    def adjoint_turn(c, to):
        return move(b.relay_a, adjoint_in, b.ra_send.at[c], b.adj_recv, c, to)

    decay_copy = remote(b.decay, b.decay_in, b.decay_send.at[0], b.decay_recv.at[0], {"tm": s - 1})
    decay_leg = remote(b.decay, b.decay_relay, b.decay_send.at[0], b.decay_recv.at[1], {"tm": s - 2})
    decay_turn = remote(b.decay_relay, b.decay_in, b.decay_send.at[1], b.decay_recv.at[0], {"tm": s + 1})
    turns = jnp.logical_and(even, s < n - 2)

    def load(i, p):
        src = (increment, multiplier, error_var)[i]
        dst = (b.inc, b.mult, b.work)[i]
        return pltpu.make_async_copy(
            src.at[0, p // levels, p % levels], dst.at[p, pl.ds(PAD, rows), :], b.loads.at[p]
        )

    barrier = pltpu.get_barrier_semaphore()
    near = ((s >= 0, partner), (s >= 2, s - 2), (s < n - 2, s + 2))
    for there, who in near:
        @pl.when(there)
        def _():
            pl.semaphore_signal(barrier, inc=1, device_id={"tm": who}, device_id_type=MESH_ID)
    bits = []
    bit = 1
    while bit < size:
        bits.append(bit)
        bit *= 2

    def across(bit):
        return lev + bit - 2 * bit * ((lev // bit) % 2)

    for bit in bits:
        pl.semaphore_signal(barrier, inc=1, device_id={"lev": across(bit)}, device_id_type=MESH_ID)

    small_loads = [
        pltpu.make_async_copy(src, dst, b.small_loads.at[i])
        for i, (src, dst) in enumerate((
            (decay_at, chain_decay), (gain_at, level_gain), (depth_at, mean_depth),
            (cell_at, obs_cell), (obs_dual_at, obs_dual), (obs_var_at, obs_var),
        ))
    ]
    small_loads[0].start()
    for p in range(planes):
        for i in range(3):
            load(i, p).start()
    for copy in small_loads[1:]:
        copy.start()

    def edges(ref, planes):
        zero = jnp.zeros((PAD, cols), jnp.float32)
        for p in range(planes):
            ref[p, pl.ds(0, PAD), :] = zero
            ref[p, pl.ds(PAD + rows, PAD), :] = zero

    def own_at(c):
        p, r = where_in(c)

        @pl.when(c % per == 0)
        def _():
            pltpu.make_async_copy(
                increment.at[0, :, 0], b.inc.at[pl.ds(0, fields), pl.ds(PAD, rows), :], b.loads.at[p]
            ).wait()

        inner = pl.ds(pl.multiple_of((c % per) * part + PAD, 8), part)
        b.own[p, r, :] = b.work[p, inner, :] * b.mult[p, inner, :] + b.inc[p, inner, :]

    gives_own = jnp.logical_or(even, s < n - 1)

    def give_own(c):
        @pl.when(gives_own)
        def _():
            own_copy(c).start()

    with jax.named_scope("greet"):
        small_loads[0].wait()
        for f in range(fields):
            for l in range(levels):
                b.decay[f * levels + l] = jnp.full((1, 128), chain_decay[0, l, f], jnp.float32)
        own_at(0)
        pl.semaphore_wait(barrier, len(bits) + sum(there.astype(jnp.int32) for there, _ in near))

        @pl.when(odd == 1)
        def _():
            decay_copy.start()

        @pl.when(jnp.logical_and(even, s >= 2))
        def _():
            decay_leg.start()

    def own_next(c):
        own_at(c)
        give_own(c - 1)

    with jax.named_scope("own"):
        loop(1, chunks, own_next)
        give_own(chunks - 1)

    for copy in small_loads[1:]:
        copy.wait()
    for ref in (b.inc, b.mult, b.work, b.b1):
        edges(ref, planes)
    edges(b.columns, 4)

    def row_index(r0):
        return lax.broadcasted_iota(jnp.int32, (wide, cols), 0) + (r0 - PAD)

    def forward(h, u, v, column, r0, gain, depth):
        p = gain * h
        if column is not None:
            p = p + COUPLING * column
        u_new = u + TIME_STEP * (ROTATION_PARAM * v - (up_x(p) - p))
        v_new = v - TIME_STEP * (ROTATION_PARAM * u + (up_y(p) - p))
        u_new = jnp.where(row_index(r0) < 0, 0.0, u_new)
        h_new = h - TIME_STEP * depth * ((u_new - down_x(u_new)) + (v_new - down_y(v_new)))
        return h_new, u_new, v_new

    def back(h, u, v, r0, gain, depth):
        w = depth * h
        u2 = u + TIME_STEP * (up_x(w) - w)
        v2 = v + TIME_STEP * (up_y(w) - w)
        u2 = jnp.where(row_index(r0) < 0, 0.0, u2)
        p = TIME_STEP * ((u2 - down_x(u2)) + (v2 - down_y(v2)))
        return h + gain * p, u2 - HALF * v2, v2 + HALF * u2, p

    def middle(a):
        return a[PAD:PAD + step]

    def state_at(ref, l, r0):
        at = pl.ds(r0, wide)
        return ref[l, at, :], ref[levels + l, at, :], ref[2 * levels + l, at, :]

    def sweep(fn):
        loop(0, rows // step, lambda i: fn(pl.multiple_of(i * step, 8)))

    def put(ref, l, r0, values):
        for f, value in enumerate(values):
            ref[f * levels + l, pl.ds(r0, step), :] = middle(value)

    def put_padded(ref, l, r0, values):
        put(ref, l, r0 + PAD, values)

    sums = b.sums

    def ahead(r0):
        c0 = c1 = None
        for l in range(levels):
            h, u, v = state_at(b.inc, l, r0)
            h_new, _, _ = forward(h, u, v, None, r0, level_gain[l], mean_depth[l])
            c0 = middle(h) if c0 is None else c0 + middle(h)
            c1 = middle(h_new) if c1 is None else c1 + middle(h_new)
        sums[0, pl.ds(r0, step), :] = c0
        sums[0, pl.ds(rows + r0, step), :] = c1

    def behind(source, to):
        def fn(r0):
            bar = None
            for l in range(levels):
                h, u, v = state_at(source, l, r0)
                h2, u2, v2, p = back(h, u, v, r0, level_gain[l], mean_depth[l])
                if to == 0:
                    put_padded(b.b1, l, r0, (h2, u2, v2))
                bar = middle(p) if bar is None else bar + middle(p)
            sums[1, pl.ds(to * rows + r0, step), :] = COUPLING * bar
        return fn

    with jax.named_scope("ahead"):
        sweep(ahead)
    with jax.named_scope("behind"):
        sweep(behind(b.mult, 0))
        sweep(behind(b.b1, 1))
    depth_sum = mean_depth[0]
    for l in range(1, levels):
        depth_sum = depth_sum + mean_depth[l]
    for k in range(2):
        sums[k, pl.ds(2 * rows, PAD), :] = jnp.full((PAD, cols), depth_sum, jnp.float32)

    half = lev % 2
    tall = 2 * rows + PAD
    total = b.total

    def meet_copy():
        return lev_move(sums.at[1 - half], b.met.at[0], 0, across(1))

    def add_met(slot, first):
        def fn(r0):
            at = pl.ds(r0, PAD)
            kept = sums[half, at, :] if first else total[at, :]
            total[at, :] = kept + b.met[slot, at, :]
        loop(0, tall // PAD, lambda i: fn(pl.multiple_of(i * PAD, 8)))

    meet = meet_copy()
    with jax.named_scope("meet"):
        meet.start()
        meet.wait()
        add_met(0, True)

    def observe():
        count = obs_cell.shape[2]
        if cols & (cols - 1) == 0:
            shift = cols.bit_length() - 1

            def split(cells):
                return cells >> shift, cells & (cols - 1)
        else:
            def split(cells):
                return lax.div(cells, cols), lax.rem(cells, cols)

        row = lax.broadcasted_iota(jnp.int32, (rows, count), 0)
        col = lax.broadcasted_iota(jnp.int32, (cols, count), 0)
        for l in range(levels):
            at_row, at_col = split(obs_cell[0, pl.ds(l, 1), :])
            values = obs_dual[0, pl.ds(l, 1), :]
            hit_row = jnp.where(row == at_row, 1.0, 0.0)
            hit_col = jnp.where(col == at_col, 1.0, 0.0)
            seen = lax.dot_general(
                b.inc[l, pl.ds(PAD, rows), :], hit_col, (((1,), (0,)), ((), ())),
                precision=lax.Precision.HIGHEST, preferred_element_type=jnp.float32,
            )
            picked = jnp.sum(hit_row * seen, axis=0, keepdims=True)
            obs_out[0, pl.ds(l, 1), :] = obs_var[0, pl.ds(l, 1), :] * values + picked
            b.added[l] = lax.dot_general(
                hit_row * values, hit_col, (((1,), (1,)), ((), ())),
                precision=lax.Precision.HIGHEST, preferred_element_type=jnp.float32,
            )

    for i, bit in enumerate(bits[1:], 1):
        far = lev_move(total, b.met.at[i], i, across(bit))
        far.start()
        if i == 1:
            with jax.named_scope("observe"):
                observe()
        with jax.named_scope("far"):
            far.wait()
            add_met(i, False)
    if len(bits) < 2:
        observe()

    columns = b.columns

    def first_column(r0):
        columns[2 * half, pl.ds(r0 + PAD, step), :] = total[pl.ds(r0, step), :]

    def second_column(r0):
        c = columns[2 * half, pl.ds(r0, wide), :]
        gx = jnp.where(row_index(r0) < 0, 0.0, up_x(c) - c)
        gy = up_y(c) - c
        lap = (gx - down_x(gx)) + (gy - down_y(gy))
        scale = (TIME_STEP * TIME_STEP * COUPLING) * total[pl.ds(2 * rows, 1), pl.ds(0, 1)]
        columns[2 * half + 1, pl.ds(r0 + PAD, step), :] = total[pl.ds(rows + r0, step), :] + scale * middle(lap)

    with jax.named_scope("column"):
        sweep(first_column)
        sweep(second_column)
    mine = columns.at[pl.ds(2 * half, 2)]
    near_copy = lev_move(mine, mine, len(bits), across(1))
    with jax.named_scope("near"):
        near_copy.start()
        near_copy.wait()

    def last_back(r0):
        at = pl.ds(r0, wide)
        bar0, bar1 = columns[2, at, :], columns[3, at, :]
        for l in range(levels):
            h, u, v = state_at(b.b1, l, r0)
            h2, u2, v2, _ = back(h + bar0, u, v, r0, level_gain[l], mean_depth[l])
            put(b.adjoint, l, r0, (h2 + bar1, u2, v2))

    def first_forward(r0):
        column = columns[0, pl.ds(r0, wide), :]
        for l in range(levels):
            h, u, v = state_at(b.inc, l, r0)
            put_padded(b.work, l, r0, forward(h, u, v, column, r0, level_gain[l], mean_depth[l]))

    def last_forward(r0):
        column = columns[1, pl.ds(r0, wide), :]
        for l in range(levels):
            h, u, v = state_at(b.work, l, r0)
            put(b.tangent, l, r0, forward(h, u, v, column, r0, level_gain[l], mean_depth[l]))

    @pl.when(turns)
    def _():
        decay_leg.wait_recv()
        decay_turn.start()

    with jax.named_scope("back"):
        sweep(last_back)
    below = pair - 1
    down_cut = adjoint_cut(below)
    across_cut = adjoint_cut(pair)

    @pl.when(jnp.logical_and(even, s >= 2))
    def _():
        loop(0, down_cut, lambda c: adjoint_leg(c, s - 2).start())
        loop(down_cut, chunks, lambda c: adjoint_leg(c, s + 1).start())

    with jax.named_scope("forward"):
        sweep(first_forward)
        sweep(last_forward)
    up_cut = tangent_cut(pair)
    here_cut = tangent_cut(below)
    climbs = jnp.logical_and(odd == 1, s < n - 1)

    @pl.when(even)
    def _():
        loop(0, chunks, lambda c: tangent_copy(c).start())

    @pl.when(climbs)
    def _():
        loop(0, up_cut, lambda c: tangent_leg(c, s + 2).start())
        loop(up_cut, chunks, lambda c: tangent_leg(c, s - 1).start())

    def chain_step(c):
        p, r = where_in(c)
        d = chain_decay[0, p % levels, p // levels]

        @pl.when(s >= 1)
        def _():
            tangent_copy(c).wait_recv()

        @pl.when(s == 0)
        def _():
            tangent_in[p, r, :] = jnp.zeros((part, cols), jnp.float32)

        @pl.when(s >= 2)
        def _():
            chain_copy(c).wait_recv()

        @pl.when(s < 2)
        def _():
            carried[p, r, :] = jnp.zeros((part, cols), jnp.float32)

        @pl.when(jnp.logical_and(c % per == 0, jnp.logical_or(odd == 1, s < n - 2)))
        def _():
            own_plane(p).wait_recv()

        swap = b.swap[p, r, :]
        product = b.own[p, r, :] - tangent_in[p, r, :]
        here = d * (carried[p, r, :] + jnp.where(odd == 1, swap, 0.0)) + product
        tangent_in[p, r, :] = product
        carried[p, r, :] = here

        @pl.when(s < n - 2)
        def _():
            d_next = b.decay_in[p][:, :1]
            b.sent[p, r, :] = d_next * here + (jnp.where(even, swap, 0.0) - b.tangent[p, r, :])
            chain_copy(c).start()

    @pl.when(s == 0)
    def _():
        decay_copy.wait_recv()

    with jax.named_scope("chain0"):
        loop(0, jnp.where(s == 0, chunks, 0), chain_step)

    @pl.when(jnp.logical_and(even, s < n - 2))
    def _():
        def turn_up(c):
            tangent_leg(c, s - 1).wait_recv()
            tangent_turn(c, s + 2).start()

        def turn_across(c):
            adjoint_leg(c, s - 2).wait_recv()
            adjoint_turn(c, s + 1).start()

        with jax.named_scope("turn_up"):
            loop(up_cut, chunks, turn_up)
        with jax.named_scope("turn_over"):
            loop(0, across_cut, turn_across)

    early = jnp.where(s == n - 1, chunks // 2, 0)

    @pl.when(odd == 1)
    def _():
        loop(0, early, lambda c: adjoint_copy(c).start())

        @pl.when(s >= 3)
        def _():
            def turn_across(c):
                tangent_leg(c, s + 2).wait_recv()
                tangent_turn(c, s - 1).start()

            with jax.named_scope("turn_back"):
                loop(0, here_cut, turn_across)

        loop(early, chunks, lambda c: adjoint_copy(c).start())

        @pl.when(s >= 3)
        def _():
            def turn_down(c):
                adjoint_leg(c, s + 1).wait_recv()
                adjoint_turn(c, s - 2).start()

            with jax.named_scope("turn_down"):
                loop(down_cut, chunks, turn_down)

    def block_step(i):
        c = lax.rem(i + across_cut * odd, chunks)
        p, r = where_in(c)
        inner = pl.ds(pl.multiple_of((c % per) * part + PAD, 8), part)

        @pl.when(s < n - 1)
        def _():
            adjoint_copy(c).wait_recv()

        kept = b.mult[p, inner, :] - jnp.where(s < n - 1, adjoint_in[p, r, :], 0.0)
        adjoint_in[p, r, :] = kept

        @pl.when(p < levels)
        def _():
            adjoint_in[p, r, :] = kept + b.added[jnp.minimum(p, levels - 1), r, :]

    loop(0, jnp.where(s == n - 1, chunks, 0), block_step)

    @pl.when(jnp.logical_and(s > 0, s < n - 1))
    def _():
        decay_copy.wait_recv()

    with jax.named_scope("chain"):
        loop(0, jnp.where(s == 0, 0, chunks), chain_step)

    with jax.named_scope("block"):
        loop(0, jnp.where(s == n - 1, 0, chunks), block_step)

    with jax.named_scope("drain"):
        @pl.when(gives_own)
        def _():
            all_sent(b.own, b.swap, 0)

        @pl.when(s < n - 1)
        def _():
            all_sent(b.tangent, tangent_in, 1)

        @pl.when(s >= 1)
        def _():
            all_sent(b.adjoint, adjoint_in, 2)
            decay_copy.wait_send()

        @pl.when(turns)
        def _():
            decay_turn.wait_send()

        @pl.when(jnp.logical_and(even, s < n - 2))
        def _():
            loop(up_cut, chunks, lambda c: tangent_turn(c, s + 2).wait_send())
            loop(0, across_cut, lambda c: adjoint_turn(c, s + 1).wait_send())

        @pl.when(jnp.logical_and(odd == 1, s >= 3))
        def _():
            loop(0, here_cut, lambda c: tangent_turn(c, s - 1).wait_send())
            loop(down_cut, chunks, lambda c: adjoint_turn(c, s - 2).wait_send())

        @pl.when(s < n - 2)
        def _():
            all_sent(b.sent, carried, 3)


def write_out(dual_in, seen_in, block_in, chain_in, dual, seen, block, chain, sems):
    copies = [
        pltpu.make_async_copy(src, dst, sems.at[i])
        for i, (src, dst) in enumerate(((dual_in, dual), (block_in, block), (chain_in, chain), (seen_in, seen)))
    ]
    for copy in copies:
        copy.start()
    for copy in copies:
        copy.wait()


def shards(
    increment, multiplier, error_var, obs_cell, obs_dual, obs_var,
    level_gain, mean_depth, chain_decay,
):
    n = lax.axis_size("tm")
    size = lax.axis_size("lev")
    if n % 2 or size < 2 or size & (size - 1):
        raise ValueError("unsupported mesh")
    _, fields, levels, rows, cols = increment.shape
    planes = fields * levels
    chunks = planes * pieces(rows)
    rounds = size.bit_length() - 1
    tall = 2 * rows + PAD

    def room(*shape):
        return pltpu.VMEM(shape, jnp.float32)

    def flags(count):
        return pltpu.SemaphoreType.DMA((count,))

    scratch = Scratch(
        *[room(planes, rows + 2 * PAD, cols)] * 4,
        *[room(planes, rows, cols)] * 7,
        room(2, tall, cols), room(rounds, tall, cols), room(tall, cols),
        room(4, rows + 2 * PAD, cols), room(levels, rows, cols),
        *[room(planes, 1, 128)] * 3,
        pltpu.VMEM(obs_cell.shape, jnp.int32), room(*obs_dual.shape), room(*obs_var.shape),
        pltpu.SMEM(level_gain.shape, jnp.float32), pltpu.SMEM(mean_depth.shape, jnp.float32),
        pltpu.SMEM((1, levels, fields), jnp.float32),
        flags(4), *[flags(planes)] * 2, *[flags(chunks)] * 7,
        flags(2), flags(2), flags(6), flags(rounds + 1), flags(rounds + 1),
    )
    place = pl.BlockSpec(memory_space=pl.ANY)
    small = pl.BlockSpec(memory_space=pltpu.VMEM)
    held = pltpu.VMEM((planes, rows, cols), jnp.float32)
    results = pl.pallas_call(
        functools.partial(kernel, n, size),
        out_shape=[held, pltpu.VMEM(obs_dual.shape, jnp.float32), held, held],
        in_specs=[place] * 9,
        out_specs=[small] * 4,
        scratch_shapes=list(scratch),
        compiler_params=pltpu.CompilerParams(
            collective_id=0, has_side_effects=True, vmem_limit_bytes=50 * 1024 * 1024
        ),
    )(
        increment, multiplier, error_var, obs_cell, obs_dual, obs_var,
        level_gain, mean_depth, jnp.swapaxes(chain_decay, 1, 2),
    )
    dual, seen, block, chain = pl.pallas_call(
        write_out,
        out_shape=[jax.ShapeDtypeStruct(r.shape, jnp.float32) for r in results],
        in_specs=[small] * 4,
        out_specs=[place] * 4,
        scratch_shapes=[flags(4)],
        compiler_params=pltpu.CompilerParams(vmem_limit_bytes=1024 * 1024),
    )(*[pltpu.with_memory_space_constraint(r, pltpu.VMEM) for r in results])
    return (
        dual.reshape(increment.shape), seen, block.reshape(increment.shape), chain.reshape(increment.shape),
    )


def solution(mesh):
    state = P("tm", None, "lev", None, None)
    obs = P("tm", "lev", None)
    return jax.shard_map(
        shards,
        mesh=mesh,
        in_specs=(state, state, state, obs, obs, obs, P("lev"), P("lev"), P("tm", None, "lev")),
        out_specs=(state, obs, state, state),
        check_vma=False,
    )
```

```python
import functools
from typing import Any, NamedTuple

import jax
import jax.numpy as jnp
from jax import lax
from jax.experimental import pallas as pl
from jax.experimental.pallas import tpu as pltpu
from jax.sharding import PartitionSpec as P

TIME_STEP = 0.25
ROTATION_PARAM = 0.5
COUPLING = 0.25
HALF = TIME_STEP * ROTATION_PARAM
SPLIT = 2
PAD = 8
MESH_ID = pl.DeviceIdType.MESH


class Scratch(NamedTuple):
    inc: Any
    mult: Any
    work: Any
    b1: Any
    own: Any
    swap: Any
    tangent: Any
    adjoint: Any
    sent: Any
    relay_t: Any
    relay_a: Any
    sums: Any
    met: Any
    total: Any
    columns: Any
    added: Any
    decay: Any
    decay_in: Any
    decay_relay: Any
    cells: Any
    obs_dual: Any
    obs_var: Any
    gain: Any
    depth: Any
    chain_decay: Any
    sends: Any
    own_recv: Any
    loads: Any
    tan_recv: Any
    adj_recv: Any
    rt_recv: Any
    ra_recv: Any
    ch_recv: Any
    decay_send: Any
    decay_recv: Any
    small_loads: Any
    lev_send: Any
    lev_recv: Any


def pieces(rows):
    return SPLIT if rows % (8 * SPLIT) == 0 else 1


def block_rows(rows):
    part = rows // pieces(rows)
    return next(b for b in (32, 16, 8, part) if part % b == 0)


def up_y(a):
    lane = lax.broadcasted_iota(jnp.int32, a.shape, 1)
    return jnp.where(lane == a.shape[1] - 1, 0.0, pltpu.roll(a, a.shape[1] - 1, 1))


def down_y(a):
    lane = lax.broadcasted_iota(jnp.int32, a.shape, 1)
    return jnp.where(lane == 0, 0.0, pltpu.roll(a, 1, 1))


def up_x(a):
    return pltpu.roll(a, a.shape[0] - 1, 0)


def down_x(a):
    return pltpu.roll(a, 1, 0)


def kernel(
    n, size, increment, multiplier, error_var, cell_at, obs_dual_at, obs_var_at, gain_at, depth_at,
    decay_at, tangent_in, obs_out, adjoint_in, carried, *scratch,
):
    b = Scratch(*scratch)
    obs_cell, obs_dual, obs_var = b.cells, b.obs_dual, b.obs_var
    level_gain, mean_depth, chain_decay = b.gain, b.depth, b.chain_decay
    fields, levels, rows, cols = increment.shape[1:]
    planes = fields * levels
    per = pieces(rows)
    chunks = planes * per
    part = rows // per
    step = block_rows(rows)
    wide = step + 2 * PAD

    s = lax.axis_index("tm")
    lev = lax.axis_index("lev")
    odd = s % 2
    even = odd == 0
    pair = s // 2
    pairs = n // 2
    partner = s + 1 - 2 * odd

    def adjoint_cut(k):
        return chunks * (pairs - 1 - k) // pairs

    def tangent_cut(k):
        return chunks * (k + 1) // max(pairs - 1, 1)

    def loop(low, high, fn):
        lax.fori_loop(low, high, lambda c, z: (fn(c), z)[1], 0)

    def where_in(c):
        return c // per, pl.ds(pl.multiple_of((c % per) * part, 8), part)

    def piece(ref, c):
        p, r = where_in(c)
        return ref.at[p, r, :]

    def remote(src, dst, send, recv, where):
        return pltpu.make_async_remote_copy(
            src_ref=src, dst_ref=dst, send_sem=send, recv_sem=recv, device_id=where, device_id_type=MESH_ID,
        )

    def move(src, dst, send, recv, c, to):
        return remote(piece(src, c), piece(dst, c), send, recv.at[c], {"tm": to})

    def lev_move(src, dst, i, to):
        return remote(src, dst, b.lev_send.at[i], b.lev_recv.at[i], {"lev": to})

    def own_copy(c):
        return remote(piece(b.own, c), piece(b.swap, c), b.sends.at[0], b.own_recv.at[c // per], {"tm": partner})

    def own_plane(p):
        return remote(b.own.at[p], b.swap.at[p], b.sends.at[0], b.own_recv.at[p], {"tm": partner})

    def all_sent(src, dst, i):
        remote(src, dst, b.sends.at[i], b.own_recv.at[0], {"tm": partner}).wait_send()

    def tangent_copy(c):
        return move(b.tangent, tangent_in, b.sends.at[1], b.tan_recv, c, s + 1)

    def adjoint_copy(c):
        return move(b.adjoint, adjoint_in, b.sends.at[2], b.adj_recv, c, s - 1)

    def chain_copy(c):
        return move(b.sent, carried, b.sends.at[3], b.ch_recv, c, s + 2)

    def tangent_leg(c, to):
        return remote(piece(b.tangent, c), b.relay_t.at[c], b.sends.at[1], b.rt_recv.at[c], {"tm": to})

    def tangent_turn(c, to):
        return remote(b.relay_t.at[c], piece(tangent_in, c), b.sends.at[4], b.tan_recv.at[c], {"tm": to})

    def adjoint_leg(c, to):
        return remote(piece(b.adjoint, c), b.relay_a.at[c], b.sends.at[2], b.ra_recv.at[c], {"tm": to})

    def adjoint_turn(c, to):
        return remote(b.relay_a.at[c], piece(adjoint_in, c), b.sends.at[5], b.adj_recv.at[c], {"tm": to})

    decay_copy = remote(b.decay, b.decay_in, b.decay_send.at[0], b.decay_recv.at[0], {"tm": s - 1})
    decay_leg = remote(b.decay, b.decay_relay, b.decay_send.at[0], b.decay_recv.at[1], {"tm": s - 2})
    decay_turn = remote(b.decay_relay, b.decay_in, b.decay_send.at[1], b.decay_recv.at[0], {"tm": s + 1})
    turns = jnp.logical_and(even, s < n - 2)

    def load(i, p):
        src = (increment, multiplier, error_var)[i]
        dst = (b.inc, b.mult, b.work)[i]
        return pltpu.make_async_copy(
            src.at[0, p // levels, p % levels], dst.at[p, pl.ds(PAD, rows), :], b.loads.at[p]
        )

    barrier = pltpu.get_barrier_semaphore()
    near = ((s >= 0, partner), (s >= 2, s - 2), (s < n - 2, s + 2))
    for there, who in near:
        @pl.when(there)
        def _():
            pl.semaphore_signal(barrier, inc=1, device_id={"tm": who}, device_id_type=MESH_ID)
    bits = []
    bit = 1
    while bit < size:
        bits.append(bit)
        bit *= 2

    def across(bit):
        return lev + bit - 2 * bit * ((lev // bit) % 2)

    for bit in bits:
        pl.semaphore_signal(barrier, inc=1, device_id={"lev": across(bit)}, device_id_type=MESH_ID)

    small_loads = [
        pltpu.make_async_copy(src, dst, b.small_loads.at[i])
        for i, (src, dst) in enumerate((
            (decay_at, chain_decay), (gain_at, level_gain), (depth_at, mean_depth),
            (cell_at, obs_cell), (obs_dual_at, obs_dual), (obs_var_at, obs_var),
        ))
    ]
    small_loads[0].start()
    for p in range(planes):
        for i in range(3):
            load(i, p).start()
    for copy in small_loads[1:]:
        copy.start()

    def edges(ref, planes):
        zero = jnp.zeros((PAD, cols), jnp.float32)
        for p in range(planes):
            ref[p, pl.ds(0, PAD), :] = zero
            ref[p, pl.ds(PAD + rows, PAD), :] = zero

    def own_at(c):
        p, r = where_in(c)

        @pl.when(c % per == 0)
        def _():
            pltpu.make_async_copy(
                increment.at[0, :, 0], b.inc.at[pl.ds(0, fields), pl.ds(PAD, rows), :], b.loads.at[p]
            ).wait()

        inner = pl.ds(pl.multiple_of((c % per) * part + PAD, 8), part)
        b.own[p, r, :] = b.work[p, inner, :] * b.mult[p, inner, :] + b.inc[p, inner, :]

    gives_own = jnp.logical_or(even, s < n - 1)

    def give_own(c):
        @pl.when(gives_own)
        def _():
            own_copy(c).start()

    with jax.named_scope("greet"):
        small_loads[0].wait()
        for f in range(fields):
            for l in range(levels):
                b.decay[f * levels + l] = jnp.full((1, 128), chain_decay[0, l, f], jnp.float32)
        own_at(0)
        pl.semaphore_wait(barrier, len(bits) + sum(there.astype(jnp.int32) for there, _ in near))

        @pl.when(odd == 1)
        def _():
            decay_copy.start()

        @pl.when(jnp.logical_and(even, s >= 2))
        def _():
            decay_leg.start()

    def own_next(c):
        own_at(c)
        give_own(c - 1)

    with jax.named_scope("own"):
        give_own(0)
        own_at(1)
        loop(2, chunks, own_next)
        give_own(chunks - 1)

    for copy in small_loads[1:]:
        copy.wait()
    for ref in (b.inc, b.mult, b.work, b.b1):
        edges(ref, planes)
    edges(b.columns, 4)

    def row_index(r0):
        return lax.broadcasted_iota(jnp.int32, (wide, cols), 0) + (r0 - PAD)

    def forward(h, u, v, column, r0, gain, depth):
        p = gain * h
        if column is not None:
            p = p + COUPLING * column
        u_new = u + TIME_STEP * (ROTATION_PARAM * v - (up_x(p) - p))
        v_new = v - TIME_STEP * (ROTATION_PARAM * u + (up_y(p) - p))
        u_new = jnp.where(row_index(r0) < 0, 0.0, u_new)
        h_new = h - TIME_STEP * depth * ((u_new - down_x(u_new)) + (v_new - down_y(v_new)))
        return h_new, u_new, v_new

    def back(h, u, v, r0, gain, depth):
        w = depth * h
        u2 = u + TIME_STEP * (up_x(w) - w)
        v2 = v + TIME_STEP * (up_y(w) - w)
        u2 = jnp.where(row_index(r0) < 0, 0.0, u2)
        p = TIME_STEP * ((u2 - down_x(u2)) + (v2 - down_y(v2)))
        return h + gain * p, u2 - HALF * v2, v2 + HALF * u2, p

    def middle(a):
        return a[PAD:PAD + step]

    def state_at(ref, l, r0):
        at = pl.ds(r0, wide)
        return ref[l, at, :], ref[levels + l, at, :], ref[2 * levels + l, at, :]

    def sweep(fn):
        loop(0, rows // step, lambda i: fn(pl.multiple_of(i * step, 8)))

    def put(ref, l, r0, values):
        for f, value in enumerate(values):
            ref[f * levels + l, pl.ds(r0, step), :] = middle(value)

    def put_padded(ref, l, r0, values):
        put(ref, l, r0 + PAD, values)

    sums = b.sums

    def ahead(r0):
        c0 = c1 = None
        for l in range(levels):
            h, u, v = state_at(b.inc, l, r0)
            h_new, _, _ = forward(h, u, v, None, r0, level_gain[l], mean_depth[l])
            c0 = middle(h) if c0 is None else c0 + middle(h)
            c1 = middle(h_new) if c1 is None else c1 + middle(h_new)
        sums[0, pl.ds(r0, step), :] = c0
        sums[0, pl.ds(rows + r0, step), :] = c1

    def behind(source, to):
        def fn(r0):
            bar = None
            for l in range(levels):
                h, u, v = state_at(source, l, r0)
                h2, u2, v2, p = back(h, u, v, r0, level_gain[l], mean_depth[l])
                if to == 0:
                    put_padded(b.b1, l, r0, (h2, u2, v2))
                bar = middle(p) if bar is None else bar + middle(p)
            sums[1, pl.ds(to * rows + r0, step), :] = COUPLING * bar
        return fn

    with jax.named_scope("ahead"):
        sweep(ahead)
    with jax.named_scope("behind"):
        sweep(behind(b.mult, 0))
        sweep(behind(b.b1, 1))
    depth_sum = mean_depth[0]
    for l in range(1, levels):
        depth_sum = depth_sum + mean_depth[l]
    for k in range(2):
        sums[k, pl.ds(2 * rows, PAD), :] = jnp.full((PAD, cols), depth_sum, jnp.float32)

    half = lev % 2
    tall = 2 * rows + PAD
    total = b.total

    def meet_copy():
        return lev_move(sums.at[1 - half], b.met.at[0], 0, across(1))

    def add_met(slot, first):
        def fn(r0):
            at = pl.ds(r0, PAD)
            kept = sums[half, at, :] if first else total[at, :]
            total[at, :] = kept + b.met[slot, at, :]
        loop(0, tall // PAD, lambda i: fn(pl.multiple_of(i * PAD, 8)))

    meet = meet_copy()
    with jax.named_scope("meet"):
        meet.start()
        meet.wait()
        add_met(0, True)

    def observe():
        count = obs_cell.shape[2]
        if cols & (cols - 1) == 0:
            shift = cols.bit_length() - 1

            def split(cells):
                return cells >> shift, cells & (cols - 1)
        else:
            def split(cells):
                return lax.div(cells, cols), lax.rem(cells, cols)

        row = lax.broadcasted_iota(jnp.int32, (rows, count), 0)
        col = lax.broadcasted_iota(jnp.int32, (cols, count), 0)
        for l in range(levels):
            at_row, at_col = split(obs_cell[0, pl.ds(l, 1), :])
            values = obs_dual[0, pl.ds(l, 1), :]
            hit_row = jnp.where(row == at_row, 1.0, 0.0)
            hit_col = jnp.where(col == at_col, 1.0, 0.0)
            seen = lax.dot_general(
                b.inc[l, pl.ds(PAD, rows), :], hit_col, (((1,), (0,)), ((), ())),
                precision=lax.Precision.HIGHEST, preferred_element_type=jnp.float32,
            )
            picked = jnp.sum(hit_row * seen, axis=0, keepdims=True)
            obs_out[0, pl.ds(l, 1), :] = obs_var[0, pl.ds(l, 1), :] * values + picked
            b.added[l] = lax.dot_general(
                hit_row * values, hit_col, (((1,), (1,)), ((), ())),
                precision=lax.Precision.HIGHEST, preferred_element_type=jnp.float32,
            )

    for i, bit in enumerate(bits[1:], 1):
        far = lev_move(total, b.met.at[i], i, across(bit))
        far.start()
        if i == 1:
            with jax.named_scope("observe"):
                observe()
        with jax.named_scope("far"):
            far.wait()
            add_met(i, False)
    if len(bits) < 2:
        observe()

    columns = b.columns

    def first_column(r0):
        columns[2 * half, pl.ds(r0 + PAD, step), :] = total[pl.ds(r0, step), :]

    def second_column(r0):
        c = columns[2 * half, pl.ds(r0, wide), :]
        gx = jnp.where(row_index(r0) < 0, 0.0, up_x(c) - c)
        gy = up_y(c) - c
        lap = (gx - down_x(gx)) + (gy - down_y(gy))
        scale = (TIME_STEP * TIME_STEP * COUPLING) * total[pl.ds(2 * rows, 1), pl.ds(0, 1)]
        columns[2 * half + 1, pl.ds(r0 + PAD, step), :] = total[pl.ds(rows + r0, step), :] + scale * middle(lap)

    with jax.named_scope("column"):
        sweep(first_column)
        sweep(second_column)
    mine = columns.at[pl.ds(2 * half, 2)]
    near_copy = lev_move(mine, mine, len(bits), across(1))
    with jax.named_scope("near"):
        near_copy.start()
        near_copy.wait()

    def last_back(r0):
        at = pl.ds(r0, wide)
        bar0, bar1 = columns[2, at, :], columns[3, at, :]
        for l in range(levels):
            h, u, v = state_at(b.b1, l, r0)
            h2, u2, v2, _ = back(h + bar0, u, v, r0, level_gain[l], mean_depth[l])
            put(b.adjoint, l, r0, (h2 + bar1, u2, v2))

    def first_forward(r0):
        column = columns[0, pl.ds(r0, wide), :]
        for l in range(levels):
            h, u, v = state_at(b.inc, l, r0)
            put_padded(b.work, l, r0, forward(h, u, v, column, r0, level_gain[l], mean_depth[l]))

    def last_forward(r0):
        column = columns[1, pl.ds(r0, wide), :]
        for l in range(levels):
            h, u, v = state_at(b.work, l, r0)
            put(b.tangent, l, r0, forward(h, u, v, column, r0, level_gain[l], mean_depth[l]))

    @pl.when(turns)
    def _():
        decay_leg.wait_recv()
        decay_turn.start()

    with jax.named_scope("back"):
        sweep(last_back)
    below = pair - 1
    down_cut = adjoint_cut(below)
    across_cut = adjoint_cut(pair)

    @pl.when(jnp.logical_and(even, s >= 2))
    def _():
        loop(0, down_cut, lambda c: adjoint_leg(c, s - 2).start())
        loop(down_cut, chunks, lambda c: adjoint_leg(c, s + 1).start())

    with jax.named_scope("forward"):
        sweep(first_forward)
        sweep(last_forward)
    up_cut = tangent_cut(pair)
    here_cut = tangent_cut(below)
    climbs = jnp.logical_and(odd == 1, s < n - 1)

    @pl.when(even)
    def _():
        loop(0, chunks, lambda c: tangent_copy(c).start())

    @pl.when(climbs)
    def _():
        loop(0, up_cut, lambda c: tangent_leg(c, s + 2).start())
        loop(up_cut, chunks, lambda c: tangent_leg(c, s - 1).start())

    def chain_step(c):
        p, r = where_in(c)
        d = chain_decay[0, p % levels, p // levels]

        @pl.when(s >= 1)
        def _():
            tangent_copy(c).wait_recv()

        @pl.when(s == 0)
        def _():
            tangent_in[p, r, :] = jnp.zeros((part, cols), jnp.float32)

        @pl.when(s >= 2)
        def _():
            chain_copy(c).wait_recv()

        @pl.when(s < 2)
        def _():
            carried[p, r, :] = jnp.zeros((part, cols), jnp.float32)

        @pl.when(jnp.logical_and(c % per == 0, jnp.logical_or(odd == 1, s < n - 2)))
        def _():
            own_plane(p).wait_recv()

        swap = b.swap[p, r, :]
        product = b.own[p, r, :] - tangent_in[p, r, :]
        here = d * (carried[p, r, :] + jnp.where(odd == 1, swap, 0.0)) + product

        @pl.when(s < n - 2)
        def _():
            d_next = b.decay_in[p][:, :1]
            b.sent[p, r, :] = d_next * here + (jnp.where(even, swap, 0.0) - b.tangent[p, r, :])

        tangent_in[p, r, :] = product
        carried[p, r, :] = here

        @pl.when(s < n - 2)
        def _():
            chain_copy(c).start()

    @pl.when(s == 0)
    def _():
        decay_copy.wait_recv()

    with jax.named_scope("chain0"):
        loop(0, jnp.where(s == 0, chunks, 0), chain_step)

    @pl.when(jnp.logical_and(even, s < n - 2))
    def _():
        def turn_up(c):
            tangent_leg(c, s - 1).wait_recv()
            tangent_turn(c, s + 2).start()

        def turn_across(c):
            adjoint_leg(c, s - 2).wait_recv()
            adjoint_turn(c, s + 1).start()

        with jax.named_scope("turn_up"):
            loop(up_cut, chunks, turn_up)
        with jax.named_scope("turn_over"):
            loop(0, across_cut, turn_across)

    early = jnp.where(s == n - 1, chunks // 2, 0)

    @pl.when(odd == 1)
    def _():
        loop(0, early, lambda c: adjoint_copy(c).start())

        @pl.when(s >= 3)
        def _():
            def turn_across(c):
                tangent_leg(c, s + 2).wait_recv()
                tangent_turn(c, s - 1).start()

            with jax.named_scope("turn_back"):
                loop(0, here_cut, turn_across)

        loop(early, chunks, lambda c: adjoint_copy(c).start())

        @pl.when(s >= 3)
        def _():
            def turn_down(c):
                adjoint_leg(c, s + 1).wait_recv()
                adjoint_turn(c, s - 2).start()

            with jax.named_scope("turn_down"):
                loop(down_cut, chunks, turn_down)

    def block_step(i):
        c = lax.rem(i + across_cut * odd, chunks)
        p, r = where_in(c)
        inner = pl.ds(pl.multiple_of((c % per) * part + PAD, 8), part)

        @pl.when(s < n - 1)
        def _():
            adjoint_copy(c).wait_recv()

        kept = b.mult[p, inner, :] - jnp.where(s < n - 1, adjoint_in[p, r, :], 0.0)
        adjoint_in[p, r, :] = kept

        @pl.when(p < levels)
        def _():
            adjoint_in[p, r, :] = kept + b.added[jnp.minimum(p, levels - 1), r, :]

    loop(0, jnp.where(s == n - 1, chunks, 0), block_step)

    @pl.when(jnp.logical_and(s > 0, s < n - 1))
    def _():
        decay_copy.wait_recv()

    with jax.named_scope("chain"):
        loop(0, jnp.where(s == 0, 0, chunks), chain_step)

    with jax.named_scope("block"):
        loop(0, jnp.where(s == n - 1, 0, chunks), block_step)

    with jax.named_scope("drain"):
        @pl.when(gives_own)
        def _():
            all_sent(b.own, b.swap, 0)

        @pl.when(s < n - 1)
        def _():
            all_sent(b.tangent, tangent_in, 1)

        @pl.when(s >= 1)
        def _():
            all_sent(b.adjoint, adjoint_in, 2)
            decay_copy.wait_send()

        @pl.when(turns)
        def _():
            decay_turn.wait_send()

        def turned(ref, i, count):
            if count:
                all_sent(ref.at[pl.ds(0, count)], ref.at[pl.ds(0, count)], i)

        for k in range(pairs - 1):
            @pl.when(s == 2 * k)
            def _():
                turned(b.relay_t, 4, chunks - tangent_cut(k))
                turned(b.relay_a, 5, adjoint_cut(k))

            @pl.when(s == 2 * k + 3)
            def _():
                turned(b.relay_t, 4, tangent_cut(k))
                turned(b.relay_a, 5, chunks - adjoint_cut(k))

        @pl.when(s < n - 2)
        def _():
            all_sent(b.sent, carried, 3)


def write_out(dual_in, seen_in, block_in, chain_in, dual, seen, block, chain, sems):
    copies = [
        pltpu.make_async_copy(src, dst, sems.at[i])
        for i, (src, dst) in enumerate(((dual_in, dual), (block_in, block), (chain_in, chain), (seen_in, seen)))
    ]
    for copy in copies:
        copy.start()
    for copy in copies:
        copy.wait()


def shards(
    increment, multiplier, error_var, obs_cell, obs_dual, obs_var,
    level_gain, mean_depth, chain_decay,
):
    n = lax.axis_size("tm")
    size = lax.axis_size("lev")
    if n % 2 or size < 2 or size & (size - 1):
        raise ValueError("unsupported mesh")
    _, fields, levels, rows, cols = increment.shape
    planes = fields * levels
    chunks = planes * pieces(rows)
    rounds = size.bit_length() - 1
    tall = 2 * rows + PAD

    def room(*shape):
        return pltpu.VMEM(shape, jnp.float32)

    def flags(count):
        return pltpu.SemaphoreType.DMA((count,))

    scratch = Scratch(
        *[room(planes, rows + 2 * PAD, cols)] * 4,
        *[room(planes, rows, cols)] * 5, *[room(chunks, rows // pieces(rows), cols)] * 2,
        room(2, tall, cols), room(rounds, tall, cols), room(tall, cols),
        room(4, rows + 2 * PAD, cols), room(levels, rows, cols),
        *[room(planes, 1, 128)] * 3,
        pltpu.VMEM(obs_cell.shape, jnp.int32), room(*obs_dual.shape), room(*obs_var.shape),
        pltpu.SMEM(level_gain.shape, jnp.float32), pltpu.SMEM(mean_depth.shape, jnp.float32),
        pltpu.SMEM((1, levels, fields), jnp.float32),
        flags(6), *[flags(planes)] * 2, *[flags(chunks)] * 5,
        flags(2), flags(2), flags(6), flags(rounds + 1), flags(rounds + 1),
    )
    place = pl.BlockSpec(memory_space=pl.ANY)
    small = pl.BlockSpec(memory_space=pltpu.VMEM)
    held = pltpu.VMEM((planes, rows, cols), jnp.float32)
    results = pl.pallas_call(
        functools.partial(kernel, n, size),
        out_shape=[held, pltpu.VMEM(obs_dual.shape, jnp.float32), held, held],
        in_specs=[place] * 9,
        out_specs=[small] * 4,
        scratch_shapes=list(scratch),
        compiler_params=pltpu.CompilerParams(
            collective_id=0, has_side_effects=True, vmem_limit_bytes=50 * 1024 * 1024
        ),
    )(
        increment, multiplier, error_var, obs_cell, obs_dual, obs_var,
        level_gain, mean_depth, jnp.swapaxes(chain_decay, 1, 2),
    )
    dual, seen, block, chain = pl.pallas_call(
        write_out,
        out_shape=[jax.ShapeDtypeStruct(r.shape, jnp.float32) for r in results],
        in_specs=[small] * 4,
        out_specs=[place] * 4,
        scratch_shapes=[flags(4)],
        compiler_params=pltpu.CompilerParams(vmem_limit_bytes=1024 * 1024),
    )(*[pltpu.with_memory_space_constraint(r, pltpu.VMEM) for r in results])
    return (
        dual.reshape(increment.shape), seen, block.reshape(increment.shape), chain.reshape(increment.shape),
    )


def solution(mesh):
    state = P("tm", None, "lev", None, None)
    obs = P("tm", "lev", None)
    return jax.shard_map(
        shards,
        mesh=mesh,
        in_specs=(state, state, state, obs, obs, obs, P("lev"), P("lev"), P("tm", None, "lev")),
        out_specs=(state, obs, state, state),
        check_vma=False,
    )
```

```python
from typing import Any, NamedTuple

import jax
import jax.numpy as jnp
from jax import lax
from jax.experimental import pallas as pl
from jax.experimental.pallas import tpu as pltpu
from jax.sharding import PartitionSpec as P

TIME_STEP = 0.25
ROTATION_PARAM = 0.5
COUPLING = 0.25
HALF = TIME_STEP * ROTATION_PARAM
SPLIT = 4
PAD = 8
MESH_ID = pl.DeviceIdType.MESH


class Scratch(NamedTuple):
    inc: Any
    mult: Any
    work: Any
    b1: Any
    own: Any
    swap: Any
    tangent: Any
    adjoint: Any
    sent: Any
    relay_t: Any
    relay_a: Any
    sums: Any
    met: Any
    total: Any
    columns: Any
    added: Any
    decay: Any
    decay_in: Any
    decay_relay: Any
    cells: Any
    obs_dual: Any
    obs_var: Any
    gain: Any
    depth: Any
    chain_decay: Any
    sends: Any
    own_recv: Any
    loads: Any
    tan_recv: Any
    adj_recv: Any
    rt_recv: Any
    ra_recv: Any
    ch_recv: Any
    decay_send: Any
    decay_recv: Any
    small_loads: Any
    lev_send: Any
    lev_recv: Any


def pieces(rows):
    return SPLIT if rows % (8 * SPLIT) == 0 else 1


def block_rows(rows):
    part = rows // pieces(rows)
    return next(b for b in (32, 16, 8, part) if part % b == 0)


def up_y(a):
    lane = lax.broadcasted_iota(jnp.int32, a.shape, 1)
    return jnp.where(lane == a.shape[1] - 1, 0.0, pltpu.roll(a, a.shape[1] - 1, 1))


def down_y(a):
    lane = lax.broadcasted_iota(jnp.int32, a.shape, 1)
    return jnp.where(lane == 0, 0.0, pltpu.roll(a, 1, 1))


def up_x(a):
    return pltpu.roll(a, a.shape[0] - 1, 0)


def down_x(a):
    return pltpu.roll(a, 1, 0)


def kernel(
    n, size, increment, multiplier, error_var, cell_at, obs_dual_at, obs_var_at, gain_at, depth_at,
    decay_at, tangent_in, obs_out, adjoint_in, carried, *scratch,
):
    b = Scratch(*scratch)
    obs_cell, obs_dual, obs_var = b.cells, b.obs_dual, b.obs_var
    level_gain, mean_depth, chain_decay = b.gain, b.depth, b.chain_decay
    fields, levels, rows, cols = increment.shape[1:]
    planes = fields * levels
    per = pieces(rows)
    chunks = planes * per
    part = rows // per
    step = block_rows(rows)
    wide = step + 2 * PAD

    s = lax.axis_index("tm")
    lev = lax.axis_index("lev")
    odd = s % 2
    even = odd == 0
    pair = s // 2
    pairs = n // 2
    partner = s + 1 - 2 * odd

    def adjoint_cut(k):
        return chunks * (pairs - 1 - k) // pairs

    def tangent_cut(k):
        return chunks * (k + 1) // max(pairs - 1, 1)

    def loop(low, high, fn):
        lax.fori_loop(low, high, lambda c, z: (fn(c), z)[1], 0)

    def where_in(c):
        return c // per, pl.ds(pl.multiple_of((c % per) * part, 8), part)

    def piece(ref, c):
        p, r = where_in(c)
        return ref.at[p, r, :]

    def remote(src, dst, send, recv, where):
        return pltpu.make_async_remote_copy(
            src_ref=src, dst_ref=dst, send_sem=send, recv_sem=recv, device_id=where, device_id_type=MESH_ID,
        )

    def move(src, dst, send, recv, c, to):
        return remote(piece(src, c), piece(dst, c), send, recv.at[c], {"tm": to})

    def lev_move(src, dst, i, to):
        return remote(src, dst, b.lev_send.at[i], b.lev_recv.at[i], {"lev": to})

    def own_copy(c):
        return remote(piece(b.own, c), piece(b.swap, c), b.sends.at[0], b.own_recv.at[c // per], {"tm": partner})

    def own_plane(p):
        return remote(b.own.at[p], b.swap.at[p], b.sends.at[0], b.own_recv.at[p], {"tm": partner})

    def all_sent(src, dst, i):
        remote(src, dst, b.sends.at[i], b.own_recv.at[0], {"tm": partner}).wait_send()

    def tangent_copy(c):
        return move(b.tangent, tangent_in, b.sends.at[1], b.tan_recv, c, s + 1)

    def adjoint_copy(c):
        return move(b.adjoint, adjoint_in, b.sends.at[2], b.adj_recv, c, s - 1)

    def chain_copy(c):
        return move(b.sent, carried, b.sends.at[3], b.ch_recv, c, s + 2)

    def tangent_leg(c, to):
        return remote(piece(b.tangent, c), b.relay_t.at[c], b.sends.at[1], b.rt_recv.at[c], {"tm": to})

    def tangent_turn(c, to):
        return remote(b.relay_t.at[c], piece(tangent_in, c), b.sends.at[4], b.tan_recv.at[c], {"tm": to})

    def adjoint_leg(c, to):
        return remote(piece(b.adjoint, c), b.relay_a.at[c], b.sends.at[2], b.ra_recv.at[c], {"tm": to})

    def adjoint_turn(c, to):
        return remote(b.relay_a.at[c], piece(adjoint_in, c), b.sends.at[5], b.adj_recv.at[c], {"tm": to})

    decay_copy = remote(b.decay, b.decay_in, b.decay_send.at[0], b.decay_recv.at[0], {"tm": s - 1})
    decay_leg = remote(b.decay, b.decay_relay, b.decay_send.at[0], b.decay_recv.at[1], {"tm": s - 2})
    decay_turn = remote(b.decay_relay, b.decay_in, b.decay_send.at[1], b.decay_recv.at[0], {"tm": s + 1})
    turns = jnp.logical_and(even, s < n - 2)

    def load(i, p):
        src = (increment, multiplier, error_var)[i]
        dst = (b.inc, b.mult, b.work)[i]
        return pltpu.make_async_copy(
            src.at[0, p // levels, p % levels], dst.at[p, pl.ds(PAD, rows), :], b.loads.at[p]
        )

    barrier = pltpu.get_barrier_semaphore()
    near = ((s >= 0, partner), (s >= 2, s - 2), (s < n - 2, s + 2))
    for there, who in near:
        @pl.when(there)
        def _():
            pl.semaphore_signal(barrier, inc=1, device_id={"tm": who}, device_id_type=MESH_ID)
    bits = []
    bit = 1
    while bit < size:
        bits.append(bit)
        bit *= 2

    def across(bit):
        return lev + bit - 2 * bit * ((lev // bit) % 2)

    for bit in bits:
        pl.semaphore_signal(barrier, inc=1, device_id={"lev": across(bit)}, device_id_type=MESH_ID)

    small_loads = [
        pltpu.make_async_copy(src, dst, b.small_loads.at[i])
        for i, (src, dst) in enumerate((
            (decay_at, chain_decay), (gain_at, level_gain), (depth_at, mean_depth),
            (cell_at, obs_cell), (obs_dual_at, obs_dual), (obs_var_at, obs_var),
        ))
    ]
    small_loads[0].start()
    for p in range(planes):
        for i in range(3):
            load(i, p).start()
    for copy in small_loads[1:]:
        copy.start()

    def edges(ref, planes):
        zero = jnp.zeros((PAD, cols), jnp.float32)
        for p in range(planes):
            ref[p, pl.ds(0, PAD), :] = zero
            ref[p, pl.ds(PAD + rows, PAD), :] = zero

    def own_at(c):
        p, r = where_in(c)

        @pl.when(c % per == 0)
        def _():
            pltpu.make_async_copy(
                increment.at[0, :, 0], b.inc.at[pl.ds(0, fields), pl.ds(PAD, rows), :], b.loads.at[p]
            ).wait()

        inner = pl.ds(pl.multiple_of((c % per) * part + PAD, 8), part)
        b.own[p, r, :] = b.work[p, inner, :] * b.mult[p, inner, :] + b.inc[p, inner, :]

    gives_own = jnp.logical_or(even, s < n - 1)

    def give_own(c):
        @pl.when(gives_own)
        def _():
            own_copy(c).start()

    with jax.named_scope("greet"):
        small_loads[0].wait()
        for f in range(fields):
            for l in range(levels):
                b.decay[f * levels + l] = jnp.full((1, 128), chain_decay[0, l, f], jnp.float32)
        own_at(0)
        pl.semaphore_wait(barrier, len(bits) + sum(there.astype(jnp.int32) for there, _ in near))

        @pl.when(odd == 1)
        def _():
            decay_copy.start()

        @pl.when(jnp.logical_and(even, s >= 2))
        def _():
            decay_leg.start()

    def own_next(c):
        own_at(c)
        give_own(c - 1)

    with jax.named_scope("own"):
        give_own(0)
        own_at(1)
        loop(2, chunks, own_next)
        give_own(chunks - 1)

    for copy in small_loads[1:]:
        copy.wait()
    for ref in (b.inc, b.mult, b.work, b.b1):
        edges(ref, planes)
    edges(b.columns, 4)

    def row_index(r0):
        return lax.broadcasted_iota(jnp.int32, (wide, cols), 0) + (r0 - PAD)

    def forward(h, u, v, column, r0, gain, depth):
        p = gain * h
        if column is not None:
            p = p + COUPLING * column
        u_new = u + TIME_STEP * (ROTATION_PARAM * v - (up_x(p) - p))
        v_new = v - TIME_STEP * (ROTATION_PARAM * u + (up_y(p) - p))
        u_new = jnp.where(row_index(r0) < 0, 0.0, u_new)
        h_new = h - TIME_STEP * depth * ((u_new - down_x(u_new)) + (v_new - down_y(v_new)))
        return h_new, u_new, v_new

    def back(h, u, v, r0, gain, depth):
        w = depth * h
        u2 = u + TIME_STEP * (up_x(w) - w)
        v2 = v + TIME_STEP * (up_y(w) - w)
        u2 = jnp.where(row_index(r0) < 0, 0.0, u2)
        p = TIME_STEP * ((u2 - down_x(u2)) + (v2 - down_y(v2)))
        return h + gain * p, u2 - HALF * v2, v2 + HALF * u2, p

    def middle(a):
        return a[PAD:PAD + step]

    def state_at(ref, l, r0):
        at = pl.ds(r0, wide)
        return ref[l, at, :], ref[levels + l, at, :], ref[2 * levels + l, at, :]

    def sweep(fn):
        loop(0, rows // step, lambda i: fn(pl.multiple_of(i * step, 8)))

    def put(ref, l, r0, values):
        for f, value in enumerate(values):
            ref[f * levels + l, pl.ds(r0, step), :] = middle(value)

    def put_padded(ref, l, r0, values):
        put(ref, l, r0 + PAD, values)

    sums = b.sums

    def ahead(r0):
        c0 = c1 = None
        for l in range(levels):
            h, u, v = state_at(b.inc, l, r0)
            h_new, _, _ = forward(h, u, v, None, r0, level_gain[l], mean_depth[l])
            c0 = middle(h) if c0 is None else c0 + middle(h)
            c1 = middle(h_new) if c1 is None else c1 + middle(h_new)
        sums[0, pl.ds(r0, step), :] = c0
        sums[0, pl.ds(rows + r0, step), :] = c1

    def behind(source, to):
        def fn(r0):
            bar = None
            for l in range(levels):
                h, u, v = state_at(source, l, r0)
                h2, u2, v2, p = back(h, u, v, r0, level_gain[l], mean_depth[l])
                if to == 0:
                    put_padded(b.b1, l, r0, (h2, u2, v2))
                bar = middle(p) if bar is None else bar + middle(p)
            sums[1, pl.ds(to * rows + r0, step), :] = COUPLING * bar
        return fn

    with jax.named_scope("ahead"):
        sweep(ahead)
    with jax.named_scope("behind"):
        sweep(behind(b.mult, 0))
        sweep(behind(b.b1, 1))
    depth_sum = mean_depth[0]
    for l in range(1, levels):
        depth_sum = depth_sum + mean_depth[l]
    for k in range(2):
        sums[k, pl.ds(2 * rows, PAD), :] = jnp.full((PAD, cols), depth_sum, jnp.float32)

    half = lev % 2
    tall = 2 * rows + PAD
    total = b.total

    def meet_copy():
        return lev_move(sums.at[1 - half], b.met.at[0], 0, across(1))

    def add_met(slot, first):
        def fn(r0):
            at = pl.ds(r0, PAD)
            kept = sums[half, at, :] if first else total[at, :]
            total[at, :] = kept + b.met[slot, at, :]
        loop(0, tall // PAD, lambda i: fn(pl.multiple_of(i * PAD, 8)))

    meet = meet_copy()
    with jax.named_scope("meet"):
        meet.start()
        meet.wait()
        add_met(0, True)

    def observe():
        count = obs_cell.shape[2]
        if cols & (cols - 1) == 0:
            shift = cols.bit_length() - 1

            def split(cells):
                return cells >> shift, cells & (cols - 1)
        else:
            def split(cells):
                return lax.div(cells, cols), lax.rem(cells, cols)

        row = lax.broadcasted_iota(jnp.int32, (rows, count), 0)
        col = lax.broadcasted_iota(jnp.int32, (cols, count), 0)
        for l in range(levels):
            at_row, at_col = split(obs_cell[0, pl.ds(l, 1), :])
            values = obs_dual[0, pl.ds(l, 1), :]
            hit_row = jnp.where(row == at_row, 1.0, 0.0)
            hit_col = jnp.where(col == at_col, 1.0, 0.0)
            seen = lax.dot_general(
                b.inc[l, pl.ds(PAD, rows), :], hit_col, (((1,), (0,)), ((), ())),
                precision=lax.Precision.HIGHEST, preferred_element_type=jnp.float32,
            )
            picked = jnp.sum(hit_row * seen, axis=0, keepdims=True)
            obs_out[0, pl.ds(l, 1), :] = obs_var[0, pl.ds(l, 1), :] * values + picked
            b.added[l] = lax.dot_general(
                hit_row * values, hit_col, (((1,), (1,)), ((), ())),
                precision=lax.Precision.HIGHEST, preferred_element_type=jnp.float32,
            )

    for i, bit in enumerate(bits[1:], 1):
        far = lev_move(total, b.met.at[i], i, across(bit))
        far.start()
        if i == 1:
            with jax.named_scope("observe"):
                observe()
        with jax.named_scope("far"):
            far.wait()
            add_met(i, False)
    if len(bits) < 2:
        observe()

    columns = b.columns

    def first_column(r0):
        columns[2 * half, pl.ds(r0 + PAD, step), :] = total[pl.ds(r0, step), :]

    def second_column(r0):
        c = columns[2 * half, pl.ds(r0, wide), :]
        gx = jnp.where(row_index(r0) < 0, 0.0, up_x(c) - c)
        gy = up_y(c) - c
        lap = (gx - down_x(gx)) + (gy - down_y(gy))
        scale = (TIME_STEP * TIME_STEP * COUPLING) * total[pl.ds(2 * rows, 1), pl.ds(0, 1)]
        columns[2 * half + 1, pl.ds(r0 + PAD, step), :] = total[pl.ds(rows + r0, step), :] + scale * middle(lap)

    with jax.named_scope("column"):
        sweep(first_column)
        sweep(second_column)
    mine = columns.at[pl.ds(2 * half, 2)]
    near_copy = lev_move(mine, mine, len(bits), across(1))
    with jax.named_scope("near"):
        near_copy.start()
        near_copy.wait()

    def last_back(r0):
        at = pl.ds(r0, wide)
        bar0, bar1 = columns[2, at, :], columns[3, at, :]
        for l in range(levels):
            h, u, v = state_at(b.b1, l, r0)
            h2, u2, v2, _ = back(h + bar0, u, v, r0, level_gain[l], mean_depth[l])
            put(b.adjoint, l, r0, (h2 + bar1, u2, v2))

    def first_forward(r0):
        column = columns[0, pl.ds(r0, wide), :]
        for l in range(levels):
            h, u, v = state_at(b.inc, l, r0)
            put_padded(b.work, l, r0, forward(h, u, v, column, r0, level_gain[l], mean_depth[l]))

    def last_forward(r0):
        column = columns[1, pl.ds(r0, wide), :]
        for l in range(levels):
            h, u, v = state_at(b.work, l, r0)
            put(b.tangent, l, r0, forward(h, u, v, column, r0, level_gain[l], mean_depth[l]))

    @pl.when(turns)
    def _():
        decay_leg.wait_recv()
        decay_turn.start()

    with jax.named_scope("back"):
        sweep(last_back)
    below = pair - 1
    down_cut = adjoint_cut(below)
    across_cut = adjoint_cut(pair)

    @pl.when(jnp.logical_and(even, s >= 2))
    def _():
        loop(0, down_cut, lambda c: adjoint_leg(c, s - 2).start())
        loop(down_cut, chunks, lambda c: adjoint_leg(c, s + 1).start())

    with jax.named_scope("forward"):
        sweep(first_forward)
        sweep(last_forward)
    up_cut = tangent_cut(pair)
    here_cut = tangent_cut(below)
    climbs = jnp.logical_and(odd == 1, s < n - 1)

    @pl.when(even)
    def _():
        loop(0, chunks, lambda c: tangent_copy(c).start())

    @pl.when(climbs)
    def _():
        loop(0, up_cut, lambda c: tangent_leg(c, s + 2).start())
        loop(up_cut, chunks, lambda c: tangent_leg(c, s - 1).start())

    def chain_step(c):
        p, r = where_in(c)
        d = chain_decay[0, p % levels, p // levels]

        @pl.when(s >= 1)
        def _():
            tangent_copy(c).wait_recv()

        @pl.when(s == 0)
        def _():
            tangent_in[p, r, :] = jnp.zeros((part, cols), jnp.float32)

        @pl.when(s >= 2)
        def _():
            chain_copy(c).wait_recv()

        @pl.when(s < 2)
        def _():
            carried[p, r, :] = jnp.zeros((part, cols), jnp.float32)

        @pl.when(jnp.logical_and(c % per == 0, jnp.logical_or(odd == 1, s < n - 2)))
        def _():
            own_plane(p).wait_recv()

        swap = b.swap[p, r, :]
        product = b.own[p, r, :] - tangent_in[p, r, :]
        here = d * (carried[p, r, :] + jnp.where(odd == 1, swap, 0.0)) + product

        @pl.when(s < n - 2)
        def _():
            d_next = b.decay_in[p][:, :1]
            b.sent[p, r, :] = d_next * here + (jnp.where(even, swap, 0.0) - b.tangent[p, r, :])

        tangent_in[p, r, :] = product
        carried[p, r, :] = here

        @pl.when(s < n - 2)
        def _():
            chain_copy(c).start()

    @pl.when(s == 0)
    def _():
        decay_copy.wait_recv()

    with jax.named_scope("chain0"):
        loop(0, jnp.where(s == 0, chunks, 0), chain_step)

    @pl.when(jnp.logical_and(even, s < n - 2))
    def _():
        def turn_up(c):
            tangent_leg(c, s - 1).wait_recv()
            tangent_turn(c, s + 2).start()

        def turn_across(c):
            adjoint_leg(c, s - 2).wait_recv()
            adjoint_turn(c, s + 1).start()

        with jax.named_scope("turn_up"):
            loop(up_cut, chunks, turn_up)
        with jax.named_scope("turn_over"):
            loop(0, across_cut, turn_across)

    early = jnp.where(s == n - 1, chunks // 2, 0)

    @pl.when(odd == 1)
    def _():
        loop(0, early, lambda c: adjoint_copy(c).start())

        @pl.when(s >= 3)
        def _():
            def turn_across(c):
                tangent_leg(c, s + 2).wait_recv()
                tangent_turn(c, s - 1).start()

            with jax.named_scope("turn_back"):
                loop(0, here_cut, turn_across)

        loop(early, chunks, lambda c: adjoint_copy(c).start())

        @pl.when(s >= 3)
        def _():
            def turn_down(c):
                adjoint_leg(c, s + 1).wait_recv()
                adjoint_turn(c, s - 2).start()

            with jax.named_scope("turn_down"):
                loop(down_cut, chunks, turn_down)

    def block_step(i):
        c = lax.rem(i + across_cut * odd, chunks)
        p, r = where_in(c)
        inner = pl.ds(pl.multiple_of((c % per) * part + PAD, 8), part)

        @pl.when(s < n - 1)
        def _():
            adjoint_copy(c).wait_recv()

        kept = b.mult[p, inner, :] - jnp.where(s < n - 1, adjoint_in[p, r, :], 0.0)
        adjoint_in[p, r, :] = kept

        @pl.when(p < levels)
        def _():
            adjoint_in[p, r, :] = kept + b.added[jnp.minimum(p, levels - 1), r, :]

    loop(0, jnp.where(s == n - 1, chunks, 0), block_step)

    @pl.when(jnp.logical_and(s > 0, s < n - 1))
    def _():
        decay_copy.wait_recv()

    with jax.named_scope("chain"):
        loop(0, jnp.where(s == 0, 0, chunks), chain_step)

    with jax.named_scope("block"):
        loop(0, jnp.where(s == n - 1, 0, chunks), block_step)

    with jax.named_scope("drain"):
        @pl.when(gives_own)
        def _():
            all_sent(b.own, b.swap, 0)

        @pl.when(s < n - 1)
        def _():
            all_sent(b.tangent, tangent_in, 1)

        @pl.when(s >= 1)
        def _():
            all_sent(b.adjoint, adjoint_in, 2)
            decay_copy.wait_send()

        @pl.when(turns)
        def _():
            decay_turn.wait_send()

        def turned(ref, i, count):
            if count:
                all_sent(ref.at[pl.ds(0, count)], ref.at[pl.ds(0, count)], i)

        for k in range(pairs - 1):
            @pl.when(s == 2 * k)
            def _():
                turned(b.relay_t, 4, chunks - tangent_cut(k))
                turned(b.relay_a, 5, adjoint_cut(k))

            @pl.when(s == 2 * k + 3)
            def _():
                turned(b.relay_t, 4, tangent_cut(k))
                turned(b.relay_a, 5, chunks - adjoint_cut(k))

        @pl.when(s < n - 2)
        def _():
            all_sent(b.sent, carried, 3)


def write_out(dual_in, seen_in, block_in, chain_in, dual, seen, block, chain, sems):
    copies = [
        pltpu.make_async_copy(src, dst, sems.at[i])
        for i, (src, dst) in enumerate(((dual_in, dual), (block_in, block), (chain_in, chain), (seen_in, seen)))
    ]
    for copy in copies:
        copy.start()
    for copy in copies:
        copy.wait()


def shards(
    increment, multiplier, error_var, obs_cell, obs_dual, obs_var,
    level_gain, mean_depth, chain_decay,
):
    n = lax.axis_size("tm")
    size = lax.axis_size("lev")
    if n % 2 or size < 2 or size & (size - 1):
        raise ValueError("unsupported mesh")
    _, fields, levels, rows, cols = increment.shape
    planes = fields * levels
    chunks = planes * pieces(rows)
    rounds = size.bit_length() - 1
    tall = 2 * rows + PAD

    def room(*shape):
        return pltpu.VMEM(shape, jnp.float32)

    def flags(count):
        return pltpu.SemaphoreType.DMA((count,))

    scratch = [
        *[room(planes, rows + 2 * PAD, cols)] * 4,
        *[room(planes, rows, cols)] * 5, *[room(chunks, rows // pieces(rows), cols)] * 2,
        room(2, tall, cols), room(rounds, tall, cols), room(tall, cols),
        room(4, rows + 2 * PAD, cols), room(levels, rows, cols),
        *[room(planes, 1, 128)] * 3,
        pltpu.VMEM(obs_cell.shape, jnp.int32), room(*obs_dual.shape), room(*obs_var.shape),
        pltpu.SMEM(level_gain.shape, jnp.float32), pltpu.SMEM(mean_depth.shape, jnp.float32),
        pltpu.SMEM((1, levels, fields), jnp.float32),
    ]
    sems = [
        flags(6), *[flags(planes)] * 2, *[flags(chunks)] * 5,
        flags(2), flags(2), flags(6), flags(rounds + 1), flags(rounds + 1),
    ]

    def scoped(*refs):
        pl.run_scoped(lambda *scope: kernel(n, size, *refs, *scope), *sems)

    place = pl.BlockSpec(memory_space=pl.ANY)
    small = pl.BlockSpec(memory_space=pltpu.VMEM)
    held = pltpu.VMEM((planes, rows, cols), jnp.float32)
    results = pl.pallas_call(
        scoped,
        out_shape=[held, pltpu.VMEM(obs_dual.shape, jnp.float32), held, held],
        in_specs=[place] * 9,
        out_specs=[small] * 4,
        scratch_shapes=scratch,
        compiler_params=pltpu.CompilerParams(
            collective_id=0, has_side_effects=True, vmem_limit_bytes=50 * 1024 * 1024
        ),
    )(
        increment, multiplier, error_var, obs_cell, obs_dual, obs_var,
        level_gain, mean_depth, jnp.swapaxes(chain_decay, 1, 2),
    )
    dual, seen, block, chain = pl.pallas_call(
        write_out,
        out_shape=[jax.ShapeDtypeStruct(r.shape, jnp.float32) for r in results],
        in_specs=[small] * 4,
        out_specs=[place] * 4,
        scratch_shapes=[flags(4)],
        compiler_params=pltpu.CompilerParams(vmem_limit_bytes=1024 * 1024),
    )(*[pltpu.with_memory_space_constraint(r, pltpu.VMEM) for r in results])
    return (
        dual.reshape(increment.shape), seen, block.reshape(increment.shape), chain.reshape(increment.shape),
    )


def solution(mesh):
    state = P("tm", None, "lev", None, None)
    obs = P("tm", "lev", None)
    return jax.shard_map(
        shards,
        mesh=mesh,
        in_specs=(state, state, state, obs, obs, obs, P("lev"), P("lev"), P("tm", None, "lev")),
        out_specs=(state, obs, state, state),
        check_vma=False,
    )
```

```python
from typing import Any, NamedTuple

import jax
import jax.numpy as jnp
from jax import lax
from jax.experimental import pallas as pl
from jax.experimental.pallas import tpu as pltpu
from jax.sharding import PartitionSpec as P

TIME_STEP = 0.25
ROTATION_PARAM = 0.5
COUPLING = 0.25
HALF = TIME_STEP * ROTATION_PARAM
SPLIT = 4
PAD = 8
MESH_ID = pl.DeviceIdType.MESH


class Scratch(NamedTuple):
    inc: Any
    mult: Any
    work: Any
    b1: Any
    own: Any
    swap: Any
    tangent: Any
    adjoint: Any
    sent: Any
    relay_t: Any
    relay_a: Any
    sums: Any
    met: Any
    total: Any
    columns: Any
    added: Any
    decay: Any
    decay_in: Any
    decay_relay: Any
    cells: Any
    obs_dual: Any
    obs_var: Any
    gain: Any
    depth: Any
    chain_decay: Any
    sends: Any
    own_recv: Any
    loads: Any
    tan_recv: Any
    adj_recv: Any
    rt_recv: Any
    ra_recv: Any
    ch_recv: Any
    decay_send: Any
    decay_recv: Any
    small_loads: Any
    lev_send: Any
    lev_recv: Any


def pieces(rows):
    return SPLIT if rows % (8 * SPLIT) == 0 else 1


def block_rows(rows):
    part = rows // pieces(rows)
    return next(b for b in (32, 16, 8, part) if part % b == 0)


def up_y(a):
    lane = lax.broadcasted_iota(jnp.int32, a.shape, 1)
    return jnp.where(lane == a.shape[1] - 1, 0.0, pltpu.roll(a, a.shape[1] - 1, 1))


def down_y(a):
    lane = lax.broadcasted_iota(jnp.int32, a.shape, 1)
    return jnp.where(lane == 0, 0.0, pltpu.roll(a, 1, 1))


def up_x(a):
    return pltpu.roll(a, a.shape[0] - 1, 0)


def down_x(a):
    return pltpu.roll(a, 1, 0)


def kernel(
    n, size, increment, multiplier, error_var, cell_at, obs_dual_at, obs_var_at, gain_at, depth_at,
    decay_at, tangent_in, obs_out, adjoint_in, carried, *scratch,
):
    b = Scratch(*scratch)
    obs_cell, obs_dual, obs_var = b.cells, b.obs_dual, b.obs_var
    level_gain, mean_depth, chain_decay = b.gain, b.depth, b.chain_decay
    fields, levels, rows, cols = increment.shape[1:]
    planes = fields * levels
    per = pieces(rows)
    chunks = planes * per
    part = rows // per
    step = block_rows(rows)
    wide = step + 2 * PAD

    s = lax.axis_index("tm")
    lev = lax.axis_index("lev")
    odd = s % 2
    even = odd == 0
    pair = s // 2
    pairs = n // 2
    partner = s + 1 - 2 * odd

    def adjoint_cut(k):
        return chunks * (pairs - 1 - k) // pairs

    def tangent_cut(k):
        return chunks * (k + 1) // max(pairs - 1, 1)

    def loop(low, high, fn):
        lax.fori_loop(low, high, lambda c, z: (fn(c), z)[1], 0)

    def where_in(c):
        return c // per, pl.ds(pl.multiple_of((c % per) * part, 8), part)

    def piece(ref, c):
        p, r = where_in(c)
        return ref.at[p, r, :]

    def remote(src, dst, send, recv, where):
        return pltpu.make_async_remote_copy(
            src_ref=src, dst_ref=dst, send_sem=send, recv_sem=recv, device_id=where, device_id_type=MESH_ID,
        )

    def move(src, dst, send, recv, c, to):
        return remote(piece(src, c), piece(dst, c), send, recv.at[c], {"tm": to})

    def lev_move(src, dst, i, to):
        return remote(src, dst, b.lev_send.at[i], b.lev_recv.at[i], {"lev": to})

    def own_copy(c):
        return remote(piece(b.own, c), piece(b.swap, c), b.sends.at[0], b.own_recv.at[c // per], {"tm": partner})

    def own_plane(p):
        return remote(b.own.at[p], b.swap.at[p], b.sends.at[0], b.own_recv.at[p], {"tm": partner})

    def all_sent(src, dst, i):
        remote(src, dst, b.sends.at[i], b.own_recv.at[0], {"tm": partner}).wait_send()

    def tangent_copy(c):
        return move(b.tangent, tangent_in, b.sends.at[1], b.tan_recv, c, s + 1)

    def adjoint_copy(c):
        return move(b.adjoint, adjoint_in, b.sends.at[2], b.adj_recv, c, s - 1)

    def chain_copy(c):
        return move(b.sent, carried, b.sends.at[3], b.ch_recv, c, s + 2)

    def tangent_leg(c, to):
        return remote(piece(b.tangent, c), b.relay_t.at[c], b.sends.at[1], b.rt_recv.at[c], {"tm": to})

    def tangent_turn(c, to):
        return remote(b.relay_t.at[c], piece(tangent_in, c), b.sends.at[4], b.tan_recv.at[c], {"tm": to})

    def adjoint_leg(c, to):
        return remote(piece(b.adjoint, c), b.relay_a.at[c], b.sends.at[2], b.ra_recv.at[c], {"tm": to})

    def adjoint_turn(c, to):
        return remote(b.relay_a.at[c], piece(adjoint_in, c), b.sends.at[5], b.adj_recv.at[c], {"tm": to})

    decay_copy = remote(b.decay, b.decay_in, b.decay_send.at[0], b.decay_recv.at[0], {"tm": s - 1})
    decay_leg = remote(b.decay, b.decay_relay, b.decay_send.at[0], b.decay_recv.at[1], {"tm": s - 2})
    decay_turn = remote(b.decay_relay, b.decay_in, b.decay_send.at[1], b.decay_recv.at[0], {"tm": s + 1})
    turns = jnp.logical_and(even, s < n - 2)

    def load(i, p, low, high, sem):
        src = (increment, multiplier, error_var)[i]
        dst = (b.inc, b.mult, b.work)[i]
        return pltpu.make_async_copy(
            src.at[0, p // levels, p % levels, pl.ds(low, high - low), :],
            dst.at[p, pl.ds(PAD + low, high - low), :], b.loads.at[sem],
        )

    def loaded(low, high, sem):
        pltpu.make_async_copy(
            increment.at[0, :, 0, pl.ds(low, high - low), :],
            b.inc.at[pl.ds(0, fields), pl.ds(PAD + low, high - low), :], b.loads.at[sem],
        ).wait()

    barrier = pltpu.get_barrier_semaphore()
    near = ((s >= 0, partner), (s >= 2, s - 2), (s < n - 2, s + 2))
    for there, who in near:
        @pl.when(there)
        def _():
            pl.semaphore_signal(barrier, inc=1, device_id={"tm": who}, device_id_type=MESH_ID)
    bits = []
    bit = 1
    while bit < size:
        bits.append(bit)
        bit *= 2

    def across(bit):
        return lev + bit - 2 * bit * ((lev // bit) % 2)

    for bit in bits:
        pl.semaphore_signal(barrier, inc=1, device_id={"lev": across(bit)}, device_id_type=MESH_ID)

    small_loads = [
        pltpu.make_async_copy(src, dst, b.small_loads.at[i])
        for i, (src, dst) in enumerate((
            (decay_at, chain_decay), (gain_at, level_gain), (depth_at, mean_depth),
            (cell_at, obs_cell), (obs_dual_at, obs_dual), (obs_var_at, obs_var),
        ))
    ]
    for i in range(3):
        load(i, 0, 0, part, planes).start()
    small_loads[0].start()
    for p in range(planes):
        low = part if p == 0 else 0
        if low < rows:
            for i in range(3):
                load(i, p, low, rows, p).start()
    for copy in small_loads[1:]:
        copy.start()

    def edges(ref, planes):
        zero = jnp.zeros((PAD, cols), jnp.float32)
        for p in range(planes):
            ref[p, pl.ds(0, PAD), :] = zero
            ref[p, pl.ds(PAD + rows, PAD), :] = zero

    def own_at(c):
        p, r = where_in(c)

        if isinstance(c, int):
            if c == 0:
                loaded(0, part, planes)
            elif c == 1 and per > 1:
                loaded(part, rows, 0)
            else:
                loaded(0, rows, p)
        else:
            @pl.when(c % per == 0)
            def _():
                loaded(0, rows, p)

        inner = pl.ds(pl.multiple_of((c % per) * part + PAD, 8), part)
        b.own[p, r, :] = b.work[p, inner, :] * b.mult[p, inner, :] + b.inc[p, inner, :]

    gives_own = jnp.logical_or(even, s < n - 1)

    def give_own(c):
        @pl.when(gives_own)
        def _():
            own_copy(c).start()

    with jax.named_scope("greet"):
        own_at(0)
        pl.semaphore_wait(barrier, len(bits) + sum(there.astype(jnp.int32) for there, _ in near))

    def own_next(c):
        own_at(c)
        give_own(c - 1)

    with jax.named_scope("own"):
        give_own(0)
        own_at(1)
        small_loads[0].wait()
        for f in range(fields):
            for l in range(levels):
                b.decay[f * levels + l] = jnp.full((1, 128), chain_decay[0, l, f], jnp.float32)

        @pl.when(odd == 1)
        def _():
            decay_copy.start()

        @pl.when(jnp.logical_and(even, s >= 2))
        def _():
            decay_leg.start()

        loop(2, chunks, own_next)
        give_own(chunks - 1)

    for copy in small_loads[1:]:
        copy.wait()
    for ref in (b.inc, b.mult, b.work, b.b1):
        edges(ref, planes)
    edges(b.columns, 4)

    def row_index(r0):
        return lax.broadcasted_iota(jnp.int32, (wide, cols), 0) + (r0 - PAD)

    def forward(h, u, v, column, r0, gain, depth):
        p = gain * h
        if column is not None:
            p = p + COUPLING * column
        u_new = u + TIME_STEP * (ROTATION_PARAM * v - (up_x(p) - p))
        v_new = v - TIME_STEP * (ROTATION_PARAM * u + (up_y(p) - p))
        u_new = jnp.where(row_index(r0) < 0, 0.0, u_new)
        h_new = h - TIME_STEP * depth * ((u_new - down_x(u_new)) + (v_new - down_y(v_new)))
        return h_new, u_new, v_new

    def back(h, u, v, r0, gain, depth):
        w = depth * h
        u2 = u + TIME_STEP * (up_x(w) - w)
        v2 = v + TIME_STEP * (up_y(w) - w)
        u2 = jnp.where(row_index(r0) < 0, 0.0, u2)
        p = TIME_STEP * ((u2 - down_x(u2)) + (v2 - down_y(v2)))
        return h + gain * p, u2 - HALF * v2, v2 + HALF * u2, p

    def middle(a):
        return a[PAD:PAD + step]

    def state_at(ref, l, r0):
        at = pl.ds(r0, wide)
        return ref[l, at, :], ref[levels + l, at, :], ref[2 * levels + l, at, :]

    def sweep(fn):
        loop(0, rows // step, lambda i: fn(pl.multiple_of(i * step, 8)))

    def put(ref, l, r0, values):
        for f, value in enumerate(values):
            ref[f * levels + l, pl.ds(r0, step), :] = middle(value)

    def put_padded(ref, l, r0, values):
        put(ref, l, r0 + PAD, values)

    sums = b.sums

    def ahead(r0):
        c0 = c1 = None
        for l in range(levels):
            h, u, v = state_at(b.inc, l, r0)
            h_new, _, _ = forward(h, u, v, None, r0, level_gain[l], mean_depth[l])
            c0 = middle(h) if c0 is None else c0 + middle(h)
            c1 = middle(h_new) if c1 is None else c1 + middle(h_new)
        sums[0, pl.ds(r0, step), :] = c0
        sums[0, pl.ds(rows + r0, step), :] = c1

    def behind(source, to):
        def fn(r0):
            bar = None
            for l in range(levels):
                h, u, v = state_at(source, l, r0)
                h2, u2, v2, p = back(h, u, v, r0, level_gain[l], mean_depth[l])
                if to == 0:
                    put_padded(b.b1, l, r0, (h2, u2, v2))
                bar = middle(p) if bar is None else bar + middle(p)
            sums[1, pl.ds(to * rows + r0, step), :] = COUPLING * bar
        return fn

    with jax.named_scope("ahead"):
        sweep(ahead)
    with jax.named_scope("behind"):
        sweep(behind(b.mult, 0))
        sweep(behind(b.b1, 1))
    depth_sum = mean_depth[0]
    for l in range(1, levels):
        depth_sum = depth_sum + mean_depth[l]
    for k in range(2):
        sums[k, pl.ds(2 * rows, PAD), :] = jnp.full((PAD, cols), depth_sum, jnp.float32)

    half = lev % 2
    tall = 2 * rows + PAD
    total = b.total

    def meet_copy():
        return lev_move(sums.at[1 - half], b.met.at[0], 0, across(1))

    def add_met(slot, first):
        def fn(r0):
            at = pl.ds(r0, PAD)
            kept = sums[half, at, :] if first else total[at, :]
            total[at, :] = kept + b.met[slot, at, :]
        loop(0, tall // PAD, lambda i: fn(pl.multiple_of(i * PAD, 8)))

    meet = meet_copy()
    with jax.named_scope("meet"):
        meet.start()
        meet.wait()
        add_met(0, True)

    def observe():
        count = obs_cell.shape[2]
        if cols & (cols - 1) == 0:
            shift = cols.bit_length() - 1

            def split(cells):
                return cells >> shift, cells & (cols - 1)
        else:
            def split(cells):
                return lax.div(cells, cols), lax.rem(cells, cols)

        row = lax.broadcasted_iota(jnp.int32, (rows, count), 0)
        col = lax.broadcasted_iota(jnp.int32, (cols, count), 0)
        for l in range(levels):
            at_row, at_col = split(obs_cell[0, pl.ds(l, 1), :])
            values = obs_dual[0, pl.ds(l, 1), :]
            hit_row = jnp.where(row == at_row, 1.0, 0.0)
            hit_col = jnp.where(col == at_col, 1.0, 0.0)
            seen = lax.dot_general(
                b.inc[l, pl.ds(PAD, rows), :], hit_col, (((1,), (0,)), ((), ())),
                precision=lax.Precision.HIGHEST, preferred_element_type=jnp.float32,
            )
            picked = jnp.sum(hit_row * seen, axis=0, keepdims=True)
            obs_out[0, pl.ds(l, 1), :] = obs_var[0, pl.ds(l, 1), :] * values + picked
            b.added[l] = lax.dot_general(
                hit_row * values, hit_col, (((1,), (1,)), ((), ())),
                precision=lax.Precision.HIGHEST, preferred_element_type=jnp.float32,
            )

    for i, bit in enumerate(bits[1:], 1):
        far = lev_move(total, b.met.at[i], i, across(bit))
        far.start()
        if i == 1:
            with jax.named_scope("observe"):
                observe()
        with jax.named_scope("far"):
            far.wait()
            add_met(i, False)
    if len(bits) < 2:
        observe()

    columns = b.columns

    def first_column(r0):
        columns[2 * half, pl.ds(r0 + PAD, step), :] = total[pl.ds(r0, step), :]

    def second_column(r0):
        c = columns[2 * half, pl.ds(r0, wide), :]
        gx = jnp.where(row_index(r0) < 0, 0.0, up_x(c) - c)
        gy = up_y(c) - c
        lap = (gx - down_x(gx)) + (gy - down_y(gy))
        scale = (TIME_STEP * TIME_STEP * COUPLING) * total[pl.ds(2 * rows, 1), pl.ds(0, 1)]
        columns[2 * half + 1, pl.ds(r0 + PAD, step), :] = total[pl.ds(rows + r0, step), :] + scale * middle(lap)

    with jax.named_scope("column"):
        sweep(first_column)
        sweep(second_column)
    mine = columns.at[pl.ds(2 * half, 2)]
    near_copy = lev_move(mine, mine, len(bits), across(1))
    with jax.named_scope("near"):
        near_copy.start()
        near_copy.wait()

    def last_back(r0):
        at = pl.ds(r0, wide)
        bar0, bar1 = columns[2, at, :], columns[3, at, :]
        for l in range(levels):
            h, u, v = state_at(b.b1, l, r0)
            h2, u2, v2, _ = back(h + bar0, u, v, r0, level_gain[l], mean_depth[l])
            put(b.adjoint, l, r0, (h2 + bar1, u2, v2))

    def first_forward(r0):
        column = columns[0, pl.ds(r0, wide), :]
        for l in range(levels):
            h, u, v = state_at(b.inc, l, r0)
            put_padded(b.work, l, r0, forward(h, u, v, column, r0, level_gain[l], mean_depth[l]))

    def last_forward(r0):
        column = columns[1, pl.ds(r0, wide), :]
        for l in range(levels):
            h, u, v = state_at(b.work, l, r0)
            put(b.tangent, l, r0, forward(h, u, v, column, r0, level_gain[l], mean_depth[l]))

    @pl.when(turns)
    def _():
        decay_leg.wait_recv()
        decay_turn.start()

    with jax.named_scope("back"):
        sweep(last_back)
    below = pair - 1
    down_cut = adjoint_cut(below)
    across_cut = adjoint_cut(pair)

    @pl.when(jnp.logical_and(even, s >= 2))
    def _():
        loop(0, down_cut, lambda c: adjoint_leg(c, s - 2).start())
        loop(down_cut, chunks, lambda c: adjoint_leg(c, s + 1).start())

    with jax.named_scope("forward"):
        sweep(first_forward)
        sweep(last_forward)
    up_cut = tangent_cut(pair)
    here_cut = tangent_cut(below)
    climbs = jnp.logical_and(odd == 1, s < n - 1)

    @pl.when(even)
    def _():
        loop(0, chunks, lambda c: tangent_copy(c).start())

    @pl.when(climbs)
    def _():
        loop(0, up_cut, lambda c: tangent_leg(c, s + 2).start())
        loop(up_cut, chunks, lambda c: tangent_leg(c, s - 1).start())

    def chain_step(c):
        p, r = where_in(c)
        d = chain_decay[0, p % levels, p // levels]

        @pl.when(s >= 1)
        def _():
            tangent_copy(c).wait_recv()

        @pl.when(s == 0)
        def _():
            tangent_in[p, r, :] = jnp.zeros((part, cols), jnp.float32)

        @pl.when(s >= 2)
        def _():
            chain_copy(c).wait_recv()

        @pl.when(s < 2)
        def _():
            carried[p, r, :] = jnp.zeros((part, cols), jnp.float32)

        @pl.when(jnp.logical_and(c % per == 0, jnp.logical_or(odd == 1, s < n - 2)))
        def _():
            own_plane(p).wait_recv()

        swap = b.swap[p, r, :]
        product = b.own[p, r, :] - tangent_in[p, r, :]
        here = d * (carried[p, r, :] + jnp.where(odd == 1, swap, 0.0)) + product

        @pl.when(s < n - 2)
        def _():
            d_next = b.decay_in[p][:, :1]
            b.sent[p, r, :] = d_next * here + (jnp.where(even, swap, 0.0) - b.tangent[p, r, :])

        tangent_in[p, r, :] = product
        carried[p, r, :] = here

        @pl.when(s < n - 2)
        def _():
            chain_copy(c).start()

    @pl.when(s == 0)
    def _():
        decay_copy.wait_recv()

    with jax.named_scope("chain0"):
        loop(0, jnp.where(s == 0, chunks, 0), chain_step)

    @pl.when(jnp.logical_and(even, s < n - 2))
    def _():
        def turn_up(c):
            tangent_leg(c, s - 1).wait_recv()
            tangent_turn(c, s + 2).start()

        def turn_across(c):
            adjoint_leg(c, s - 2).wait_recv()
            adjoint_turn(c, s + 1).start()

        with jax.named_scope("turn_up"):
            loop(up_cut, chunks, turn_up)
        with jax.named_scope("turn_over"):
            loop(0, across_cut, turn_across)

    early = jnp.where(s == n - 1, chunks // 2, 0)

    @pl.when(odd == 1)
    def _():
        loop(0, early, lambda c: adjoint_copy(c).start())

        @pl.when(s >= 3)
        def _():
            def turn_across(c):
                tangent_leg(c, s + 2).wait_recv()
                tangent_turn(c, s - 1).start()

            with jax.named_scope("turn_back"):
                loop(0, here_cut, turn_across)

        loop(early, chunks, lambda c: adjoint_copy(c).start())

        @pl.when(s >= 3)
        def _():
            def turn_down(c):
                adjoint_leg(c, s + 1).wait_recv()
                adjoint_turn(c, s - 2).start()

            with jax.named_scope("turn_down"):
                loop(down_cut, chunks, turn_down)

    def block_step(i):
        c = lax.rem(i + across_cut * odd, chunks)
        p, r = where_in(c)
        inner = pl.ds(pl.multiple_of((c % per) * part + PAD, 8), part)

        @pl.when(s < n - 1)
        def _():
            adjoint_copy(c).wait_recv()

        kept = b.mult[p, inner, :] - jnp.where(s < n - 1, adjoint_in[p, r, :], 0.0)
        adjoint_in[p, r, :] = kept

        @pl.when(p < levels)
        def _():
            adjoint_in[p, r, :] = kept + b.added[jnp.minimum(p, levels - 1), r, :]

    loop(0, jnp.where(s == n - 1, chunks, 0), block_step)

    @pl.when(jnp.logical_and(s > 0, s < n - 1))
    def _():
        decay_copy.wait_recv()

    with jax.named_scope("chain"):
        loop(0, jnp.where(s == 0, 0, chunks), chain_step)

    with jax.named_scope("block"):
        loop(0, jnp.where(s == n - 1, 0, chunks), block_step)

    with jax.named_scope("drain"):
        @pl.when(gives_own)
        def _():
            all_sent(b.own, b.swap, 0)

        @pl.when(s < n - 1)
        def _():
            all_sent(b.tangent, tangent_in, 1)

        @pl.when(s >= 1)
        def _():
            all_sent(b.adjoint, adjoint_in, 2)
            decay_copy.wait_send()

        @pl.when(turns)
        def _():
            decay_turn.wait_send()

        def turned(ref, i, count):
            if count:
                all_sent(ref.at[pl.ds(0, count)], ref.at[pl.ds(0, count)], i)

        for k in range(pairs - 1):
            @pl.when(s == 2 * k)
            def _():
                turned(b.relay_t, 4, chunks - tangent_cut(k))
                turned(b.relay_a, 5, adjoint_cut(k))

            @pl.when(s == 2 * k + 3)
            def _():
                turned(b.relay_t, 4, tangent_cut(k))
                turned(b.relay_a, 5, chunks - adjoint_cut(k))

        @pl.when(s < n - 2)
        def _():
            all_sent(b.sent, carried, 3)


def write_out(dual_in, seen_in, block_in, chain_in, dual, seen, block, chain):
    def copy_all(sems):
        copies = [
            pltpu.make_async_copy(src, dst, sems.at[i])
            for i, (src, dst) in enumerate(((dual_in, dual), (block_in, block), (chain_in, chain), (seen_in, seen)))
        ]
        for copy in copies:
            copy.start()
        for copy in copies:
            copy.wait()

    pl.run_scoped(copy_all, pltpu.SemaphoreType.DMA((4,)))


def shards(
    increment, multiplier, error_var, obs_cell, obs_dual, obs_var,
    level_gain, mean_depth, chain_decay,
):
    n = lax.axis_size("tm")
    size = lax.axis_size("lev")
    if n % 2 or size < 2 or size & (size - 1):
        raise ValueError("unsupported mesh")
    _, fields, levels, rows, cols = increment.shape
    planes = fields * levels
    chunks = planes * pieces(rows)
    rounds = size.bit_length() - 1
    tall = 2 * rows + PAD

    def room(*shape):
        return pltpu.VMEM(shape, jnp.float32)

    def flags(count):
        return pltpu.SemaphoreType.DMA((count,))

    scratch = [
        *[room(planes, rows + 2 * PAD, cols)] * 4,
        *[room(planes, rows, cols)] * 5, *[room(chunks, rows // pieces(rows), cols)] * 2,
        room(2, tall, cols), room(rounds, tall, cols), room(tall, cols),
        room(4, rows + 2 * PAD, cols), room(levels, rows, cols),
        *[room(planes, 1, 128)] * 3,
        pltpu.VMEM(obs_cell.shape, jnp.int32), room(*obs_dual.shape), room(*obs_var.shape),
        pltpu.SMEM(level_gain.shape, jnp.float32), pltpu.SMEM(mean_depth.shape, jnp.float32),
        pltpu.SMEM((1, levels, fields), jnp.float32),
    ]
    sems = [
        flags(6), flags(planes), flags(planes + 1), *[flags(chunks)] * 5,
        flags(2), flags(2), flags(6), flags(rounds + 1), flags(rounds + 1),
    ]

    def scoped(*refs):
        pl.run_scoped(lambda *scope: kernel(n, size, *refs, *scope), *sems)

    place = pl.BlockSpec(memory_space=pl.ANY)
    small = pl.BlockSpec(memory_space=pltpu.VMEM)
    held = pltpu.VMEM((planes, rows, cols), jnp.float32)
    results = pl.pallas_call(
        scoped,
        out_shape=[held, pltpu.VMEM(obs_dual.shape, jnp.float32), held, held],
        in_specs=[place] * 9,
        out_specs=[small] * 4,
        scratch_shapes=scratch,
        compiler_params=pltpu.CompilerParams(
            collective_id=0, has_side_effects=True, vmem_limit_bytes=50 * 1024 * 1024
        ),
    )(
        increment, multiplier, error_var, obs_cell, obs_dual, obs_var,
        level_gain, mean_depth, jnp.swapaxes(chain_decay, 1, 2),
    )
    dual, seen, block, chain = pl.pallas_call(
        write_out,
        out_shape=[jax.ShapeDtypeStruct(r.shape, jnp.float32) for r in results],
        in_specs=[small] * 4,
        out_specs=[place] * 4,
        compiler_params=pltpu.CompilerParams(vmem_limit_bytes=1024 * 1024),
    )(*[pltpu.with_memory_space_constraint(r, pltpu.VMEM) for r in results])
    return (
        dual.reshape(increment.shape), seen, block.reshape(increment.shape), chain.reshape(increment.shape),
    )


def solution(mesh):
    state = P("tm", None, "lev", None, None)
    obs = P("tm", "lev", None)
    return jax.shard_map(
        shards,
        mesh=mesh,
        in_specs=(state, state, state, obs, obs, obs, P("lev"), P("lev"), P("tm", None, "lev")),
        out_specs=(state, obs, state, state),
        check_vma=False,
    )
```

```python
from typing import Any, NamedTuple

import jax
import jax.numpy as jnp
from jax import lax
from jax.experimental import pallas as pl
from jax.experimental.pallas import tpu as pltpu
from jax.sharding import PartitionSpec as P

TIME_STEP = 0.25
ROTATION_PARAM = 0.5
COUPLING = 0.25
HALF = TIME_STEP * ROTATION_PARAM
SPLIT = 8
PAD = 8
MESH_ID = pl.DeviceIdType.MESH


class Scratch(NamedTuple):
    inc: Any
    mult: Any
    work: Any
    b1: Any
    own: Any
    swap: Any
    tangent: Any
    adjoint: Any
    sent: Any
    relay_t: Any
    relay_a: Any
    sums: Any
    met: Any
    total: Any
    columns: Any
    added: Any
    decay: Any
    decay_in: Any
    decay_relay: Any
    cells: Any
    obs_dual: Any
    obs_var: Any
    gain: Any
    depth: Any
    chain_decay: Any
    sends: Any
    own_recv: Any
    loads: Any
    tan_recv: Any
    adj_recv: Any
    rt_recv: Any
    ra_recv: Any
    ch_recv: Any
    decay_send: Any
    decay_recv: Any
    small_loads: Any
    lev_send: Any
    lev_recv: Any


def pieces(rows):
    return SPLIT if rows % (8 * SPLIT) == 0 else 1


def block_rows(rows):
    part = rows // pieces(rows)
    return next(b for b in (32, 16, 8, part) if part % b == 0)


def up_y(a):
    lane = lax.broadcasted_iota(jnp.int32, a.shape, 1)
    return jnp.where(lane == a.shape[1] - 1, 0.0, pltpu.roll(a, a.shape[1] - 1, 1))


def down_y(a):
    lane = lax.broadcasted_iota(jnp.int32, a.shape, 1)
    return jnp.where(lane == 0, 0.0, pltpu.roll(a, 1, 1))


def up_x(a):
    return pltpu.roll(a, a.shape[0] - 1, 0)


def down_x(a):
    return pltpu.roll(a, 1, 0)


def kernel(
    n, size, increment, multiplier, error_var, cell_at, obs_dual_at, obs_var_at, gain_at, depth_at,
    decay_at, tangent_in, obs_out, adjoint_in, carried, *scratch,
):
    b = Scratch(*scratch)
    obs_cell, obs_dual, obs_var = b.cells, b.obs_dual, b.obs_var
    level_gain, mean_depth, chain_decay = b.gain, b.depth, b.chain_decay
    fields, levels, rows, cols = increment.shape[1:]
    planes = fields * levels
    per = pieces(rows)
    chunks = planes * per
    part = rows // per
    step = block_rows(rows)
    wide = step + 2 * PAD

    s = lax.axis_index("tm")
    lev = lax.axis_index("lev")
    odd = s % 2
    even = odd == 0
    pair = s // 2
    pairs = n // 2
    partner = s + 1 - 2 * odd

    def adjoint_cut(k):
        return chunks * (pairs - 1 - k) // pairs

    def tangent_cut(k):
        return chunks * (k + 1) // max(pairs - 1, 1)

    def loop(low, high, fn):
        lax.fori_loop(low, high, lambda c, z: (fn(c), z)[1], 0)

    def where_in(c):
        return c // per, pl.ds(pl.multiple_of((c % per) * part, 8), part)

    def piece(ref, c):
        p, r = where_in(c)
        return ref.at[p, r, :]

    def remote(src, dst, send, recv, where):
        return pltpu.make_async_remote_copy(
            src_ref=src, dst_ref=dst, send_sem=send, recv_sem=recv, device_id=where, device_id_type=MESH_ID,
        )

    def move(src, dst, send, recv, c, to):
        return remote(piece(src, c), piece(dst, c), send, recv.at[c], {"tm": to})

    def lev_move(src, dst, i, to):
        return remote(src, dst, b.lev_send.at[i], b.lev_recv.at[i], {"lev": to})

    def own_copy(c):
        return remote(piece(b.own, c), piece(b.swap, c), b.sends.at[0], b.own_recv.at[c // per], {"tm": partner})

    def own_plane(p):
        return remote(b.own.at[p], b.swap.at[p], b.sends.at[0], b.own_recv.at[p], {"tm": partner})

    def all_sent(src, dst, i):
        remote(src, dst, b.sends.at[i], b.own_recv.at[0], {"tm": partner}).wait_send()

    def tangent_copy(c):
        return move(b.tangent, tangent_in, b.sends.at[1], b.tan_recv, c, s + 1)

    def adjoint_copy(c):
        return move(b.adjoint, adjoint_in, b.sends.at[2], b.adj_recv, c, s - 1)

    def chain_copy(c):
        return move(b.sent, carried, b.sends.at[3], b.ch_recv, c, s + 2)

    def tangent_leg(c, to):
        return remote(piece(b.tangent, c), b.relay_t.at[c], b.sends.at[1], b.rt_recv.at[c], {"tm": to})

    def tangent_turn(c, to):
        return remote(b.relay_t.at[c], piece(tangent_in, c), b.sends.at[4], b.tan_recv.at[c], {"tm": to})

    def adjoint_leg(c, to):
        return remote(piece(b.adjoint, c), b.relay_a.at[c], b.sends.at[2], b.ra_recv.at[c], {"tm": to})

    def adjoint_turn(c, to):
        return remote(b.relay_a.at[c], piece(adjoint_in, c), b.sends.at[5], b.adj_recv.at[c], {"tm": to})

    decay_copy = remote(b.decay, b.decay_in, b.decay_send.at[0], b.decay_recv.at[0], {"tm": s - 1})
    decay_leg = remote(b.decay, b.decay_relay, b.decay_send.at[0], b.decay_recv.at[1], {"tm": s - 2})
    decay_turn = remote(b.decay_relay, b.decay_in, b.decay_send.at[1], b.decay_recv.at[0], {"tm": s + 1})
    turns = jnp.logical_and(even, s < n - 2)

    def load(i, p, low, high, sem):
        src = (increment, multiplier, error_var)[i]
        dst = (b.inc, b.mult, b.work)[i]
        return pltpu.make_async_copy(
            src.at[0, p // levels, p % levels, pl.ds(low, high - low), :],
            dst.at[p, pl.ds(PAD + low, high - low), :], b.loads.at[sem],
        )

    def loaded(low, high, sem):
        pltpu.make_async_copy(
            increment.at[0, :, 0, pl.ds(low, high - low), :],
            b.inc.at[pl.ds(0, fields), pl.ds(PAD + low, high - low), :], b.loads.at[sem],
        ).wait()

    barrier = pltpu.get_barrier_semaphore()
    near = ((s >= 0, partner), (s >= 2, s - 2), (s < n - 2, s + 2))
    for there, who in near:
        @pl.when(there)
        def _():
            pl.semaphore_signal(barrier, inc=1, device_id={"tm": who}, device_id_type=MESH_ID)
    bits = []
    bit = 1
    while bit < size:
        bits.append(bit)
        bit *= 2

    def across(bit):
        return lev + bit - 2 * bit * ((lev // bit) % 2)

    for bit in bits:
        pl.semaphore_signal(barrier, inc=1, device_id={"lev": across(bit)}, device_id_type=MESH_ID)

    small_loads = [
        pltpu.make_async_copy(src, dst, b.small_loads.at[i])
        for i, (src, dst) in enumerate((
            (decay_at, chain_decay), (gain_at, level_gain), (depth_at, mean_depth),
            (cell_at, obs_cell), (obs_dual_at, obs_dual), (obs_var_at, obs_var),
        ))
    ]
    for i in range(3):
        load(i, 0, 0, part, planes).start()
    small_loads[0].start()
    for p in range(planes):
        low = part if p == 0 else 0
        if low < rows:
            for i in range(3):
                load(i, p, low, rows, p).start()
    for copy in small_loads[1:]:
        copy.start()

    def edges(ref, planes):
        zero = jnp.zeros((PAD, cols), jnp.float32)
        for p in range(planes):
            ref[p, pl.ds(0, PAD), :] = zero
            ref[p, pl.ds(PAD + rows, PAD), :] = zero

    def own_at(c):
        p, r = where_in(c)

        if isinstance(c, int):
            if c == 0:
                loaded(0, part, planes)
            elif c == 1 and per > 1:
                loaded(part, rows, 0)
            else:
                loaded(0, rows, p)
        else:
            @pl.when(c % per == 0)
            def _():
                loaded(0, rows, p)

        inner = pl.ds(pl.multiple_of((c % per) * part + PAD, 8), part)
        b.own[p, r, :] = b.work[p, inner, :] * b.mult[p, inner, :] + b.inc[p, inner, :]

    gives_own = jnp.logical_or(even, s < n - 1)

    def give_own(c):
        @pl.when(gives_own)
        def _():
            own_copy(c).start()

    with jax.named_scope("greet"):
        own_at(0)
        pl.semaphore_wait(barrier, len(bits) + sum(there.astype(jnp.int32) for there, _ in near))

    def own_next(c):
        own_at(c)
        give_own(c - 1)

    with jax.named_scope("own"):
        give_own(0)
        own_at(1)
        small_loads[0].wait()
        for f in range(fields):
            for l in range(levels):
                b.decay[f * levels + l] = jnp.full((1, 128), chain_decay[0, l, f], jnp.float32)

        @pl.when(odd == 1)
        def _():
            decay_copy.start()

        @pl.when(jnp.logical_and(even, s >= 2))
        def _():
            decay_leg.start()

        loop(2, chunks, own_next)
        give_own(chunks - 1)

    for copy in small_loads[1:]:
        copy.wait()
    for ref in (b.inc, b.mult, b.work, b.b1):
        edges(ref, planes)
    edges(b.columns, 4)

    def row_index(r0):
        return lax.broadcasted_iota(jnp.int32, (wide, cols), 0) + (r0 - PAD)

    def forward(h, u, v, column, r0, gain, depth):
        p = gain * h
        if column is not None:
            p = p + COUPLING * column
        u_new = u + TIME_STEP * (ROTATION_PARAM * v - (up_x(p) - p))
        v_new = v - TIME_STEP * (ROTATION_PARAM * u + (up_y(p) - p))
        u_new = jnp.where(row_index(r0) < 0, 0.0, u_new)
        h_new = h - TIME_STEP * depth * ((u_new - down_x(u_new)) + (v_new - down_y(v_new)))
        return h_new, u_new, v_new

    def back(h, u, v, r0, gain, depth):
        w = depth * h
        u2 = u + TIME_STEP * (up_x(w) - w)
        v2 = v + TIME_STEP * (up_y(w) - w)
        u2 = jnp.where(row_index(r0) < 0, 0.0, u2)
        p = TIME_STEP * ((u2 - down_x(u2)) + (v2 - down_y(v2)))
        return h + gain * p, u2 - HALF * v2, v2 + HALF * u2, p

    def middle(a):
        return a[PAD:PAD + step]

    def state_at(ref, l, r0):
        at = pl.ds(r0, wide)
        return ref[l, at, :], ref[levels + l, at, :], ref[2 * levels + l, at, :]

    def sweep(fn):
        loop(0, rows // step, lambda i: fn(pl.multiple_of(i * step, 8)))

    def put(ref, l, r0, values):
        for f, value in enumerate(values):
            ref[f * levels + l, pl.ds(r0, step), :] = middle(value)

    def put_padded(ref, l, r0, values):
        put(ref, l, r0 + PAD, values)

    sums = b.sums

    def ahead(r0):
        c0 = c1 = None
        for l in range(levels):
            h, u, v = state_at(b.inc, l, r0)
            h_new, _, _ = forward(h, u, v, None, r0, level_gain[l], mean_depth[l])
            c0 = middle(h) if c0 is None else c0 + middle(h)
            c1 = middle(h_new) if c1 is None else c1 + middle(h_new)
        sums[0, pl.ds(r0, step), :] = c0
        sums[0, pl.ds(rows + r0, step), :] = c1

    def behind(source, to):
        def fn(r0):
            bar = None
            for l in range(levels):
                h, u, v = state_at(source, l, r0)
                h2, u2, v2, p = back(h, u, v, r0, level_gain[l], mean_depth[l])
                if to == 0:
                    put_padded(b.b1, l, r0, (h2, u2, v2))
                bar = middle(p) if bar is None else bar + middle(p)
            sums[1, pl.ds(to * rows + r0, step), :] = COUPLING * bar
        return fn

    with jax.named_scope("ahead"):
        sweep(ahead)
    with jax.named_scope("behind"):
        sweep(behind(b.mult, 0))
        sweep(behind(b.b1, 1))
    depth_sum = mean_depth[0]
    for l in range(1, levels):
        depth_sum = depth_sum + mean_depth[l]
    for k in range(2):
        sums[k, pl.ds(2 * rows, PAD), :] = jnp.full((PAD, cols), depth_sum, jnp.float32)

    half = lev % 2
    tall = 2 * rows + PAD
    total = b.total

    def meet_copy():
        return lev_move(sums.at[1 - half], b.met.at[0], 0, across(1))

    def add_met(slot, first):
        def fn(r0):
            at = pl.ds(r0, PAD)
            kept = sums[half, at, :] if first else total[at, :]
            total[at, :] = kept + b.met[slot, at, :]
        loop(0, tall // PAD, lambda i: fn(pl.multiple_of(i * PAD, 8)))

    meet = meet_copy()
    with jax.named_scope("meet"):
        meet.start()
        meet.wait()
        add_met(0, True)

    def observe():
        count = obs_cell.shape[2]
        if cols & (cols - 1) == 0:
            shift = cols.bit_length() - 1

            def split(cells):
                return cells >> shift, cells & (cols - 1)
        else:
            def split(cells):
                return lax.div(cells, cols), lax.rem(cells, cols)

        row = lax.broadcasted_iota(jnp.int32, (rows, count), 0)
        col = lax.broadcasted_iota(jnp.int32, (cols, count), 0)
        for l in range(levels):
            at_row, at_col = split(obs_cell[0, pl.ds(l, 1), :])
            values = obs_dual[0, pl.ds(l, 1), :]
            hit_row = jnp.where(row == at_row, 1.0, 0.0)
            hit_col = jnp.where(col == at_col, 1.0, 0.0)
            seen = lax.dot_general(
                b.inc[l, pl.ds(PAD, rows), :], hit_col, (((1,), (0,)), ((), ())),
                precision=lax.Precision.HIGHEST, preferred_element_type=jnp.float32,
            )
            picked = jnp.sum(hit_row * seen, axis=0, keepdims=True)
            obs_out[0, pl.ds(l, 1), :] = obs_var[0, pl.ds(l, 1), :] * values + picked
            b.added[l] = lax.dot_general(
                hit_row * values, hit_col, (((1,), (1,)), ((), ())),
                precision=lax.Precision.HIGHEST, preferred_element_type=jnp.float32,
            )

    for i, bit in enumerate(bits[1:], 1):
        far = lev_move(total, b.met.at[i], i, across(bit))
        far.start()
        if i == 1:
            with jax.named_scope("observe"):
                observe()
        with jax.named_scope("far"):
            far.wait()
            add_met(i, False)
    if len(bits) < 2:
        observe()

    columns = b.columns

    def first_column(r0):
        columns[2 * half, pl.ds(r0 + PAD, step), :] = total[pl.ds(r0, step), :]

    def second_column(r0):
        c = columns[2 * half, pl.ds(r0, wide), :]
        gx = jnp.where(row_index(r0) < 0, 0.0, up_x(c) - c)
        gy = up_y(c) - c
        lap = (gx - down_x(gx)) + (gy - down_y(gy))
        scale = (TIME_STEP * TIME_STEP * COUPLING) * total[pl.ds(2 * rows, 1), pl.ds(0, 1)]
        columns[2 * half + 1, pl.ds(r0 + PAD, step), :] = total[pl.ds(rows + r0, step), :] + scale * middle(lap)

    with jax.named_scope("column"):
        sweep(first_column)
        sweep(second_column)
    mine = columns.at[pl.ds(2 * half, 2)]
    near_copy = lev_move(mine, mine, len(bits), across(1))
    with jax.named_scope("near"):
        near_copy.start()
        near_copy.wait()

    def last_back(r0):
        at = pl.ds(r0, wide)
        bar0, bar1 = columns[2, at, :], columns[3, at, :]
        for l in range(levels):
            h, u, v = state_at(b.b1, l, r0)
            h2, u2, v2, _ = back(h + bar0, u, v, r0, level_gain[l], mean_depth[l])
            put(b.adjoint, l, r0, (h2 + bar1, u2, v2))

    def first_forward(r0):
        column = columns[0, pl.ds(r0, wide), :]
        for l in range(levels):
            h, u, v = state_at(b.inc, l, r0)
            put_padded(b.work, l, r0, forward(h, u, v, column, r0, level_gain[l], mean_depth[l]))

    def last_forward(r0):
        column = columns[1, pl.ds(r0, wide), :]
        for l in range(levels):
            h, u, v = state_at(b.work, l, r0)
            put(b.tangent, l, r0, forward(h, u, v, column, r0, level_gain[l], mean_depth[l]))

    @pl.when(turns)
    def _():
        decay_leg.wait_recv()
        decay_turn.start()

    with jax.named_scope("back"):
        sweep(last_back)
    below = pair - 1
    down_cut = adjoint_cut(below)
    across_cut = adjoint_cut(pair)

    @pl.when(jnp.logical_and(even, s >= 2))
    def _():
        loop(0, down_cut, lambda c: adjoint_leg(c, s - 2).start())
        loop(down_cut, chunks, lambda c: adjoint_leg(c, s + 1).start())

    with jax.named_scope("forward"):
        sweep(first_forward)
        sweep(last_forward)
    up_cut = tangent_cut(pair)
    here_cut = tangent_cut(below)
    climbs = jnp.logical_and(odd == 1, s < n - 1)

    @pl.when(even)
    def _():
        loop(0, chunks, lambda c: tangent_copy(c).start())

    @pl.when(climbs)
    def _():
        loop(0, up_cut, lambda c: tangent_leg(c, s + 2).start())
        loop(up_cut, chunks, lambda c: tangent_leg(c, s - 1).start())

    def chain_step(c):
        p, r = where_in(c)
        d = chain_decay[0, p % levels, p // levels]

        @pl.when(s >= 1)
        def _():
            tangent_copy(c).wait_recv()

        @pl.when(s == 0)
        def _():
            tangent_in[p, r, :] = jnp.zeros((part, cols), jnp.float32)

        @pl.when(s >= 2)
        def _():
            chain_copy(c).wait_recv()

        @pl.when(s < 2)
        def _():
            carried[p, r, :] = jnp.zeros((part, cols), jnp.float32)

        @pl.when(jnp.logical_and(c % per == 0, jnp.logical_or(odd == 1, s < n - 2)))
        def _():
            own_plane(p).wait_recv()

        swap = b.swap[p, r, :]
        product = b.own[p, r, :] - tangent_in[p, r, :]
        here = d * (carried[p, r, :] + jnp.where(odd == 1, swap, 0.0)) + product

        @pl.when(s < n - 2)
        def _():
            d_next = b.decay_in[p][:, :1]
            b.sent[p, r, :] = d_next * here + (jnp.where(even, swap, 0.0) - b.tangent[p, r, :])

        tangent_in[p, r, :] = product
        carried[p, r, :] = here

        @pl.when(s < n - 2)
        def _():
            chain_copy(c).start()

    @pl.when(s == 0)
    def _():
        decay_copy.wait_recv()

    with jax.named_scope("chain0"):
        loop(0, jnp.where(s == 0, chunks, 0), chain_step)

    @pl.when(jnp.logical_and(even, s < n - 2))
    def _():
        def turn_up(c):
            tangent_leg(c, s - 1).wait_recv()
            tangent_turn(c, s + 2).start()

        def turn_across(c):
            adjoint_leg(c, s - 2).wait_recv()
            adjoint_turn(c, s + 1).start()

        with jax.named_scope("turn_up"):
            loop(up_cut, chunks, turn_up)
        with jax.named_scope("turn_over"):
            loop(0, across_cut, turn_across)

    early = jnp.where(s == n - 1, chunks // 2, 0)

    @pl.when(odd == 1)
    def _():
        loop(0, early, lambda c: adjoint_copy(c).start())

        @pl.when(s >= 3)
        def _():
            def turn_across(c):
                tangent_leg(c, s + 2).wait_recv()
                tangent_turn(c, s - 1).start()

            with jax.named_scope("turn_back"):
                loop(0, here_cut, turn_across)

        loop(early, chunks, lambda c: adjoint_copy(c).start())

        @pl.when(s >= 3)
        def _():
            def turn_down(c):
                adjoint_leg(c, s + 1).wait_recv()
                adjoint_turn(c, s - 2).start()

            with jax.named_scope("turn_down"):
                loop(down_cut, chunks, turn_down)

    def block_step(i):
        c = lax.rem(i + across_cut * odd, chunks)
        p, r = where_in(c)
        inner = pl.ds(pl.multiple_of((c % per) * part + PAD, 8), part)

        @pl.when(s < n - 1)
        def _():
            adjoint_copy(c).wait_recv()

        kept = b.mult[p, inner, :] - jnp.where(s < n - 1, adjoint_in[p, r, :], 0.0)
        adjoint_in[p, r, :] = kept

        @pl.when(p < levels)
        def _():
            adjoint_in[p, r, :] = kept + b.added[jnp.minimum(p, levels - 1), r, :]

    loop(0, jnp.where(s == n - 1, chunks, 0), block_step)

    @pl.when(jnp.logical_and(s > 0, s < n - 1))
    def _():
        decay_copy.wait_recv()

    with jax.named_scope("chain"):
        loop(0, jnp.where(s == 0, 0, chunks), chain_step)

    with jax.named_scope("block"):
        loop(0, jnp.where(s == n - 1, 0, chunks), block_step)

    with jax.named_scope("drain"):
        @pl.when(gives_own)
        def _():
            all_sent(b.own, b.swap, 0)

        @pl.when(s < n - 1)
        def _():
            all_sent(b.tangent, tangent_in, 1)

        @pl.when(s >= 1)
        def _():
            all_sent(b.adjoint, adjoint_in, 2)
            decay_copy.wait_send()

        @pl.when(turns)
        def _():
            decay_turn.wait_send()

        def turned(ref, i, count):
            if count:
                all_sent(ref.at[pl.ds(0, count)], ref.at[pl.ds(0, count)], i)

        for k in range(pairs - 1):
            @pl.when(s == 2 * k)
            def _():
                turned(b.relay_t, 4, chunks - tangent_cut(k))
                turned(b.relay_a, 5, adjoint_cut(k))

            @pl.when(s == 2 * k + 3)
            def _():
                turned(b.relay_t, 4, tangent_cut(k))
                turned(b.relay_a, 5, chunks - adjoint_cut(k))

        @pl.when(s < n - 2)
        def _():
            all_sent(b.sent, carried, 3)


def write_out(dual_in, seen_in, block_in, chain_in, dual, seen, block, chain):
    def copy_all(sems):
        copies = [
            pltpu.make_async_copy(src, dst, sems.at[i])
            for i, (src, dst) in enumerate(((dual_in, dual), (block_in, block), (chain_in, chain), (seen_in, seen)))
        ]
        for i, copy in enumerate(copies):
            copy.start(priority=i % 2)
        for copy in copies:
            copy.wait()

    pl.run_scoped(copy_all, pltpu.SemaphoreType.DMA((4,)))


def shards(
    increment, multiplier, error_var, obs_cell, obs_dual, obs_var,
    level_gain, mean_depth, chain_decay,
):
    n = lax.axis_size("tm")
    size = lax.axis_size("lev")
    if n % 2 or size < 2 or size & (size - 1):
        raise ValueError("unsupported mesh")
    _, fields, levels, rows, cols = increment.shape
    planes = fields * levels
    chunks = planes * pieces(rows)
    rounds = size.bit_length() - 1
    tall = 2 * rows + PAD

    def room(*shape):
        return pltpu.VMEM(shape, jnp.float32)

    def flags(count):
        return pltpu.SemaphoreType.DMA((count,))

    scratch = [
        *[room(planes, rows + 2 * PAD, cols)] * 4,
        *[room(planes, rows, cols)] * 5, *[room(chunks, rows // pieces(rows), cols)] * 2,
        room(2, tall, cols), room(rounds, tall, cols), room(tall, cols),
        room(4, rows + 2 * PAD, cols), room(levels, rows, cols),
        *[room(planes, 1, 128)] * 3,
        pltpu.VMEM(obs_cell.shape, jnp.int32), room(*obs_dual.shape), room(*obs_var.shape),
        pltpu.SMEM(level_gain.shape, jnp.float32), pltpu.SMEM(mean_depth.shape, jnp.float32),
        pltpu.SMEM((1, levels, fields), jnp.float32),
    ]
    sems = [
        flags(6), flags(planes), flags(planes + 1), *[flags(chunks)] * 5,
        flags(2), flags(2), flags(6), flags(rounds + 1), flags(rounds + 1),
    ]

    def scoped(*refs):
        pl.run_scoped(lambda *scope: kernel(n, size, *refs, *scope), *sems)

    place = pl.BlockSpec(memory_space=pl.ANY)
    small = pl.BlockSpec(memory_space=pltpu.VMEM)
    held = pltpu.VMEM((planes, rows, cols), jnp.float32)
    results = pl.pallas_call(
        scoped,
        out_shape=[held, pltpu.VMEM(obs_dual.shape, jnp.float32), held, held],
        in_specs=[place] * 9,
        out_specs=[small] * 4,
        scratch_shapes=scratch,
        compiler_params=pltpu.CompilerParams(
            collective_id=0, has_side_effects=True, vmem_limit_bytes=50 * 1024 * 1024
        ),
    )(
        increment, multiplier, error_var, obs_cell, obs_dual, obs_var,
        level_gain, mean_depth, jnp.swapaxes(chain_decay, 1, 2),
    )
    dual, seen, block, chain = pl.pallas_call(
        write_out,
        out_shape=[jax.ShapeDtypeStruct(r.shape, jnp.float32) for r in results],
        in_specs=[small] * 4,
        out_specs=[place] * 4,
        compiler_params=pltpu.CompilerParams(vmem_limit_bytes=1024 * 1024),
    )(*[pltpu.with_memory_space_constraint(r, pltpu.VMEM) for r in results])
    return (
        dual.reshape(increment.shape), seen, block.reshape(increment.shape), chain.reshape(increment.shape),
    )


def solution(mesh):
    state = P("tm", None, "lev", None, None)
    obs = P("tm", "lev", None)
    return jax.shard_map(
        shards,
        mesh=mesh,
        in_specs=(state, state, state, obs, obs, obs, P("lev"), P("lev"), P("tm", None, "lev")),
        out_specs=(state, obs, state, state),
        check_vma=False,
    )
```

```python
from typing import Any, NamedTuple

import jax
import jax.numpy as jnp
from jax import lax
from jax.experimental import pallas as pl
from jax.experimental.pallas import tpu as pltpu
from jax.sharding import PartitionSpec as P

TIME_STEP = 0.25
ROTATION_PARAM = 0.5
COUPLING = 0.25
HALF = TIME_STEP * ROTATION_PARAM
SPLIT = 8
PAD = 8
MESH_ID = pl.DeviceIdType.MESH


class Scratch(NamedTuple):
    inc: Any
    mult: Any
    work: Any
    b1: Any
    own: Any
    swap: Any
    tangent: Any
    adjoint: Any
    sent: Any
    relay_t: Any
    relay_a: Any
    sums: Any
    met: Any
    total: Any
    columns: Any
    added: Any
    decay: Any
    decay_in: Any
    decay_relay: Any
    cells: Any
    obs_dual: Any
    obs_var: Any
    gain: Any
    depth: Any
    chain_decay: Any
    sends: Any
    own_recv: Any
    loads: Any
    tan_recv: Any
    adj_recv: Any
    rt_recv: Any
    ra_recv: Any
    ch_recv: Any
    decay_send: Any
    decay_recv: Any
    small_loads: Any
    lev_send: Any
    lev_recv: Any


def pieces(rows):
    return SPLIT if rows % (8 * SPLIT) == 0 else 1


def block_rows(rows):
    part = rows // pieces(rows)
    return next(b for b in (32, 16, 8, part) if part % b == 0)


def up_y(a):
    lane = lax.broadcasted_iota(jnp.int32, a.shape, 1)
    return jnp.where(lane == a.shape[1] - 1, 0.0, pltpu.roll(a, a.shape[1] - 1, 1))


def down_y(a):
    lane = lax.broadcasted_iota(jnp.int32, a.shape, 1)
    return jnp.where(lane == 0, 0.0, pltpu.roll(a, 1, 1))


def up_x(a):
    return pltpu.roll(a, a.shape[0] - 1, 0)


def down_x(a):
    return pltpu.roll(a, 1, 0)


def kernel(
    n, size, increment, multiplier, error_var, cell_at, obs_dual_at, obs_var_at, gain_at, depth_at,
    decay_at, tangent_in, obs_out, adjoint_in, carried, *scratch,
):
    b = Scratch(*scratch)
    obs_cell, obs_dual, obs_var = b.cells, b.obs_dual, b.obs_var
    level_gain, mean_depth, chain_decay = b.gain, b.depth, b.chain_decay
    fields, levels, rows, cols = increment.shape[1:]
    planes = fields * levels
    per = pieces(rows)
    chunks = planes * per
    part = rows // per
    step = block_rows(rows)
    wide = step + 2 * PAD

    s = lax.axis_index("tm")
    lev = lax.axis_index("lev")
    odd = s % 2
    even = odd == 0
    pair = s // 2
    pairs = n // 2
    partner = s + 1 - 2 * odd

    def adjoint_cut(k):
        return chunks * (pairs - 1 - k) // pairs

    def tangent_cut(k):
        return chunks * (k + 1) // max(pairs - 1, 1)

    def loop(low, high, fn):
        lax.fori_loop(low, high, lambda c, z: (fn(c), z)[1], 0)

    def where_in(c):
        return c // per, pl.ds(pl.multiple_of((c % per) * part, 8), part)

    def piece(ref, c):
        p, r = where_in(c)
        return ref.at[p, r, :]

    def remote(src, dst, send, recv, where):
        return pltpu.make_async_remote_copy(
            src_ref=src, dst_ref=dst, send_sem=send, recv_sem=recv, device_id=where, device_id_type=MESH_ID,
        )

    def move(src, dst, send, recv, c, to):
        return remote(piece(src, c), piece(dst, c), send, recv.at[c], {"tm": to})

    def lev_move(src, dst, i, to):
        return remote(src, dst, b.lev_send.at[i], b.lev_recv.at[i], {"lev": to})

    def own_copy(c):
        return remote(piece(b.own, c), piece(b.swap, c), b.sends.at[0], b.own_recv.at[c // per], {"tm": partner})

    def own_plane(p):
        return remote(b.own.at[p], b.swap.at[p], b.sends.at[0], b.own_recv.at[p], {"tm": partner})

    def all_sent(src, dst, i):
        remote(src, dst, b.sends.at[i], b.own_recv.at[0], {"tm": partner}).wait_send()

    def tangent_copy(c):
        return move(b.tangent, tangent_in, b.sends.at[1], b.tan_recv, c, s + 1)

    def adjoint_copy(c):
        return move(b.adjoint, adjoint_in, b.sends.at[2], b.adj_recv, c, s - 1)

    def chain_copy(c):
        return move(b.sent, carried, b.sends.at[3], b.ch_recv, c, s + 2)

    def tangent_leg(c, to):
        return remote(piece(b.tangent, c), b.relay_t.at[c], b.sends.at[1], b.rt_recv.at[c], {"tm": to})

    def tangent_turn(c, to):
        return remote(b.relay_t.at[c], piece(tangent_in, c), b.sends.at[4], b.tan_recv.at[c], {"tm": to})

    def adjoint_leg(c, to):
        return remote(piece(b.adjoint, c), b.relay_a.at[c], b.sends.at[2], b.ra_recv.at[c], {"tm": to})

    def adjoint_turn(c, to):
        return remote(b.relay_a.at[c], piece(adjoint_in, c), b.sends.at[5], b.adj_recv.at[c], {"tm": to})

    decay_copy = remote(b.decay, b.decay_in, b.decay_send.at[0], b.decay_recv.at[0], {"tm": s - 1})
    decay_leg = remote(b.decay, b.decay_relay, b.decay_send.at[0], b.decay_recv.at[1], {"tm": s - 2})
    decay_turn = remote(b.decay_relay, b.decay_in, b.decay_send.at[1], b.decay_recv.at[0], {"tm": s + 1})
    turns = jnp.logical_and(even, s < n - 2)

    def load(i, p, low, high, sem):
        src = (increment, multiplier, error_var)[i]
        dst = (b.inc, b.mult, b.work)[i]
        return pltpu.make_async_copy(
            src.at[0, p // levels, p % levels, pl.ds(low, high - low), :],
            dst.at[p, pl.ds(PAD + low, high - low), :], b.loads.at[sem],
        )

    def loaded(low, high, sem):
        pltpu.make_async_copy(
            increment.at[0, :, 0, pl.ds(low, high - low), :],
            b.inc.at[pl.ds(0, fields), pl.ds(PAD + low, high - low), :], b.loads.at[sem],
        ).wait()

    barrier = pltpu.get_barrier_semaphore()
    near = ((s >= 0, partner), (s >= 2, s - 2), (s < n - 2, s + 2))
    for there, who in near:
        @pl.when(there)
        def _():
            pl.semaphore_signal(barrier, inc=1, device_id={"tm": who}, device_id_type=MESH_ID)
    bits = []
    bit = 1
    while bit < size:
        bits.append(bit)
        bit *= 2

    def across(bit):
        return lev + bit - 2 * bit * ((lev // bit) % 2)

    for bit in bits:
        pl.semaphore_signal(barrier, inc=1, device_id={"lev": across(bit)}, device_id_type=MESH_ID)

    small_loads = [
        pltpu.make_async_copy(src, dst, b.small_loads.at[i])
        for i, (src, dst) in enumerate((
            (decay_at, chain_decay), (gain_at, level_gain), (depth_at, mean_depth),
            (cell_at, obs_cell), (obs_dual_at, obs_dual), (obs_var_at, obs_var),
        ))
    ]
    for i in range(3):
        load(i, 0, 0, part, planes).start()
    small_loads[0].start()
    for p in range(planes):
        low = part if p == 0 else 0
        if low < rows:
            for i in range(3):
                load(i, p, low, rows, p).start()
    for copy in small_loads[1:]:
        copy.start()

    def edges(ref, planes):
        zero = jnp.zeros((PAD, cols), jnp.float32)
        for p in range(planes):
            ref[p, pl.ds(0, PAD), :] = zero
            ref[p, pl.ds(PAD + rows, PAD), :] = zero

    def own_at(c):
        p, r = where_in(c)

        if isinstance(c, int):
            if c == 0:
                loaded(0, part, planes)
            elif c == 1 and per > 1:
                loaded(part, rows, 0)
            else:
                loaded(0, rows, p)
        else:
            @pl.when(c % per == 0)
            def _():
                loaded(0, rows, p)

        inner = pl.ds(pl.multiple_of((c % per) * part + PAD, 8), part)
        b.own[p, r, :] = b.work[p, inner, :] * b.mult[p, inner, :] + b.inc[p, inner, :]

    gives_own = jnp.logical_or(even, s < n - 1)

    def give_own(c):
        @pl.when(gives_own)
        def _():
            own_copy(c).start()

    with jax.named_scope("greet"):
        own_at(0)
        pl.semaphore_wait(barrier, len(bits) + sum(there.astype(jnp.int32) for there, _ in near))

    def own_next(c):
        own_at(c)
        give_own(c - 1)

    with jax.named_scope("own"):
        give_own(0)
        own_at(1)
        small_loads[0].wait()
        for f in range(fields):
            for l in range(levels):
                b.decay[f * levels + l] = jnp.full((1, 128), chain_decay[0, l, f], jnp.float32)

        @pl.when(odd == 1)
        def _():
            decay_copy.start()

        @pl.when(jnp.logical_and(even, s >= 2))
        def _():
            decay_leg.start()

        loop(2, chunks, own_next)
        give_own(chunks - 1)

    for copy in small_loads[1:]:
        copy.wait()
    for ref in (b.inc, b.mult, b.work, b.b1):
        edges(ref, planes)
    edges(b.columns, 4)

    def row_index(r0):
        return lax.broadcasted_iota(jnp.int32, (wide, cols), 0) + (r0 - PAD)

    def forward(h, u, v, column, r0, gain, depth):
        p = gain * h
        if column is not None:
            p = p + COUPLING * column
        u_new = u + TIME_STEP * (ROTATION_PARAM * v - (up_x(p) - p))
        v_new = v - TIME_STEP * (ROTATION_PARAM * u + (up_y(p) - p))
        u_new = jnp.where(row_index(r0) < 0, 0.0, u_new)
        h_new = h - TIME_STEP * depth * ((u_new - down_x(u_new)) + (v_new - down_y(v_new)))
        return h_new, u_new, v_new

    def back(h, u, v, r0, gain, depth):
        w = depth * h
        u2 = u + TIME_STEP * (up_x(w) - w)
        v2 = v + TIME_STEP * (up_y(w) - w)
        u2 = jnp.where(row_index(r0) < 0, 0.0, u2)
        p = TIME_STEP * ((u2 - down_x(u2)) + (v2 - down_y(v2)))
        return h + gain * p, u2 - HALF * v2, v2 + HALF * u2, p

    def middle(a):
        return a[PAD:PAD + step]

    def state_at(ref, l, r0):
        at = pl.ds(r0, wide)
        return ref[l, at, :], ref[levels + l, at, :], ref[2 * levels + l, at, :]

    def sweep(fn):
        loop(0, rows // step, lambda i: fn(pl.multiple_of(i * step, 8)))

    def put(ref, l, r0, values):
        for f, value in enumerate(values):
            ref[f * levels + l, pl.ds(r0, step), :] = middle(value)

    def put_padded(ref, l, r0, values):
        put(ref, l, r0 + PAD, values)

    sums = b.sums

    def ahead(r0):
        c0 = c1 = None
        for l in range(levels):
            h, u, v = state_at(b.inc, l, r0)
            h_new, _, _ = forward(h, u, v, None, r0, level_gain[l], mean_depth[l])
            c0 = middle(h) if c0 is None else c0 + middle(h)
            c1 = middle(h_new) if c1 is None else c1 + middle(h_new)
        sums[0, pl.ds(r0, step), :] = c0
        sums[0, pl.ds(rows + r0, step), :] = c1

    def behind(source, to):
        def fn(r0):
            bar = None
            for l in range(levels):
                h, u, v = state_at(source, l, r0)
                h2, u2, v2, p = back(h, u, v, r0, level_gain[l], mean_depth[l])
                if to == 0:
                    put_padded(b.b1, l, r0, (h2, u2, v2))
                bar = middle(p) if bar is None else bar + middle(p)
            sums[1, pl.ds(to * rows + r0, step), :] = COUPLING * bar
        return fn

    with jax.named_scope("ahead"):
        sweep(ahead)
    with jax.named_scope("behind"):
        sweep(behind(b.mult, 0))
        sweep(behind(b.b1, 1))
    depth_sum = mean_depth[0]
    for l in range(1, levels):
        depth_sum = depth_sum + mean_depth[l]
    for k in range(2):
        sums[k, pl.ds(2 * rows, PAD), :] = jnp.full((PAD, cols), depth_sum, jnp.float32)

    half = lev % 2
    tall = 2 * rows + PAD
    total = b.total

    def meet_copy():
        return lev_move(sums.at[1 - half], b.met.at[0], 0, across(1))

    def add_met(slot, first):
        def fn(r0):
            at = pl.ds(r0, PAD)
            kept = sums[half, at, :] if first else total[at, :]
            total[at, :] = kept + b.met[slot, at, :]
        loop(0, tall // PAD, lambda i: fn(pl.multiple_of(i * PAD, 8)))

    meet = meet_copy()
    with jax.named_scope("meet"):
        meet.start()
        meet.wait()
        add_met(0, True)

    def observe():
        count = obs_cell.shape[2]
        if cols & (cols - 1) == 0:
            shift = cols.bit_length() - 1

            def split(cells):
                return cells >> shift, cells & (cols - 1)
        else:
            def split(cells):
                return lax.div(cells, cols), lax.rem(cells, cols)

        row = lax.broadcasted_iota(jnp.int32, (rows, count), 0)
        col = lax.broadcasted_iota(jnp.int32, (cols, count), 0)
        for l in range(levels):
            at_row, at_col = split(obs_cell[0, pl.ds(l, 1), :])
            values = obs_dual[0, pl.ds(l, 1), :]
            hit_row = jnp.where(row == at_row, 1.0, 0.0)
            hit_col = jnp.where(col == at_col, 1.0, 0.0)
            seen = lax.dot_general(
                b.inc[l, pl.ds(PAD, rows), :], hit_col, (((1,), (0,)), ((), ())),
                precision=lax.Precision.HIGHEST, preferred_element_type=jnp.float32,
            )
            picked = jnp.sum(hit_row * seen, axis=0, keepdims=True)
            obs_out[0, pl.ds(l, 1), :] = obs_var[0, pl.ds(l, 1), :] * values + picked
            b.added[l] = lax.dot_general(
                hit_row * values, hit_col, (((1,), (1,)), ((), ())),
                precision=lax.Precision.HIGHEST, preferred_element_type=jnp.float32,
            )

    for i, bit in enumerate(bits[1:], 1):
        far = lev_move(total, b.met.at[i], i, across(bit))
        far.start()
        if i == 1:
            with jax.named_scope("observe"):
                observe()
        with jax.named_scope("far"):
            far.wait()
            add_met(i, False)
    if len(bits) < 2:
        observe()

    columns = b.columns

    def first_column(r0):
        columns[2 * half, pl.ds(r0 + PAD, step), :] = total[pl.ds(r0, step), :]

    def second_column(r0):
        c = columns[2 * half, pl.ds(r0, wide), :]
        gx = jnp.where(row_index(r0) < 0, 0.0, up_x(c) - c)
        gy = up_y(c) - c
        lap = (gx - down_x(gx)) + (gy - down_y(gy))
        scale = (TIME_STEP * TIME_STEP * COUPLING) * total[pl.ds(2 * rows, 1), pl.ds(0, 1)]
        columns[2 * half + 1, pl.ds(r0 + PAD, step), :] = total[pl.ds(rows + r0, step), :] + scale * middle(lap)

    with jax.named_scope("column"):
        sweep(first_column)
        sweep(second_column)
    mine = columns.at[pl.ds(2 * half, 2)]
    near_copy = lev_move(mine, mine, len(bits), across(1))
    with jax.named_scope("near"):
        near_copy.start()
        near_copy.wait()

    def last_back(r0):
        at = pl.ds(r0, wide)
        bar0, bar1 = columns[2, at, :], columns[3, at, :]
        for l in range(levels):
            h, u, v = state_at(b.b1, l, r0)
            h2, u2, v2, _ = back(h + bar0, u, v, r0, level_gain[l], mean_depth[l])
            put(b.adjoint, l, r0, (h2 + bar1, u2, v2))

    def first_forward(r0):
        column = columns[0, pl.ds(r0, wide), :]
        for l in range(levels):
            h, u, v = state_at(b.inc, l, r0)
            put_padded(b.work, l, r0, forward(h, u, v, column, r0, level_gain[l], mean_depth[l]))

    def last_forward(r0):
        column = columns[1, pl.ds(r0, wide), :]
        for l in range(levels):
            h, u, v = state_at(b.work, l, r0)
            put(b.tangent, l, r0, forward(h, u, v, column, r0, level_gain[l], mean_depth[l]))

    @pl.when(turns)
    def _():
        decay_leg.wait_recv()
        decay_turn.start()

    with jax.named_scope("back"):
        sweep(last_back)
    below = pair - 1
    down_cut = adjoint_cut(below)
    across_cut = adjoint_cut(pair)

    @pl.when(jnp.logical_and(even, s >= 2))
    def _():
        loop(0, down_cut, lambda c: adjoint_leg(c, s - 2).start())
        loop(down_cut, chunks, lambda c: adjoint_leg(c, s + 1).start())

    with jax.named_scope("forward"):
        sweep(first_forward)
        sweep(last_forward)
    up_cut = tangent_cut(pair)
    here_cut = tangent_cut(below)
    climbs = jnp.logical_and(odd == 1, s < n - 1)

    @pl.when(even)
    def _():
        loop(0, chunks, lambda c: tangent_copy(c).start())

    @pl.when(climbs)
    def _():
        loop(0, up_cut, lambda c: tangent_leg(c, s + 2).start())
        loop(up_cut, chunks, lambda c: tangent_leg(c, s - 1).start())

    def chain_step(c):
        p, r = where_in(c)
        d = chain_decay[0, p % levels, p // levels]

        @pl.when(s >= 1)
        def _():
            tangent_copy(c).wait_recv()

        @pl.when(s == 0)
        def _():
            tangent_in[p, r, :] = jnp.zeros((part, cols), jnp.float32)

        @pl.when(s >= 2)
        def _():
            chain_copy(c).wait_recv()

        @pl.when(s < 2)
        def _():
            carried[p, r, :] = jnp.zeros((part, cols), jnp.float32)

        @pl.when(jnp.logical_and(c % per == 0, jnp.logical_or(odd == 1, s < n - 2)))
        def _():
            own_plane(p).wait_recv()

        swap = b.swap[p, r, :]
        product = b.own[p, r, :] - tangent_in[p, r, :]
        here = d * (carried[p, r, :] + jnp.where(odd == 1, swap, 0.0)) + product

        @pl.when(s < n - 2)
        def _():
            d_next = b.decay_in[p][:, :1]
            b.sent[p, r, :] = d_next * here + (jnp.where(even, swap, 0.0) - b.tangent[p, r, :])

        tangent_in[p, r, :] = product
        carried[p, r, :] = here

        @pl.when(s < n - 2)
        def _():
            chain_copy(c).start()

    @pl.when(s == 0)
    def _():
        decay_copy.wait_recv()

    with jax.named_scope("chain0"):
        loop(0, jnp.where(s == 0, chunks, 0), chain_step)

    @pl.when(jnp.logical_and(even, s < n - 2))
    def _():
        def turn_up(c):
            tangent_leg(c, s - 1).wait_recv()
            tangent_turn(c, s + 2).start()

        def turn_across(c):
            adjoint_leg(c, s - 2).wait_recv()
            adjoint_turn(c, s + 1).start()

        with jax.named_scope("turn_up"):
            loop(up_cut, chunks, turn_up)
        with jax.named_scope("turn_over"):
            loop(0, across_cut, turn_across)

    early = jnp.where(s == n - 1, chunks // 2, 0)

    @pl.when(odd == 1)
    def _():
        loop(0, early, lambda c: adjoint_copy(c).start())

        @pl.when(s >= 3)
        def _():
            def turn_across(c):
                tangent_leg(c, s + 2).wait_recv()
                tangent_turn(c, s - 1).start()

            with jax.named_scope("turn_back"):
                loop(0, here_cut, turn_across)

        loop(early, chunks, lambda c: adjoint_copy(c).start())

        @pl.when(s >= 3)
        def _():
            def turn_down(c):
                adjoint_leg(c, s + 1).wait_recv()
                adjoint_turn(c, s - 2).start()

            with jax.named_scope("turn_down"):
                loop(down_cut, chunks, turn_down)

    def block_step(i):
        c = lax.rem(i + across_cut * odd, chunks)
        p, r = where_in(c)
        inner = pl.ds(pl.multiple_of((c % per) * part + PAD, 8), part)

        @pl.when(s < n - 1)
        def _():
            adjoint_copy(c).wait_recv()

        kept = b.mult[p, inner, :] - jnp.where(s < n - 1, adjoint_in[p, r, :], 0.0)
        adjoint_in[p, r, :] = kept

        @pl.when(p < levels)
        def _():
            adjoint_in[p, r, :] = kept + b.added[jnp.minimum(p, levels - 1), r, :]

    loop(0, jnp.where(s == n - 1, chunks, 0), block_step)

    @pl.when(jnp.logical_and(s > 0, s < n - 1))
    def _():
        decay_copy.wait_recv()

    with jax.named_scope("chain"):
        loop(0, jnp.where(s == 0, 0, chunks), chain_step)

    with jax.named_scope("block"):
        loop(0, jnp.where(s == n - 1, 0, chunks), block_step)

    with jax.named_scope("drain"):
        @pl.when(gives_own)
        def _():
            all_sent(b.own, b.swap, 0)

        @pl.when(s < n - 1)
        def _():
            all_sent(b.tangent, tangent_in, 1)

        @pl.when(s >= 1)
        def _():
            all_sent(b.adjoint, adjoint_in, 2)
            decay_copy.wait_send()

        @pl.when(turns)
        def _():
            decay_turn.wait_send()

        def turned(ref, i, count):
            if count:
                all_sent(ref.at[pl.ds(0, count)], ref.at[pl.ds(0, count)], i)

        for k in range(pairs - 1):
            @pl.when(s == 2 * k)
            def _():
                turned(b.relay_t, 4, chunks - tangent_cut(k))
                turned(b.relay_a, 5, adjoint_cut(k))

            @pl.when(s == 2 * k + 3)
            def _():
                turned(b.relay_t, 4, tangent_cut(k))
                turned(b.relay_a, 5, chunks - adjoint_cut(k))

        @pl.when(s < n - 2)
        def _():
            all_sent(b.sent, carried, 3)


def write_out(dual_in, seen_in, block_in, chain_in, dual, seen, block, chain):
    def copy_all(sems):
        copies = [
            pltpu.make_async_copy(src, dst, sems.at[i])
            for i, (src, dst) in enumerate(((dual_in, dual), (block_in, block), (chain_in, chain), (seen_in, seen)))
        ]
        for i, copy in enumerate(copies):
            copy.start(priority=(i + 1) % 2)
        for copy in copies:
            copy.wait()

    pl.run_scoped(copy_all, pltpu.SemaphoreType.DMA((4,)))


def shards(
    increment, multiplier, error_var, obs_cell, obs_dual, obs_var,
    level_gain, mean_depth, chain_decay,
):
    n = lax.axis_size("tm")
    size = lax.axis_size("lev")
    if n % 2 or size < 2 or size & (size - 1):
        raise ValueError("unsupported mesh")
    _, fields, levels, rows, cols = increment.shape
    planes = fields * levels
    chunks = planes * pieces(rows)
    rounds = size.bit_length() - 1
    tall = 2 * rows + PAD

    def room(*shape):
        return pltpu.VMEM(shape, jnp.float32)

    def flags(count):
        return pltpu.SemaphoreType.DMA((count,))

    scratch = [
        *[room(planes, rows + 2 * PAD, cols)] * 4,
        *[room(planes, rows, cols)] * 5, *[room(chunks, rows // pieces(rows), cols)] * 2,
        room(2, tall, cols), room(rounds, tall, cols), room(tall, cols),
        room(4, rows + 2 * PAD, cols), room(levels, rows, cols),
        *[room(planes, 1, 128)] * 3,
        pltpu.VMEM(obs_cell.shape, jnp.int32), room(*obs_dual.shape), room(*obs_var.shape),
        pltpu.SMEM(level_gain.shape, jnp.float32), pltpu.SMEM(mean_depth.shape, jnp.float32),
        pltpu.SMEM((1, levels, fields), jnp.float32),
    ]
    sems = [
        flags(6), flags(planes), flags(planes + 1), *[flags(chunks)] * 5,
        flags(2), flags(2), flags(6), flags(rounds + 1), flags(rounds + 1),
    ]

    def scoped(*refs):
        pl.run_scoped(lambda *scope: kernel(n, size, *refs, *scope), *sems)

    place = pl.BlockSpec(memory_space=pl.ANY)
    small = pl.BlockSpec(memory_space=pltpu.VMEM)
    held = pltpu.VMEM((planes, rows, cols), jnp.float32)
    results = pl.pallas_call(
        scoped,
        out_shape=[held, pltpu.VMEM(obs_dual.shape, jnp.float32), held, held],
        in_specs=[place] * 9,
        out_specs=[small] * 4,
        scratch_shapes=scratch,
        compiler_params=pltpu.CompilerParams(
            collective_id=0, has_side_effects=True, vmem_limit_bytes=50 * 1024 * 1024
        ),
    )(
        increment, multiplier, error_var, obs_cell, obs_dual, obs_var,
        level_gain, mean_depth, jnp.swapaxes(chain_decay, 1, 2),
    )
    dual, seen, block, chain = pl.pallas_call(
        write_out,
        out_shape=[jax.ShapeDtypeStruct(r.shape, jnp.float32) for r in results],
        in_specs=[small] * 4,
        out_specs=[place] * 4,
        compiler_params=pltpu.CompilerParams(vmem_limit_bytes=1024 * 1024),
    )(*[pltpu.with_memory_space_constraint(r, pltpu.VMEM) for r in results])
    return (
        dual.reshape(increment.shape), seen, block.reshape(increment.shape), chain.reshape(increment.shape),
    )


def solution(mesh):
    state = P("tm", None, "lev", None, None)
    obs = P("tm", "lev", None)
    return jax.shard_map(
        shards,
        mesh=mesh,
        in_specs=(state, state, state, obs, obs, obs, P("lev"), P("lev"), P("tm", None, "lev")),
        out_specs=(state, obs, state, state),
        check_vma=False,
    )
```
